128 devices in a mesh: seq: 16 (over x, y_lo, core), tp: 8 (over z, y_hi).
Axes of the slice: x: 4, y: 4 (y_hi: 2, y_lo: 2; y = y_hi * 2 + y_lo), z: 4, core: 2. Of those that a mesh axis runs over, the one named last changes fastest.
Arguments:
- x_old: bfloat16 [8192, 4608], P('seq', 'tp'), may hold values from -6 to 6
- old_blocks: int32 [16], replicated, may hold values from 1 to 4, 32 in all
- new_blocks: int32 [16], replicated, may hold values from 1 to 4, 32 in all
- order: int32 [16], replicated, may hold values from 0 to 15, as said below
- pre_gain: float32 [4608], replicated, may hold values from 0.25 to 1.75
- post_gain: float32 [4608], replicated, may hold values from 0.25 to 1.75
- w_query: bfloat16 [4608, 4096], P('seq', 'tp'), may hold values from -0.59765625 to 0.59765625
- w_key: bfloat16 [4608, 2048], P('seq', 'tp'), may hold values from -0.09375 to 0.09375
- w_value: bfloat16 [4608, 2048], P('seq', 'tp'), may hold values from -0.09375 to 0.09375
- w_out_t: bfloat16 [4608, 4096], P('seq', 'tp'), may hold values from -0.09375 to 0.09375
Outputs:
- layer_out: bfloat16 [8192, 4608], P(('seq', 'tp'))
The draws below stay inside these ranges and needn't reach their ends.
Inputs may be any that keep to these rules, and one draw needn't show every extreme that they name: `old_blocks`: counts of 128-row blocks, at least one each; they sum to 32, and the largest is exactly 4. `new_blocks`: counts of 128-row blocks, at least one each; they sum to 32, and the largest is exactly 4. A permutation of the seq indices with order[15] = 0 and order[7] = 15; the other indices, taken in increasing order, hold 1 to 14 in increasing order, except that aligned pairs of them (first and second, third and fourth, and so on) are swapped or not, pair by pair.
All inputs are finite; a program needn't handle non-finite values.
Results may differ from the reference program's by a relative error of at most 0.013.
Values may be sent and summed in bfloat16 or wider, within the bound.
No kernel may reach another device: no remote copies, remote signals or barrier semaphores. Data moves between devices by JAX's collectives and lax.ppermute only.
A program may use at most 128 MiB of HBM per device.

```python
import math
import jax
import jax.numpy as jnp
import numpy as np
from jax import lax

D = 4608
HEADS = 32
KV_HEADS = 16
HEAD = 128
BLOCK = 128
CAP = 512
TOKENS = 4096
SLOTS = 8192
N_SEQ = 16
N_TP = 8


def draw_order(key, part):
    middle = N_SEQ - 2
    kept = [place for place in range(N_SEQ) if place != N_SEQ - 1 and place != N_SEQ // 2 - 1]
    flips = jax.random.randint(jax.random.fold_in(key, 7), (middle // 2,), 0, 2).astype(jnp.int32)
    ranks = jnp.arange(middle, dtype=jnp.int32)
    shards = (jnp.bitwise_xor(ranks, jnp.repeat(flips, 2)) + 1).astype(jnp.int32)
    result = jnp.zeros((N_SEQ,), jnp.int32)
    result = result.at[jnp.array(kept, dtype=jnp.int32)].set(shards)
    result = result.at[N_SEQ - 1].set(0)
    result = result.at[N_SEQ // 2 - 1].set(N_SEQ - 1)
    return result.astype(jnp.int32)


def block_levels(rng, shape, cuts, least, largest):
    factor_of = 1.0
    for axis_at, shards_of in cuts:
        steps = jax.random.uniform(jax.random.fold_in(jax.random.fold_in(rng, 6), axis_at), (shards_of,), jnp.float32, least / len(cuts), largest / len(cuts))
        factor_of = factor_of * jnp.repeat(jnp.exp(steps), shape[axis_at] // shards_of).reshape((-1,) + (1,) * (len(shape) - 1 - axis_at))
    return factor_of


def split_up(number_of, total, reach, slope):
    portions = [(1 << 20) // math.isqrt(standing ** slope) + 1 for standing in range(2, number_of + 1)]
    rest, holding = total - reach - (number_of - 1), [1] * (number_of - 1)
    while rest > 0:
        movable = [i for i in range(number_of - 1) if holding[i] < reach]
        pool, left = sum([portions[i] for i in movable]), rest
        for i in movable:
            addition = min(reach - holding[i], max(1, left * portions[i] // pool), rest)
            holding[i] = holding[i] + addition
            rest = rest - addition
    return np.array([reach] + holding)


def uneven_parts(rng, number_of, total, reach, skew):
    if number_of == 2:
        one = jax.random.randint(rng, (), max(1, total - reach), min(reach, total - 1) + 1)
        return jnp.stack([one, total - one])
    lengths = jnp.asarray(split_up(number_of, total, reach, skew), jnp.int32)
    twos = (number_of - 1) // 2
    donor, receiver = lengths[1:1 + 2 * twos:2], lengths[2:2 + 2 * twos:2]
    room = jnp.minimum(donor - 1, reach - receiver)
    shifted = jax.random.randint(jax.random.fold_in(rng, 1), (twos,), 0, 1 << 20) % (room + 1)
    lengths = lengths.at[1:1 + 2 * twos:2].set(donor - shifted).at[2:2 + 2 * twos:2].set(receiver + shifted)
    return lengths[jax.random.permutation(jax.random.fold_in(rng, 2), number_of)]


def noise(key, shape, scale, bound, pieces=(), kind=jnp.bfloat16):
    values = jax.random.normal(key, shape, jnp.float32) * scale
    if len(pieces) > 0:
        values = block_levels(key, shape, pieces, -0.22, 0.18) * values
    return jnp.clip(values, min=-bound, max=bound).astype(kind)


def setup_inputs(seed: int = 0) -> dict:
    key_list = jax.random.split(jax.random.key(seed), 11)
    return {
        "x_old": noise(key_list[0], (SLOTS, D), 1.0, 6.0, ((0, 16), (1, 8))),
        "old_blocks": uneven_parts(key_list[1], N_SEQ, TOKENS // BLOCK, CAP // BLOCK, 1).astype(jnp.int32),
        "new_blocks": uneven_parts(key_list[2], N_SEQ, TOKENS // BLOCK, CAP // BLOCK, 2).astype(jnp.int32),
        "order": draw_order(jax.random.fold_in(key_list[10], 71), 0),
        "pre_gain": jnp.clip(1.0 + 0.15 * jax.random.normal(key_list[4], (D,), jnp.float32), 0.25, 1.75),
        "post_gain": jnp.clip(1.0 + 0.15 * jax.random.normal(key_list[5], (D,), jnp.float32), 0.25, 1.75),
        "w_query": noise(key_list[6], (D, HEADS * HEAD), 0.1, 0.59765625, ((0, 16), (1, 8))),
        "w_key": noise(key_list[7], (D, KV_HEADS * HEAD), D ** -0.5, 0.09375, ((0, 16), (1, 8))),
        "w_value": noise(key_list[8], (D, KV_HEADS * HEAD), D ** -0.5, 0.09375, ((0, 16), (1, 8))),
        "w_out_t": noise(key_list[9], (D, HEADS * HEAD), (HEADS * HEAD) ** -0.5, 0.09375, ((0, 16), (1, 8))),
    }


EPS = 1e-06

def offsets(blocks):
    return ((jnp.cumsum(blocks) - blocks) * BLOCK).astype(jnp.int32)

def rotate(values, places):
    half = values.shape[-1] // 2
    inverse = jnp.exp(jnp.arange(half, dtype=jnp.float32) * (-2.0 * math.log(10000.0) / values.shape[-1]))
    angles = places.astype(jnp.float32)[:, None] * inverse[None, :]
    cosine = jnp.cos(angles)[:, None, :]
    sine = jnp.sin(angles)[:, None, :]
    first = values[..., :half]
    second = values[..., half:]
    return jnp.concatenate([first * cosine - second * sine, second * cosine + first * sine], axis=-1)

def rms_scale(values, gain):
    return values * lax.rsqrt(lax.optimization_barrier(jnp.mean(values * values, axis=-1, keepdims=True)) + EPS) * gain

def reference(x_old, old_blocks, new_blocks, order, pre_gain, post_gain, w_query, w_key, w_value, w_out_t):
    old_start = offsets(old_blocks)
    new_start = offsets(new_blocks)
    seq_rows = jnp.arange(TOKENS, dtype=jnp.int32)
    shard = (lax.optimization_barrier(jnp.sum((old_start[None, :] <= seq_rows[:, None]).astype(jnp.int32), axis=1)) - 1).astype(jnp.int32)
    devices = jnp.arange(N_SEQ, dtype=jnp.int32)
    holder = lax.optimization_barrier(jnp.sum(devices[None, :] * (order[None, :] == shard[:, None]).astype(jnp.int32), axis=1)).astype(jnp.int32)
    source = (holder * CAP + seq_rows - old_start[shard]).astype(jnp.int32)
    resident = x_old[source]
    resident_f = resident.astype(jnp.float32)
    normed = rms_scale(resident_f, pre_gain).astype(jnp.bfloat16)
    query = jnp.dot(normed, w_query, preferred_element_type=jnp.float32).reshape(TOKENS, HEADS, HEAD)
    query = (rotate(query, seq_rows) * (D // HEADS) ** (-0.5)).astype(jnp.bfloat16)
    key = jnp.dot(normed, w_key, preferred_element_type=jnp.float32).reshape(TOKENS, KV_HEADS, HEAD)
    key = rotate(key, seq_rows).astype(jnp.bfloat16)
    value = jnp.dot(normed, w_value, preferred_element_type=jnp.float32).reshape(TOKENS, KV_HEADS, HEAD).astype(jnp.bfloat16)
    group = HEADS // KV_HEADS
    query_heads = jnp.transpose(query, (1, 0, 2)).astype(jnp.float32)
    key_heads = jnp.repeat(jnp.transpose(key, (1, 0, 2)), group, axis=0).astype(jnp.float32)
    value_heads = jnp.repeat(jnp.transpose(value, (1, 0, 2)), group, axis=0).astype(jnp.float32)
    causal = seq_rows[None, :] <= seq_rows[:, None]

    def one_head(operands):
        query_one, key_one, value_one = operands
        score = jnp.dot(query_one, key_one.T)
        capped = 50.0 * jnp.tanh(score / 50.0)
        weight = jnp.where(causal, jnp.exp(capped), 0.0)
        total = lax.optimization_barrier(jnp.sum(weight, axis=1))
        weight_b = weight.astype(jnp.bfloat16).astype(jnp.float32)
        numer = jnp.dot(weight_b, value_one)
        return (numer / total[:, None]).astype(jnp.bfloat16)
    context = lax.map(one_head, (query_heads, key_heads, value_heads))
    context = jnp.transpose(context, (1, 0, 2)).reshape(TOKENS, HEADS * HEAD)
    span = HEADS * HEAD // N_TP
    projected = jnp.zeros((TOKENS, D), jnp.float32)
    for group_index in range(N_TP):
        columns = context[:, group_index * span:(group_index + 1) * span]
        weights_part = w_out_t[:, group_index * span:(group_index + 1) * span]
        partial_sum = lax.dot_general(columns, weights_part, (((1,), (1,)), ((), ())), preferred_element_type=jnp.float32)
        projected = projected + lax.optimization_barrier(partial_sum.astype(jnp.bfloat16)).astype(jnp.float32)
    refreshed = (resident_f + rms_scale(projected, post_gain)).astype(jnp.bfloat16)
    slots = jnp.arange(N_SEQ * CAP, dtype=jnp.int32)
    owner = (slots // CAP).astype(jnp.int32)
    within = (slots - owner * CAP).astype(jnp.int32)
    valid = within < new_blocks[owner] * BLOCK
    target = jnp.clip(new_start[owner] + within, 0, TOKENS - 1).astype(jnp.int32)
    return jnp.where(valid[:, None], refreshed[target], jnp.zeros((), jnp.bfloat16)).astype(jnp.bfloat16)
```

```python
import functools
import math

import jax
import jax.numpy as jnp
from jax import lax
from jax.experimental import pallas as pl
from jax.experimental.pallas import tpu as pltpu
from jax.sharding import Mesh
from jax.sharding import PartitionSpec as P

D = 4608
HEADS = 32
HEAD = 128
BLOCK = 128
EPS = 1e-06
F32 = jnp.float32
BF16 = jnp.bfloat16

AXES = ("x", "yl", "c", "z", "yh")
SEQ = ("x", "yl", "c")
TP = ("z", "yh")


SMEM = pl.BlockSpec(memory_space=pltpu.SMEM)


def shift(value, axis, by):
    n = lax.axis_size(axis)
    return lax.ppermute(value, axis, [(i, (i + by) % n) for i in range(n)])


def pick(index, options):
    result = options[-1]
    for k in range(len(options) - 2, -1, -1):
        result = jnp.where(index == k, options[k], result)
    return result


def rope(values, cos, sin):
    half = HEAD // 2
    swapped = jnp.concatenate([values[:, half:], values[:, :half]], axis=1)
    return values * cos + swapped * sin


def norm_kv_kernel(tsrc, *refs):
    pieces, (gain, weight, cos, sin, normed, kv) = refs[:8], refs[8:]
    width = pieces[0].shape[1]

    @pl.when(pl.program_id(0) == 0)
    def _():
        total = jnp.zeros((pieces[0].shape[0], 1), F32)
        for piece in pieces:
            wide = piece[...].astype(F32)
            total = total + jnp.sum(wide * wide, axis=1, keepdims=True)
        scale = lax.rsqrt(total / D + EPS)
        for n, piece in enumerate(pieces):
            normed[n] = (piece[...].astype(F32) * scale * gain[tsrc[n]]).astype(BF16)

    total = jnp.zeros(kv.shape, F32)
    for n in range(8):
        rows = pl.ds(pl.multiple_of(tsrc[n] * width, 64), width)
        total = total + jnp.dot(normed[n], weight[rows, :], preferred_element_type=F32)
    kv[:, :HEAD] = rope(total[:, :HEAD], cos[...], sin[...]).astype(BF16)
    kv[:, HEAD:] = total[:, HEAD:].astype(BF16)


def query_kernel(tsrc, normed, weight, cos, sin, query):
    width = normed.shape[2]
    total = jnp.zeros(query.shape, F32)
    for n in range(8):
        rows = pl.ds(pl.multiple_of(tsrc[n] * width, 64), width)
        total = total + jnp.dot(normed[n], weight[rows, :], preferred_element_type=F32)
    for h in range(query.shape[1] // HEAD):
        cols = slice(h * HEAD, (h + 1) * HEAD)
        turned = rope(total[:, cols], cos[...], sin[...]) * (D // HEADS) ** (-0.5)
        query[:, cols] = turned.astype(BF16)


def attention_kernel(place, query, *refs):
    kv = [refs[4 * k : 4 * k + 4] for k in range(4)]
    context, numer, denom = refs[16:]
    x, w = place[0], place[1]
    numer[...] = jnp.zeros_like(numer)
    denom[...] = jnp.zeros_like(denom)
    row = lax.broadcasted_iota(jnp.int32, (2 * BLOCK, BLOCK), 0) % BLOCK
    col = lax.broadcasted_iota(jnp.int32, (2 * BLOCK, BLOCK), 1)

    def chunk(dw, block, slot, masked):
        if isinstance(block, int):
            q_rows, k_rows = pl.ds(block * BLOCK, BLOCK), pl.ds(slot * BLOCK, BLOCK)
        else:
            q_rows = pl.ds(pl.multiple_of(block * BLOCK, BLOCK), BLOCK)
            k_rows = pl.ds(pl.multiple_of(slot * BLOCK, BLOCK), BLOCK)
        q2 = jnp.concatenate([query[q_rows, :HEAD], query[q_rows, HEAD:]], axis=0)
        keys = jnp.concatenate([kv[dw][d][k_rows, :HEAD] for d in range(4)], axis=0)
        values = jnp.concatenate([kv[dw][d][k_rows, HEAD:] for d in range(4)], axis=0)
        score = lax.dot_general(q2, keys, (((1,), (1,)), ((), ())), preferred_element_type=F32)
        weight = jnp.exp(50.0 * jnp.tanh(score * (1.0 / 50.0)))
        parts = [weight[:, d * BLOCK : (d + 1) * BLOCK] for d in range(4)]
        if masked:
            parts = [jnp.where(col <= row, parts[0], 0.0)] + [
                jnp.where(x >= d, parts[d], 0.0) for d in range(1, 4)
            ]
            weight = jnp.concatenate(parts, axis=1)
        denom[block] += (parts[0] + parts[1]) + (parts[2] + parts[3])
        numer[block] += jnp.dot(weight.astype(BF16), values, preferred_element_type=F32)

    chunk(0, 0, 0, True)
    chunk(0, 1, 0, False)
    chunk(0, 1, 1, True)
    for dw in range(1, 4):
        later = (jnp.bitwise_xor(w, dw) > w).astype(jnp.int32)
        chunk(dw, 1, 0, False)
        chunk(dw, later, later, False)
    for block in range(2):
        out = numer[block] / jnp.sum(denom[block], axis=1, keepdims=True)
        rows = slice(block * BLOCK, (block + 1) * BLOCK)
        context[rows, :HEAD] = out[:BLOCK].astype(BF16)
        context[rows, HEAD:] = out[BLOCK:].astype(BF16)


def out_kernel(place, context, weight, *refs):
    outs, scratch = refs[:8], refs[8]
    z, yh = place[2], place[3]
    scratch[...] = lax.dot_general(
        context[...], weight[...], (((1,), (1,)), ((), ())), preferred_element_type=F32
    ).astype(BF16)
    for dy in range(2):
        for dz in range(4):
            first = jnp.bitwise_xor(yh, dy) * 64 + jnp.bitwise_and(z + dz, 3) * 16
            first = pl.multiple_of(first, 16)
            for block in range(2):
                outs[4 * dy + dz][block * 16 : block * 16 + 16, :] = scratch[
                    pl.ds(pl.multiple_of(first + block * BLOCK, 16), 16), :
                ]


def finish_kernel(resident, gain, *refs):
    terms, out = refs[:8], refs[8]
    total = terms[0][...].astype(F32)
    for term in terms[1:]:
        total = total + term[...].astype(F32)
    scale = lax.rsqrt(jnp.mean(total * total, axis=1, keepdims=True) + EPS)
    out[...] = (resident[...].astype(F32) + total * scale * gain[...]).astype(BF16)


def per_device(
    x_old, old_blocks, new_blocks, order, pre_gain, post_gain, w_query, w_key, w_value, w_out_t
):
    x, yl, c, z, yh = (lax.axis_index(a).astype(jnp.int32) for a in AXES)
    w = 2 * yl + c
    p = 4 * x + w
    old_start = jnp.cumsum(old_blocks) - old_blocks
    new_start = jnp.cumsum(new_blocks) - new_blocks
    ids = jnp.arange(16, dtype=jnp.int32)
    place = jnp.stack([x, w, z, yh])
    tp_src = [2 * ((z - dz) % 4) + (yh ^ dy) for dy in range(2) for dz in range(4)]
    tsrc = jnp.stack(tp_src)
    width = x_old.shape[1]

    qkv_local = jnp.concatenate(
        [w_key[:, :HEAD], w_value[:, :HEAD], w_key[:, HEAD:], w_value[:, HEAD:], w_query], axis=1
    )
    qkv_full = lax.all_gather(qkv_local, SEQ, axis=0, tiled=True)
    out_full = lax.all_gather(w_out_t, SEQ, axis=0, tiled=True)

    my_old = jnp.sum(jnp.where(ids == order[p], old_start, 0))

    def stored(g):
        return lax.dynamic_slice_in_dim(x_old, ((g - my_old) % 4) * BLOCK, BLOCK, 0)

    near = [stored(x)] + [shift(stored((x + d) % 4), "x", d) for d in range(1, 4)]

    def holder(block):
        shard = jnp.sum((old_start <= block).astype(jnp.int32)) - 1
        return jnp.sum(jnp.where(order == shard, ids, 0))

    def targets(a, b):
        to = 2 * a + b
        return [x + 4 * to, x + 28 - 4 * to]

    def candidates(blocks):
        return jnp.concatenate([pick((x - holder(b) // 4) % 4, near) for b in blocks], axis=0)

    mine = targets(yl, c)
    theirs = targets(1 - yl, c)
    passed = shift(candidates(targets(yl, 1 - c) + targets(1 - yl, 1 - c)), "c", 1)
    kept = candidates(mine + theirs)
    merged = [
        jnp.where(
            holder(b) % 2 == c,
            kept[n * BLOCK : (n + 1) * BLOCK],
            passed[n * BLOCK : (n + 1) * BLOCK],
        )
        for n, b in enumerate(mine + theirs)
    ]
    crossed = shift(jnp.concatenate(merged[2:], axis=0), "yl", 1)
    rows = jnp.concatenate(
        [
            jnp.where((holder(b) // 2) % 2 == yl, merged[n], crossed[n * BLOCK : (n + 1) * BLOCK])
            for n, b in enumerate(mine)
        ],
        axis=0,
    )
    count = 2 * BLOCK

    facing = shift(rows, "yh", 1)
    pieces = [rows] + [shift(rows, "z", d) for d in range(1, 4)]
    pieces += [facing] + [shift(facing, "z", d) for d in range(1, 4)]

    slot_rows = jnp.arange(BLOCK, dtype=jnp.int32)
    positions = jnp.concatenate([b * BLOCK + slot_rows for b in mine])
    inverse = jnp.exp(jnp.arange(HEAD // 2, dtype=F32) * (-2.0 * math.log(10000.0) / HEAD))
    angles = positions.astype(F32)[:, None] * inverse[None, :]
    cosine, sine = jnp.cos(angles), jnp.sin(angles)
    cosine = jnp.concatenate([cosine, cosine], axis=1)
    sine = jnp.concatenate([-sine, sine], axis=1)

    whole = lambda *shape: pl.BlockSpec(shape, lambda n: (0,) * len(shape))
    normed, kv = pl.pallas_call(
        norm_kv_kernel,
        grid=(2,),
        in_specs=[SMEM]
        + [whole(count, width)] * 8
        + [
            whole(8, 1, width),
            pl.BlockSpec((D, 2 * HEAD), lambda n: (0, n)),
            whole(count, HEAD),
            whole(count, HEAD),
        ],
        out_specs=[whole(8, count, width), pl.BlockSpec((count, 2 * HEAD), lambda n: (0, n))],
        out_shape=[
            jax.ShapeDtypeStruct((8, count, width), BF16),
            jax.ShapeDtypeStruct((count, 4 * HEAD), BF16),
        ],
        name="norm_kv",
    )(tsrc, *pieces, pre_gain.reshape(8, 1, width), qkv_full, cosine, sine)

    pair = shift(kv, "yl", 1)
    spread = []
    for part in (kv, pair):
        same = [part] + [shift(part, "x", d) for d in range(1, 4)]
        spread.append(same)
        spread.append([shift(s, "c", 1) for s in same])
    spread = [s for same in spread for s in same]

    query = pl.pallas_call(
        query_kernel,
        grid=(2,),
        in_specs=[
            SMEM,
            whole(8, count, width),
            pl.BlockSpec((D, 2 * HEAD), lambda n: (0, n + 2)),
            whole(count, HEAD),
            whole(count, HEAD),
        ],
        out_specs=pl.BlockSpec((count, 2 * HEAD), lambda n: (0, n)),
        out_shape=jax.ShapeDtypeStruct((count, 4 * HEAD), BF16),
        name="query",
    )(tsrc, normed, qkv_full, cosine, sine)

    by_head = pl.BlockSpec((count, 2 * HEAD), lambda n: (0, n))
    context = pl.pallas_call(
        attention_kernel,
        grid=(2,),
        in_specs=[SMEM, by_head] + [by_head] * 16,
        out_specs=by_head,
        out_shape=jax.ShapeDtypeStruct((count, 4 * HEAD), BF16),
        scratch_shapes=[pltpu.VMEM((2, 2 * BLOCK, HEAD), F32), pltpu.VMEM((2, 2 * BLOCK, HEAD), F32)],
        name="attention",
    )(place, query, *spread)

    tile = 512
    shares = pl.pallas_call(
        out_kernel,
        grid=(D // tile,),
        in_specs=[SMEM, whole(count, 4 * HEAD), pl.BlockSpec((tile, 4 * HEAD), lambda n: (n, 0))],
        out_specs=[pl.BlockSpec((32, tile), lambda n: (0, n))] * 8,
        out_shape=[jax.ShapeDtypeStruct((32, D), BF16)] * 8,
        scratch_shapes=[pltpu.VMEM((count, tile), BF16)],
        name="project",
    )(place, context, out_full)
    received = []
    for dy in range(2):
        for dz in range(4):
            part = shares[4 * dy + dz]
            if dy and dz:
                n = [(i, j) for i in range(4) for j in range(2)]
                part = lax.ppermute(
                    part, TP, [(2 * i + j, 2 * ((i + dz) % 4) + (j ^ dy)) for i, j in n]
                )
            elif dy:
                part = shift(part, "yh", 1)
            elif dz:
                part = shift(part, "z", dz)
            received.append(part)

    first = 64 * yh + 16 * z
    by_source = [
        jnp.concatenate(
            [lax.dynamic_slice_in_dim(s, first + b * BLOCK, 16, 0) for b in range(2)], axis=0
        )
        for s in pieces
    ]
    by_source = jnp.stack(by_source)
    where_from = jnp.stack([4 * (yh ^ (t % 2)) + (z - t // 2) % 4 for t in range(8)])
    resident = jnp.transpose(by_source[where_from], (1, 0, 2)).reshape(32, D)
    refreshed = pl.pallas_call(
        finish_kernel, out_shape=jax.ShapeDtypeStruct((32, D), BF16), name="finish"
    )(resident, post_gain.reshape(1, D), *received)

    by_yl = shift(refreshed, "yl", 1)
    by_w = [refreshed, shift(refreshed, "c", 1), by_yl, shift(by_yl, "c", 1)]
    halves = [part[s * 16 : s * 16 + 16] for part in by_w for s in range(2)]

    def start_of(j):
        return jnp.sum(jnp.where(ids == j, new_start, 0))

    def for_owner(j):
        start = start_of(j)
        m = (start + (x - start) % 4) // 4
        slot = (m >= 4).astype(jnp.int32)
        source = jnp.clip(jnp.where(m < 4, m, 7 - m), 0, 3)
        return pick(2 * (source ^ w) + slot, halves)

    gathered = [for_owner(4 * x + w)]
    gathered += [shift(for_owner(4 * ((x + d) % 4) + w), "x", d) for d in range(1, 4)]
    start = start_of(p)

    def for_z(q):
        return pick((x - start - q) % 4, gathered)

    final = [for_z(z)] + [shift(for_z((z + d) % 4), "z", d) for d in range(1, 4)]
    live = z < jnp.sum(jnp.where(ids == p, new_blocks, 0))
    return jnp.concatenate(
        [jnp.where(live, pick((z - s) % 4, final), jnp.zeros((), BF16)) for s in range(4)], axis=0
    )


def solution(mesh):
    torus = Mesh(mesh.devices.reshape(4, 2, 2, 4, 2), AXES)
    in_specs = (
        P(SEQ, TP),
        P(),
        P(),
        P(),
        P(),
        P(),
        P(SEQ, TP),
        P(SEQ, TP),
        P(SEQ, TP),
        P(SEQ, TP),
    )
    out_specs = P(SEQ + TP, None)
    return jax.shard_map(
        per_device, mesh=torus, in_specs=in_specs, out_specs=out_specs, check_vma=False
    )
```

```python
import functools
import math

import jax
import jax.numpy as jnp
from jax import lax
from jax.experimental import pallas as pl
from jax.experimental.pallas import tpu as pltpu
from jax.sharding import Mesh
from jax.sharding import PartitionSpec as P

D = 4608
HEADS = 32
HEAD = 128
BLOCK = 128
EPS = 1e-06
F32 = jnp.float32
BF16 = jnp.bfloat16

AXES = ("x", "yl", "c", "z", "yh")
SEQ = ("x", "yl", "c")
TP = ("z", "yh")


SMEM = pl.BlockSpec(memory_space=pltpu.SMEM)


def shift(value, axis, by):
    n = lax.axis_size(axis)
    return lax.ppermute(value, axis, [(i, (i + by) % n) for i in range(n)])


def rope(values, cos, sin):
    half = HEAD // 2
    swapped = jnp.concatenate([values[:, half:], values[:, :half]], axis=1)
    return values * cos + swapped * sin


def spot(flat):
    me = flat[0]
    return me >> 5, (me >> 4) & 1, (me >> 3) & 1, (me >> 1) & 3, me & 1


def starts(blocks):
    result, so_far = [], jnp.int32(0)
    for m in range(16):
        result.append(so_far)
        so_far = so_far + blocks[m]
    return result


def take(index, sources, copy):
    for k, source in enumerate(sources):
        pl.when(index == k)(functools.partial(copy, source))


def leave_kernel(flat, old_blocks, order, x_old, *outs):
    x, yl, c, _, _ = spot(flat)
    shard = order[4 * x + 2 * yl + c]
    first = jnp.int32(0)
    for m in range(16):
        first = first + jnp.where(m < shard, old_blocks[m], 0)
    for d in range(4):
        row = jnp.bitwise_and(x + d - first, 3) * BLOCK
        outs[d][...] = x_old[pl.ds(pl.multiple_of(row, BLOCK), BLOCK), :]


def holders(old_blocks, order, blocks):
    begin = starts(old_blocks)
    result = []
    for block in blocks:
        shard = jnp.int32(-1)
        for m in range(16):
            shard = shard + (begin[m] <= block).astype(jnp.int32)
        holder = jnp.int32(0)
        for m in range(16):
            holder = holder + jnp.where(order[m] == shard, m, 0)
        result.append(holder)
    return result


def targets(x, yl, c):
    to = 2 * yl + c
    return [x + 4 * to, x + 28 - 4 * to]


def sort_kernel(flat, old_blocks, order, *refs):
    near, (passed, kept) = refs[:4], refs[4:]
    x, yl, c, _, _ = spot(flat)
    for core, out in ((1 - c, passed), (c, kept)):
        blocks = targets(x, yl, core) + targets(x, 1 - yl, core)
        for n, holder in enumerate(holders(old_blocks, order, blocks)):

            def copy(source, out=out, n=n):
                out[n * BLOCK : (n + 1) * BLOCK, :] = source[...]

            take(jnp.bitwise_and(x - (holder >> 2), 3), near, copy)


def merge_kernel(flat, old_blocks, order, kept, passed, mine, cross):
    x, yl, c, _, _ = spot(flat)
    blocks = targets(x, yl, c) + targets(x, 1 - yl, c)
    for n, holder in enumerate(holders(old_blocks, order, blocks)):
        out, at = (mine, n) if n < 2 else (cross, n - 2)

        def copy(source, out=out, at=at, n=n):
            out[at * BLOCK : (at + 1) * BLOCK, :] = source[n * BLOCK : (n + 1) * BLOCK, :]

        take(jnp.bitwise_xor(holder & 1, c), (kept, passed), copy)


def settle_kernel(flat, old_blocks, order, mine, crossed, rows):
    x, yl, c, _, _ = spot(flat)
    for n, holder in enumerate(holders(old_blocks, order, targets(x, yl, c))):

        def copy(source, n=n):
            rows[n * BLOCK : (n + 1) * BLOCK, :] = source[n * BLOCK : (n + 1) * BLOCK, :]

        take(jnp.bitwise_xor((holder >> 1) & 1, yl), (mine, crossed), copy)


def norm_kernel(flat, *refs):
    pieces, (gain, normed, resident) = refs[:8], refs[8:]
    _, _, _, z, yh = spot(flat)
    total = jnp.zeros((pieces[0].shape[0], 1), F32)
    for piece in pieces:
        wide = piece[...].astype(F32)
        total = total + jnp.sum(wide * wide, axis=1, keepdims=True)
    scale = lax.rsqrt(total / D + EPS)
    first = pl.multiple_of(64 * yh + 16 * z, 16)
    for n, piece in enumerate(pieces):
        t = 2 * jnp.bitwise_and(z - n % 4, 3) + jnp.bitwise_xor(yh, n // 4)
        normed[t] = (piece[...].astype(F32) * scale * gain[t]).astype(BF16)
        for block in range(2):
            source = pl.ds(pl.multiple_of(first + block * BLOCK, 16), 16)
            resident[t, block * 16 : block * 16 + 16, :] = piece[source, :]


def project_rows(normed, weight, shape):
    width = normed.shape[2]
    total = jnp.zeros(shape, F32)
    for t in range(8):
        rows = slice(t * width, (t + 1) * width)
        total = total + jnp.dot(normed[t], weight[rows, :], preferred_element_type=F32)
    return total


def key_value_kernel(normed, weight, cos, sin, kv):
    total = project_rows(normed, weight, kv.shape)
    kv[:, :HEAD] = rope(total[:, :HEAD], cos[...], sin[...]).astype(BF16)
    kv[:, HEAD:] = total[:, HEAD:].astype(BF16)


def query_kernel(normed, weight, cos, sin, query):
    total = project_rows(normed, weight, query.shape)
    for h in range(query.shape[1] // HEAD):
        cols = slice(h * HEAD, (h + 1) * HEAD)
        turned = rope(total[:, cols], cos[...], sin[...]) * (D // HEADS) ** (-0.5)
        query[:, cols] = turned.astype(BF16)


def attention_kernel(flat, query, *refs):
    kv = [refs[4 * k : 4 * k + 4] for k in range(4)]
    context, numer, denom = refs[16:]
    x, yl, c, _, _ = spot(flat)
    w = 2 * yl + c
    numer[...] = jnp.zeros_like(numer)
    denom[...] = jnp.zeros_like(denom)
    row = lax.broadcasted_iota(jnp.int32, (2 * BLOCK, BLOCK), 0) % BLOCK
    col = lax.broadcasted_iota(jnp.int32, (2 * BLOCK, BLOCK), 1)

    def chunk(dw, block, slot, masked):
        if isinstance(block, int):
            q_rows, k_rows = pl.ds(block * BLOCK, BLOCK), pl.ds(slot * BLOCK, BLOCK)
        else:
            q_rows = pl.ds(pl.multiple_of(block * BLOCK, BLOCK), BLOCK)
            k_rows = pl.ds(pl.multiple_of(slot * BLOCK, BLOCK), BLOCK)
        q2 = jnp.concatenate([query[q_rows, :HEAD], query[q_rows, HEAD:]], axis=0)
        keys = jnp.concatenate([kv[dw][d][k_rows, :HEAD] for d in range(4)], axis=0)
        values = jnp.concatenate([kv[dw][d][k_rows, HEAD:] for d in range(4)], axis=0)
        score = lax.dot_general(q2, keys, (((1,), (1,)), ((), ())), preferred_element_type=F32)
        weight = jnp.exp(50.0 * jnp.tanh(score * (1.0 / 50.0)))
        parts = [weight[:, d * BLOCK : (d + 1) * BLOCK] for d in range(4)]
        if masked:
            parts = [jnp.where(col <= row, parts[0], 0.0)] + [
                jnp.where(x >= d, parts[d], 0.0) for d in range(1, 4)
            ]
            weight = jnp.concatenate(parts, axis=1)
        denom[block] += (parts[0] + parts[1]) + (parts[2] + parts[3])
        numer[block] += jnp.dot(weight.astype(BF16), values, preferred_element_type=F32)

    chunk(0, 0, 0, True)
    chunk(0, 1, 0, False)
    chunk(0, 1, 1, True)
    for dw in range(1, 4):
        later = (jnp.bitwise_xor(w, dw) > w).astype(jnp.int32)
        chunk(dw, 1, 0, False)
        chunk(dw, later, later, False)
    for block in range(2):
        out = numer[block] / jnp.sum(denom[block], axis=1, keepdims=True)
        rows = slice(block * BLOCK, (block + 1) * BLOCK)
        context[rows, :HEAD] = out[:BLOCK].astype(BF16)
        context[rows, HEAD:] = out[BLOCK:].astype(BF16)


def out_kernel(flat, context, weight, *refs):
    outs, scratch = refs[:8], refs[8]
    _, _, _, z, yh = spot(flat)
    scratch[...] = lax.dot_general(
        context[...], weight[...], (((1,), (1,)), ((), ())), preferred_element_type=F32
    ).astype(BF16)
    for dy in range(2):
        for dz in range(4):
            first = jnp.bitwise_xor(yh, dy) * 64 + jnp.bitwise_and(z + dz, 3) * 16
            first = pl.multiple_of(first, 16)
            for block in range(2):
                outs[4 * dy + dz][block * 16 : block * 16 + 16, :] = scratch[
                    pl.ds(pl.multiple_of(first + block * BLOCK, 16), 16), :
                ]


def finish_kernel(resident, gain, *refs):
    terms, out = refs[:8], refs[8]
    total = terms[0][...].astype(F32)
    for term in terms[1:]:
        total = total + term[...].astype(F32)
    scale = lax.rsqrt(jnp.mean(total * total, axis=1, keepdims=True) + EPS)
    out[...] = (resident[...].astype(F32) + total * scale * gain[...]).astype(BF16)


def owner_kernel(flat, new_blocks, *refs):
    by_w, outs = refs[:4], refs[4:]
    x, yl, c, _, _ = spot(flat)
    w = 2 * yl + c
    for d in range(4):
        owner = 4 * jnp.bitwise_and(x + d, 3) + w
        start = jnp.int32(0)
        for m in range(16):
            start = start + jnp.where(m < owner, new_blocks[m], 0)
        level = (start + jnp.bitwise_and(x - start, 3)) >> 2
        slot = (level >= 4).astype(jnp.int32)
        source = jnp.bitwise_and(jnp.where(level < 4, level, 7 - level), 3)
        row = pl.ds(pl.multiple_of(slot * 16, 16), 16)

        def copy(part, d=d, row=row):
            outs[d][...] = part[row, :]

        take(jnp.bitwise_xor(source, w), by_w, copy)


def my_shard(flat, new_blocks):
    x, yl, c, z, _ = spot(flat)
    owner = 4 * x + 2 * yl + c
    start = jnp.int32(0)
    for m in range(16):
        start = start + jnp.where(m < owner, new_blocks[m], 0)
    return x, z, start, new_blocks[owner]


def place_kernel(flat, new_blocks, *refs):
    gathered, outs = refs[:4], refs[4:]
    x, z, start, _ = my_shard(flat, new_blocks)
    for d in range(4):

        def copy(part, d=d):
            outs[d][...] = part[...]

        take(jnp.bitwise_and(x - start - (z + d), 3), gathered, copy)


def close_kernel(flat, new_blocks, *refs):
    parts, out = refs[:4], refs[4]
    _, z, _, count = my_shard(flat, new_blocks)

    @pl.when(z >= count)
    def _():
        out[...] = jnp.zeros_like(out)

    @pl.when(z < count)
    def _():
        for d in range(4):
            row = pl.multiple_of(jnp.bitwise_and(z - d, 3) * 16, 16)
            out[pl.ds(row, 16), :] = parts[d][...]


def per_device(
    x_old, old_blocks, new_blocks, order, pre_gain, post_gain, w_query, w_key, w_value, w_out_t
):
    flat = lax.axis_index(AXES).astype(jnp.int32).reshape(1)
    width = x_old.shape[1]
    count = 2 * BLOCK

    def call(kernel, name, tables, arrays, shapes):
        results = pl.pallas_call(
            kernel,
            in_specs=[SMEM] * (1 + len(tables)) + [pl.BlockSpec()] * len(arrays),
            out_shape=[jax.ShapeDtypeStruct(s, BF16) for s in shapes],
            name=name,
        )(flat, *tables, *arrays)
        return list(results)

    qkv_local = jnp.concatenate(
        [w_key[:, :HEAD], w_value[:, :HEAD], w_key[:, HEAD:], w_value[:, HEAD:], w_query], axis=1
    )
    qkv_full = lax.all_gather(qkv_local, SEQ, axis=0, tiled=True)
    out_full = lax.all_gather(w_out_t, SEQ, axis=0, tiled=True)

    old = (old_blocks, order)
    near = call(leave_kernel, "leave", old, (x_old,), [(BLOCK, width)] * 4)
    near = near[:1] + [shift(near[d], "x", d) for d in range(1, 4)]
    passed, kept = call(sort_kernel, "sort", old, near, [(2 * count, width)] * 2)
    passed = shift(passed, "c", 1)
    mine, cross = call(merge_kernel, "merge", old, (kept, passed), [(count, width)] * 2)
    cross = shift(cross, "yl", 1)
    (rows,) = call(settle_kernel, "settle", old, (mine, cross), [(count, width)])

    with jax.named_scope("across"):
        facing = shift(rows, "yh", 1)
    with jax.named_scope("along"):
        pieces = [rows] + [shift(rows, "z", d) for d in range(1, 4)]
    with jax.named_scope("beyond"):
        pieces += [facing] + [shift(facing, "z", d) for d in range(1, 4)]

    slot_rows = jnp.arange(BLOCK, dtype=jnp.int32)
    x, w = flat[0] >> 5, (flat[0] >> 3) & 3
    positions = jnp.concatenate(
        [b * BLOCK + slot_rows for b in (x + 4 * w, x + 28 - 4 * w)]
    )
    inverse = jnp.exp(jnp.arange(HEAD // 2, dtype=F32) * (-2.0 * math.log(10000.0) / HEAD))
    angles = positions.astype(F32)[:, None] * inverse[None, :]
    cosine, sine = jnp.cos(angles), jnp.sin(angles)
    cosine = jnp.concatenate([cosine, cosine], axis=1)
    sine = jnp.concatenate([-sine, sine], axis=1)

    whole = lambda *shape: pl.BlockSpec(shape, lambda n: (0,) * len(shape))
    normed, resident = call(
        norm_kernel,
        "norm",
        (),
        (*pieces, pre_gain.reshape(8, 1, width)),
        [(8, count, width), (8, 32, width)],
    )
    kv = pl.pallas_call(
        key_value_kernel,
        grid=(2,),
        in_specs=[
            whole(8, count, width),
            pl.BlockSpec((D, 2 * HEAD), lambda n: (0, n)),
            whole(count, HEAD),
            whole(count, HEAD),
        ],
        out_specs=pl.BlockSpec((count, 2 * HEAD), lambda n: (0, n)),
        out_shape=jax.ShapeDtypeStruct((count, 4 * HEAD), BF16),
        name="key_value",
    )(normed, qkv_full, cosine, sine)

    with jax.named_scope("pair"):
        pair = shift(kv, "yl", 1)
    spread = []
    for part in (kv, pair):
        same = [part] + [shift(part, "x", d) for d in range(1, 4)]
        spread.append(same)
        spread.append([shift(s, "c", 1) for s in same])
    spread = [s for same in spread for s in same]

    query = pl.pallas_call(
        query_kernel,
        grid=(2,),
        in_specs=[
            whole(8, count, width),
            pl.BlockSpec((D, 2 * HEAD), lambda n: (0, n + 2)),
            whole(count, HEAD),
            whole(count, HEAD),
        ],
        out_specs=pl.BlockSpec((count, 2 * HEAD), lambda n: (0, n)),
        out_shape=jax.ShapeDtypeStruct((count, 4 * HEAD), BF16),
        name="query",
    )(normed, qkv_full, cosine, sine)

    by_head = pl.BlockSpec((count, 2 * HEAD), lambda n: (0, n))
    context = pl.pallas_call(
        attention_kernel,
        grid=(2,),
        in_specs=[SMEM, by_head] + [by_head] * 16,
        out_specs=by_head,
        out_shape=jax.ShapeDtypeStruct((count, 4 * HEAD), BF16),
        scratch_shapes=[pltpu.VMEM((2, 2 * BLOCK, HEAD), F32), pltpu.VMEM((2, 2 * BLOCK, HEAD), F32)],
        name="attention",
    )(flat, query, *spread)

    tile = 512
    shares = pl.pallas_call(
        out_kernel,
        grid=(D // tile,),
        in_specs=[SMEM, whole(count, 4 * HEAD), pl.BlockSpec((tile, 4 * HEAD), lambda n: (n, 0))],
        out_specs=[pl.BlockSpec((32, tile), lambda n: (0, n))] * 8,
        out_shape=[jax.ShapeDtypeStruct((32, D), BF16)] * 8,
        scratch_shapes=[pltpu.VMEM((count, tile), BF16)],
        name="project",
    )(flat, context, out_full)
    received = []
    for dy in range(2):
        for dz in range(4):
            part = shares[4 * dy + dz]
            if dy and dz:
                n = [(i, j) for i in range(4) for j in range(2)]
                part = lax.ppermute(
                    part, TP, [(2 * i + j, 2 * ((i + dz) % 4) + (j ^ dy)) for i, j in n]
                )
            elif dy:
                part = shift(part, "yh", 1)
            elif dz:
                part = shift(part, "z", dz)
            received.append(part)

    resident = jnp.transpose(resident, (1, 0, 2)).reshape(32, D)
    refreshed = pl.pallas_call(
        finish_kernel, out_shape=jax.ShapeDtypeStruct((32, D), BF16), name="finish"
    )(resident, post_gain.reshape(1, D), *received)

    by_yl = shift(refreshed, "yl", 1)
    by_w = [refreshed, shift(refreshed, "c", 1), by_yl, shift(by_yl, "c", 1)]
    new = (new_blocks,)
    slices = [(16, D)] * 4
    gathered = call(owner_kernel, "owner", new, by_w, slices)
    gathered = gathered[:1] + [shift(gathered[d], "x", d) for d in range(1, 4)]
    final = call(place_kernel, "place", new, gathered, slices)
    final = final[:1] + [shift(final[d], "z", d) for d in range(1, 4)]
    (layer_out,) = call(close_kernel, "close", new, final, [(64, D)])
    return layer_out


def solution(mesh):
    torus = Mesh(mesh.devices.reshape(4, 2, 2, 4, 2), AXES)
    in_specs = (
        P(SEQ, TP),
        P(),
        P(),
        P(),
        P(),
        P(),
        P(SEQ, TP),
        P(SEQ, TP),
        P(SEQ, TP),
        P(SEQ, TP),
    )
    out_specs = P(SEQ + TP, None)
    return jax.shard_map(
        per_device, mesh=torus, in_specs=in_specs, out_specs=out_specs, check_vma=False
    )
```

```python
import math

import jax
import jax.numpy as jnp
from jax import lax
from jax.experimental import pallas as pl
from jax.experimental.pallas import tpu as pltpu
from jax.sharding import Mesh
from jax.sharding import PartitionSpec as P

D = 4608
HEADS = 32
HEAD = 128
BLOCK = 128
EPS = 1e-06
F32 = jnp.float32
BF16 = jnp.bfloat16

AXES = ("x", "yl", "c", "z", "yh")
SEQ = ("x", "yl", "c")
TP = ("z", "yh")


SMEM = pl.BlockSpec(memory_space=pltpu.SMEM)


def shift(value, axis, by):
    n = lax.axis_size(axis)
    return lax.ppermute(value, axis, [(i, (i + by) % n) for i in range(n)])


def rope(values, cos, sin):
    half = HEAD // 2
    swapped = jnp.concatenate([values[:, half:], values[:, :half]], axis=1)
    return values * cos + swapped * sin


def spot(flat):
    me = flat[0]
    return me >> 5, (me >> 4) & 1, (me >> 3) & 1, (me >> 1) & 3, me & 1


def starts(blocks):
    result, so_far = [], jnp.int32(0)
    for m in range(16):
        result.append(so_far)
        so_far = so_far + blocks[m]
    return result


ANY = pl.BlockSpec(memory_space=pl.ANY)


def move(jobs, sems):
    for n, (index, sources, target) in enumerate(jobs):
        for k, source in enumerate(sources):
            copy = pltpu.make_async_copy(source, target, sems.at[n])
            if len(sources) == 1:
                copy.start()
            else:
                pl.when(index == k)(copy.start)
    for n, (_, sources, target) in enumerate(jobs):
        pltpu.make_async_copy(sources[0], target, sems.at[n]).wait()


def lanes(first):
    return pl.ds(pl.multiple_of(first, BLOCK), BLOCK)


def join_kernel(key, value, query, out_t, joined, sems):
    jobs, at = [], 0
    for source, first, width in (
        (key, 0, HEAD),
        (value, 0, HEAD),
        (key, HEAD, HEAD),
        (value, HEAD, HEAD),
        (query, 0, 4 * HEAD),
        (out_t, 0, 4 * HEAD),
    ):
        part = source.at[:, first : first + width]
        jobs.append((0, [part], joined.at[:, at : at + width]))
        at += width
    move(jobs, sems)


def leave_kernel(flat, old_blocks, order, x_old, *refs):
    outs, sems = refs[:4], refs[4]
    x, yl, c, _, _ = spot(flat)
    shard = order[4 * x + 2 * yl + c]
    first = jnp.int32(0)
    for m in range(16):
        first = first + jnp.where(m < shard, old_blocks[m], 0)
    jobs = []
    for d in range(4):
        row = jnp.bitwise_and(x + d - first, 3) * BLOCK
        jobs.append((0, [x_old.at[:, lanes(row)]], outs[d]))
    move(jobs, sems)


def holders(old_blocks, order, blocks):
    begin = starts(old_blocks)
    result = []
    for block in blocks:
        shard = jnp.int32(-1)
        for m in range(16):
            shard = shard + (begin[m] <= block).astype(jnp.int32)
        holder = jnp.int32(0)
        for m in range(16):
            holder = holder + jnp.where(order[m] == shard, m, 0)
        result.append(holder)
    return result


def targets(x, yl, c):
    to = 2 * yl + c
    return [x + 4 * to, x + 28 - 4 * to]


def sort_kernel(flat, old_blocks, order, *refs):
    sources, (mine, cross, sems) = refs[:8], refs[8:]
    x, yl, c, _, _ = spot(flat)
    blocks = targets(x, yl, c) + targets(x, 1 - yl, c)
    jobs = []
    for n, holder in enumerate(holders(old_blocks, order, blocks)):
        index = jnp.bitwise_and(x - (holder >> 2), 3) + 4 * jnp.bitwise_xor(holder & 1, c)
        out, at = (mine, n) if n < 2 else (cross, n - 2)
        jobs.append((index, sources, out.at[:, at * BLOCK : (at + 1) * BLOCK]))
    move(jobs, sems)


def settle_kernel(flat, old_blocks, order, mine, crossed, rows, sems):
    x, yl, c, _, _ = spot(flat)
    jobs = []
    for n, holder in enumerate(holders(old_blocks, order, targets(x, yl, c))):
        at = slice(n * BLOCK, (n + 1) * BLOCK)
        index = jnp.bitwise_xor((holder >> 1) & 1, yl)
        jobs.append((index, [mine.at[:, at], crossed.at[:, at]], rows.at[:, at]))
    move(jobs, sems)


def norm_kernel(flat, *refs):
    pieces, (gain, normed, resident, features, raw) = refs[:8], refs[8:]
    _, _, _, z, yh = spot(flat)
    width, count = pieces[0].shape
    total = jnp.zeros((1, count), F32)
    for n, piece in enumerate(pieces):
        wide = piece[...].astype(F32)
        total = total + jnp.sum(wide * wide, axis=0, keepdims=True)
        t = 2 * jnp.bitwise_and(z - n % 4, 3) + jnp.bitwise_xor(yh, n // 4)
        features[pl.ds(pl.multiple_of(t * width, 64), width), :] = piece[...]
    scale = lax.rsqrt(total / D + EPS)
    scale = jnp.transpose(jnp.broadcast_to(scale, (BLOCK, count)))
    step = 512
    for at in range(0, D, step):
        rows = jnp.transpose(features[at : at + step, :])
        raw[:, at : at + step] = rows
        for k in range(0, step, BLOCK):
            cols = slice(at + k, at + k + BLOCK)
            wide = rows[:, k : k + BLOCK].astype(F32) * scale * gain[:, cols]
            normed[:, cols] = wide.astype(BF16)
    first = pl.multiple_of(64 * yh + 16 * z, 16)
    for block in range(2):
        source = pl.ds(pl.multiple_of(first + block * BLOCK, 16), 16)
        resident[block * 16 : block * 16 + 16, :] = raw[source, :]


def key_value_kernel(normed, weight, cos, sin, kv):
    total = jnp.dot(normed[...], weight[...], preferred_element_type=F32)
    kv[:, :HEAD] = rope(total[:, :HEAD], cos[...], sin[...]).astype(BF16)
    kv[:, HEAD:] = total[:, HEAD:].astype(BF16)


def query_kernel(normed, weight, cos, sin, query):
    total = jnp.dot(normed[...], weight[...], preferred_element_type=F32)
    for h in range(query.shape[1] // HEAD):
        cols = slice(h * HEAD, (h + 1) * HEAD)
        turned = rope(total[:, cols], cos[...], sin[...]) * (D // HEADS) ** (-0.5)
        query[:, cols] = turned.astype(BF16)


def attention_kernel(flat, query, *refs):
    kv = [refs[4 * k : 4 * k + 4] for k in range(4)]
    context, numer, denom = refs[16:]
    x, yl, c, _, _ = spot(flat)
    w = 2 * yl + c
    numer[...] = jnp.zeros_like(numer)
    denom[...] = jnp.zeros_like(denom)
    row = lax.broadcasted_iota(jnp.int32, (2 * BLOCK, BLOCK), 0) % BLOCK
    col = lax.broadcasted_iota(jnp.int32, (2 * BLOCK, BLOCK), 1)

    def chunk(dw, block, slot, masked):
        if isinstance(block, int):
            q_rows, k_rows = pl.ds(block * BLOCK, BLOCK), pl.ds(slot * BLOCK, BLOCK)
        else:
            q_rows = pl.ds(pl.multiple_of(block * BLOCK, BLOCK), BLOCK)
            k_rows = pl.ds(pl.multiple_of(slot * BLOCK, BLOCK), BLOCK)
        q2 = jnp.concatenate([query[q_rows, :HEAD], query[q_rows, HEAD:]], axis=0)
        keys = jnp.concatenate([kv[dw][d][k_rows, :HEAD] for d in range(4)], axis=0)
        values = jnp.concatenate([kv[dw][d][k_rows, HEAD:] for d in range(4)], axis=0)
        score = lax.dot_general(q2, keys, (((1,), (1,)), ((), ())), preferred_element_type=F32)
        weight = jnp.exp(50.0 * jnp.tanh(score * (1.0 / 50.0)))
        parts = [weight[:, d * BLOCK : (d + 1) * BLOCK] for d in range(4)]
        if masked:
            parts = [jnp.where(col <= row, parts[0], 0.0)] + [
                jnp.where(x >= d, parts[d], 0.0) for d in range(1, 4)
            ]
            weight = jnp.concatenate(parts, axis=1)
        denom[block] += (parts[0] + parts[1]) + (parts[2] + parts[3])
        numer[block] += jnp.dot(weight.astype(BF16), values, preferred_element_type=F32)

    chunk(0, 0, 0, True)
    chunk(0, 1, 0, False)
    chunk(0, 1, 1, True)
    for dw in range(1, 4):
        later = (jnp.bitwise_xor(w, dw) > w).astype(jnp.int32)
        chunk(dw, 1, 0, False)
        chunk(dw, later, later, False)
    for block in range(2):
        out = numer[block] / jnp.sum(denom[block], axis=1, keepdims=True)
        rows = slice(block * BLOCK, (block + 1) * BLOCK)
        context[rows, :HEAD] = out[:BLOCK].astype(BF16)
        context[rows, HEAD:] = out[BLOCK:].astype(BF16)


def out_kernel(flat, context, weight, *refs):
    outs, scratch = refs[:8], refs[8]
    _, _, _, z, yh = spot(flat)
    scratch[...] = lax.dot_general(
        context[...], weight[...], (((1,), (1,)), ((), ())), preferred_element_type=F32
    ).astype(BF16)
    for dy in range(2):
        for dz in range(4):
            first = jnp.bitwise_xor(yh, dy) * 64 + jnp.bitwise_and(z + dz, 3) * 16
            first = pl.multiple_of(first, 16)
            for block in range(2):
                outs[4 * dy + dz][block * 16 : block * 16 + 16, :] = scratch[
                    pl.ds(pl.multiple_of(first + block * BLOCK, 16), 16), :
                ]


def finish_kernel(resident, gain, *refs):
    terms, out = refs[:8], refs[8]
    total = terms[0][...].astype(F32)
    for term in terms[1:]:
        total = total + term[...].astype(F32)
    scale = lax.rsqrt(jnp.mean(total * total, axis=1, keepdims=True) + EPS)
    out[...] = (resident[...].astype(F32) + total * scale * gain[...]).astype(BF16)


def before(blocks, shard):
    result = jnp.int32(0)
    for m in range(16):
        result = result + jnp.where(m < shard, blocks[m], 0)
    return result


def owner_kernel(flat, new_blocks, *refs):
    by_w, outs, sems = refs[:4], refs[4:8], refs[8]
    x, yl, c, _, _ = spot(flat)
    w = 2 * yl + c
    jobs = []
    for d in range(4):
        start = before(new_blocks, 4 * jnp.bitwise_and(x + d, 3) + w)
        level = (start + jnp.bitwise_and(x - start, 3)) >> 2
        slot = (level >= 4).astype(jnp.int32)
        source = jnp.bitwise_and(jnp.where(level < 4, level, 7 - level), 3)
        row = pl.ds(pl.multiple_of(slot * 16, 16), 16)
        jobs.append((jnp.bitwise_xor(source, w), [part.at[row, :] for part in by_w], outs[d]))
    move(jobs, sems)


def place_kernel(flat, new_blocks, *refs):
    gathered, outs, sems = refs[:4], refs[4:8], refs[8]
    x, yl, c, z, _ = spot(flat)
    start = before(new_blocks, 4 * x + 2 * yl + c)
    move(
        [(jnp.bitwise_and(x - start - (z + d), 3), gathered, outs[d]) for d in range(4)], sems
    )


def close_kernel(flat, new_blocks, *refs):
    parts, (out, zeros, sems) = refs[:4], refs[4:]
    x, yl, c, z, _ = spot(flat)
    dead = (z >= new_blocks[4 * x + 2 * yl + c]).astype(jnp.int32)
    zeros[...] = jnp.zeros_like(zeros)
    jobs = []
    for d in range(4):
        row = pl.multiple_of(jnp.bitwise_and(z - d, 3) * 16, 16)
        jobs.append((dead, [parts[d], zeros], out.at[pl.ds(row, 16), :]))
    move(jobs, sems)


def per_device(
    x_old, old_blocks, new_blocks, order, pre_gain, post_gain, w_query, w_key, w_value, w_out_t
):
    flat = lax.axis_index(AXES).astype(jnp.int32).reshape(1)
    width = x_old.shape[1]
    count = 2 * BLOCK

    def call(kernel, name, tables, arrays, shapes, copies, scratch=()):
        tables = tables and (flat, *tables)
        results = pl.pallas_call(
            kernel,
            in_specs=[SMEM] * len(tables) + [ANY] * len(arrays),
            out_specs=[ANY] * len(shapes),
            out_shape=[jax.ShapeDtypeStruct(s, BF16) for s in shapes],
            scratch_shapes=[*scratch, pltpu.SemaphoreType.DMA((copies,))],
            name=name,
        )(*tables, *arrays)
        return list(results)

    (joined,) = call(
        join_kernel, "join", (), (w_key, w_value, w_query, w_out_t), [(w_key.shape[0], 12 * HEAD)], 6
    )
    weights = lax.all_gather(joined, SEQ, axis=0, tiled=True)

    old = (old_blocks, order)
    near = call(leave_kernel, "leave", old, (x_old.T,), [(width, BLOCK)] * 4, 4)
    near = near[:1] + [shift(near[d], "x", d) for d in range(1, 4)]
    far = [shift(part, "c", 1) for part in near]
    mine, cross = call(sort_kernel, "sort", old, near + far, [(width, count)] * 2, 4)
    cross = shift(cross, "yl", 1)
    (rows,) = call(settle_kernel, "settle", old, (mine, cross), [(width, count)], 2)

    with jax.named_scope("across"):
        facing = shift(rows, "yh", 1)
    with jax.named_scope("along"):
        pieces = [rows] + [shift(rows, "z", d) for d in range(1, 4)]
    with jax.named_scope("beyond"):
        pieces += [facing] + [shift(facing, "z", d) for d in range(1, 4)]

    slot_rows = jnp.arange(BLOCK, dtype=jnp.int32)
    x, w = flat[0] >> 5, (flat[0] >> 3) & 3
    positions = jnp.concatenate(
        [b * BLOCK + slot_rows for b in (x + 4 * w, x + 28 - 4 * w)]
    )
    inverse = jnp.exp(jnp.arange(HEAD // 2, dtype=F32) * (-2.0 * math.log(10000.0) / HEAD))
    angles = positions.astype(F32)[:, None] * inverse[None, :]
    cosine, sine = jnp.cos(angles), jnp.sin(angles)
    cosine = jnp.concatenate([cosine, cosine], axis=1)
    sine = jnp.concatenate([-sine, sine], axis=1)

    whole = lambda *shape: pl.BlockSpec(shape, lambda n: (0,) * len(shape))
    normed, resident = pl.pallas_call(
        norm_kernel,
        in_specs=[SMEM] + [pl.BlockSpec()] * 9,
        out_shape=[
            jax.ShapeDtypeStruct((count, D), BF16),
            jax.ShapeDtypeStruct((32, D), BF16),
        ],
        scratch_shapes=[pltpu.VMEM((D, count), BF16), pltpu.VMEM((count, D), BF16)],
        name="norm",
    )(flat, *pieces, pre_gain.reshape(1, D))
    kv = pl.pallas_call(
        key_value_kernel,
        grid=(2,),
        in_specs=[
            whole(count, D),
            pl.BlockSpec((D, 2 * HEAD), lambda n: (0, n)),
            whole(count, HEAD),
            whole(count, HEAD),
        ],
        out_specs=pl.BlockSpec((count, 2 * HEAD), lambda n: (0, n)),
        out_shape=jax.ShapeDtypeStruct((count, 4 * HEAD), BF16),
        name="key_value",
    )(normed, weights, cosine, sine)

    with jax.named_scope("pair"):
        pair = shift(kv, "yl", 1)
    spread = []
    for part in (kv, pair):
        same = [part] + [shift(part, "x", d) for d in range(1, 4)]
        spread.append(same)
        spread.append([shift(s, "c", 1) for s in same])
    spread = [s for same in spread for s in same]

    query = pl.pallas_call(
        query_kernel,
        grid=(2,),
        in_specs=[
            whole(count, D),
            pl.BlockSpec((D, 2 * HEAD), lambda n: (0, n + 2)),
            whole(count, HEAD),
            whole(count, HEAD),
        ],
        out_specs=pl.BlockSpec((count, 2 * HEAD), lambda n: (0, n)),
        out_shape=jax.ShapeDtypeStruct((count, 4 * HEAD), BF16),
        name="query",
    )(normed, weights, cosine, sine)

    by_head = pl.BlockSpec((count, 2 * HEAD), lambda n: (0, n))
    context = pl.pallas_call(
        attention_kernel,
        grid=(2,),
        in_specs=[SMEM, by_head] + [by_head] * 16,
        out_specs=by_head,
        out_shape=jax.ShapeDtypeStruct((count, 4 * HEAD), BF16),
        scratch_shapes=[pltpu.VMEM((2, 2 * BLOCK, HEAD), F32), pltpu.VMEM((2, 2 * BLOCK, HEAD), F32)],
        name="attention",
    )(flat, query, *spread)

    tile = 512
    shares = pl.pallas_call(
        out_kernel,
        grid=(D // tile,),
        in_specs=[SMEM, whole(count, 4 * HEAD), pl.BlockSpec((tile, 4 * HEAD), lambda n: (n, 2))],
        out_specs=[pl.BlockSpec((32, tile), lambda n: (0, n))] * 8,
        out_shape=[jax.ShapeDtypeStruct((32, D), BF16)] * 8,
        scratch_shapes=[pltpu.VMEM((count, tile), BF16)],
        name="project",
    )(flat, context, weights)
    received = []
    for dy in range(2):
        for dz in range(4):
            part = shares[4 * dy + dz]
            if dy and dz:
                n = [(i, j) for i in range(4) for j in range(2)]
                part = lax.ppermute(
                    part, TP, [(2 * i + j, 2 * ((i + dz) % 4) + (j ^ dy)) for i, j in n]
                )
            elif dy:
                part = shift(part, "yh", 1)
            elif dz:
                part = shift(part, "z", dz)
            received.append(part)

    refreshed = pl.pallas_call(
        finish_kernel, out_shape=jax.ShapeDtypeStruct((32, D), BF16), name="finish"
    )(resident, post_gain.reshape(1, D), *received)

    by_yl = shift(refreshed, "yl", 1)
    by_w = [refreshed, shift(refreshed, "c", 1), by_yl, shift(by_yl, "c", 1)]
    new = (new_blocks,)
    slices = [(16, D)] * 4
    gathered = call(owner_kernel, "owner", new, by_w, slices, 4)
    gathered = gathered[:1] + [shift(gathered[d], "x", d) for d in range(1, 4)]
    final = call(place_kernel, "place", new, gathered, slices, 4)
    final = final[:1] + [shift(final[d], "z", d) for d in range(1, 4)]
    zeros = pltpu.VMEM((16, D), BF16)
    (layer_out,) = call(close_kernel, "close", new, final, [(64, D)], 4, (zeros,))
    return layer_out


def solution(mesh):
    torus = Mesh(mesh.devices.reshape(4, 2, 2, 4, 2), AXES)
    in_specs = (
        P(SEQ, TP),
        P(),
        P(),
        P(),
        P(),
        P(),
        P(SEQ, TP),
        P(SEQ, TP),
        P(SEQ, TP),
        P(SEQ, TP),
    )
    out_specs = P(SEQ + TP, None)
    return jax.shard_map(
        per_device, mesh=torus, in_specs=in_specs, out_specs=out_specs, check_vma=False
    )
```

```python
import math

import jax
import jax.numpy as jnp
from jax import lax
from jax.experimental import pallas as pl
from jax.experimental.pallas import tpu as pltpu
from jax.sharding import Mesh
from jax.sharding import PartitionSpec as P

D = 4608
HEADS = 32
HEAD = 128
BLOCK = 128
EPS = 1e-06
F32 = jnp.float32
BF16 = jnp.bfloat16

AXES = ("x", "yl", "c", "z", "yh")
SEQ = ("x", "yl", "c")
TP = ("z", "yh")


SMEM = pl.BlockSpec(memory_space=pltpu.SMEM)


def shift(value, axis, by):
    n = lax.axis_size(axis)
    return lax.ppermute(value, axis, [(i, (i + by) % n) for i in range(n)])


def rope(values, cos, sin):
    half = HEAD // 2
    swapped = jnp.concatenate([values[:, half:], values[:, :half]], axis=1)
    return values * cos + swapped * sin


def spot(flat):
    me = flat[0]
    return me >> 5, (me >> 4) & 1, (me >> 3) & 1, (me >> 1) & 3, me & 1


def starts(blocks):
    result, so_far = [], jnp.int32(0)
    for m in range(16):
        result.append(so_far)
        so_far = so_far + blocks[m]
    return result


VMEM = pl.BlockSpec(memory_space=pltpu.VMEM)


def grant(mib):
    return pltpu.CompilerParams(vmem_limit_bytes=mib << 20)


def move(jobs):
    for index, sources, target in jobs:
        for k, source in enumerate(sources):

            def copy(source=source, target=target):
                target[...] = source[...]

            if len(sources) == 1:
                copy()
            else:
                pl.when(index == k)(copy)


def lanes(first):
    return pl.ds(pl.multiple_of(first, BLOCK), BLOCK)


def join_kernel(key, value, query, out_t, joined):
    jobs, at = [], 0
    for source, first, width in (
        (key, 0, HEAD),
        (value, 0, HEAD),
        (key, HEAD, HEAD),
        (value, HEAD, HEAD),
        (query, 0, 4 * HEAD),
        (out_t, 0, 4 * HEAD),
    ):
        part = source.at[:, first : first + width]
        jobs.append((0, [part], joined.at[:, at : at + width]))
        at += width
    move(jobs)


def leave_kernel(flat, old_blocks, order, x_old, *refs):
    outs = refs
    x, yl, c, _, _ = spot(flat)
    shard = order[4 * x + 2 * yl + c]
    first = jnp.int32(0)
    for m in range(16):
        first = first + jnp.where(m < shard, old_blocks[m], 0)
    jobs = []
    for d in range(4):
        row = jnp.bitwise_and(x + d - first, 3) * BLOCK
        jobs.append((0, [x_old.at[:, lanes(row)]], outs[d]))
    move(jobs)


def holders(old_blocks, order, blocks):
    begin = starts(old_blocks)
    result = []
    for block in blocks:
        shard = jnp.int32(-1)
        for m in range(16):
            shard = shard + (begin[m] <= block).astype(jnp.int32)
        holder = jnp.int32(0)
        for m in range(16):
            holder = holder + jnp.where(order[m] == shard, m, 0)
        result.append(holder)
    return result


def targets(x, yl, c):
    to = 2 * yl + c
    return [x + 4 * to, x + 28 - 4 * to]


def sort_kernel(flat, old_blocks, order, *refs):
    sources, (mine, cross) = refs[:8], refs[8:]
    x, yl, c, _, _ = spot(flat)
    blocks = targets(x, yl, c) + targets(x, 1 - yl, c)
    jobs = []
    for n, holder in enumerate(holders(old_blocks, order, blocks)):
        index = jnp.bitwise_and(x - (holder >> 2), 3) + 4 * jnp.bitwise_xor(holder & 1, c)
        out, at = (mine, n) if n < 2 else (cross, n - 2)
        jobs.append((index, sources, out.at[:, at * BLOCK : (at + 1) * BLOCK]))
    move(jobs)


def settle_kernel(flat, old_blocks, order, mine, crossed, rows):
    x, yl, c, _, _ = spot(flat)
    jobs = []
    for n, holder in enumerate(holders(old_blocks, order, targets(x, yl, c))):
        at = slice(n * BLOCK, (n + 1) * BLOCK)
        index = jnp.bitwise_xor((holder >> 1) & 1, yl)
        jobs.append((index, [mine.at[:, at], crossed.at[:, at]], rows.at[:, at]))
    move(jobs)


def norm_kernel(flat, *refs):
    pieces, (gain, normed, resident, features, raw) = refs[:8], refs[8:]
    _, _, _, z, yh = spot(flat)
    width, count = pieces[0].shape
    total = jnp.zeros((1, count), F32)
    for n, piece in enumerate(pieces):
        wide = piece[...].astype(F32)
        total = total + jnp.sum(wide * wide, axis=0, keepdims=True)
        t = 2 * jnp.bitwise_and(z - n % 4, 3) + jnp.bitwise_xor(yh, n // 4)
        features[pl.ds(pl.multiple_of(t * width, 64), width), :] = piece[...]
    scale = lax.rsqrt(total / D + EPS)
    scale = jnp.transpose(jnp.broadcast_to(scale, (BLOCK, count)))
    step = 512
    for at in range(0, D, step):
        rows = jnp.transpose(features[at : at + step, :])
        raw[:, at : at + step] = rows
        for k in range(0, step, BLOCK):
            cols = slice(at + k, at + k + BLOCK)
            wide = rows[:, k : k + BLOCK].astype(F32) * scale * gain[:, cols]
            normed[:, cols] = wide.astype(BF16)
    first = pl.multiple_of(64 * yh + 16 * z, 16)
    for block in range(2):
        source = pl.ds(pl.multiple_of(first + block * BLOCK, 16), 16)
        resident[block * 16 : block * 16 + 16, :] = raw[source, :]


def key_value_kernel(normed, weight, cos, sin, kv):
    total = jnp.dot(normed[...], weight[...], preferred_element_type=F32)
    at = pl.multiple_of(pl.program_id(0) * 2 * HEAD, 2 * HEAD)
    kv[:, pl.ds(at, HEAD)] = rope(total[:, :HEAD], cos[...], sin[...]).astype(BF16)
    kv[:, pl.ds(at + HEAD, HEAD)] = total[:, HEAD:].astype(BF16)


def query_kernel(normed, weight, cos, sin, query):
    total = jnp.dot(normed[...], weight[...], preferred_element_type=F32)
    at = pl.multiple_of(pl.program_id(0) * 2 * HEAD, 2 * HEAD)
    for h in range(2):
        part = total[:, h * HEAD : (h + 1) * HEAD]
        turned = rope(part, cos[...], sin[...]) * (D // HEADS) ** (-0.5)
        query[:, pl.ds(at + h * HEAD, HEAD)] = turned.astype(BF16)


def attention_kernel(flat, query, *refs):
    kv = [refs[4 * k : 4 * k + 4] for k in range(4)]
    context, numer, denom = refs[16:]
    x, yl, c, _, _ = spot(flat)
    w = 2 * yl + c
    row = lax.broadcasted_iota(jnp.int32, (2 * BLOCK, BLOCK), 0) % BLOCK
    col = lax.broadcasted_iota(jnp.int32, (2 * BLOCK, BLOCK), 1)

    def chunk(first, dw, block, slot, masked):
        near, far = pl.ds(first, HEAD), pl.ds(first + HEAD, HEAD)
        if isinstance(block, int):
            q_rows, k_rows = pl.ds(block * BLOCK, BLOCK), pl.ds(slot * BLOCK, BLOCK)
        else:
            q_rows = pl.ds(pl.multiple_of(block * BLOCK, BLOCK), BLOCK)
            k_rows = pl.ds(pl.multiple_of(slot * BLOCK, BLOCK), BLOCK)
        q2 = jnp.concatenate([query[q_rows, near], query[q_rows, far]], axis=0)
        keys = jnp.concatenate([kv[dw][d][k_rows, near] for d in range(4)], axis=0)
        values = jnp.concatenate([kv[dw][d][k_rows, far] for d in range(4)], axis=0)
        score = lax.dot_general(q2, keys, (((1,), (1,)), ((), ())), preferred_element_type=F32)
        weight = jnp.exp(50.0 * jnp.tanh(score * (1.0 / 50.0)))
        parts = [weight[:, d * BLOCK : (d + 1) * BLOCK] for d in range(4)]
        if masked:
            parts = [jnp.where(col <= row, parts[0], 0.0)] + [
                jnp.where(x >= d, parts[d], 0.0) for d in range(1, 4)
            ]
            weight = jnp.concatenate(parts, axis=1)
        denom[block] += (parts[0] + parts[1]) + (parts[2] + parts[3])
        numer[block] += jnp.dot(weight.astype(BF16), values, preferred_element_type=F32)

    @pl.loop(0, 2)
    def _(head):
        first = pl.multiple_of(head * 2 * HEAD, 2 * HEAD)
        numer[...] = jnp.zeros_like(numer)
        denom[...] = jnp.zeros_like(denom)
        chunk(first, 0, 0, 0, True)
        chunk(first, 0, 1, 0, False)
        chunk(first, 0, 1, 1, True)
        for dw in range(1, 4):
            later = (jnp.bitwise_xor(w, dw) > w).astype(jnp.int32)
            chunk(first, dw, 1, 0, False)
            chunk(first, dw, later, later, False)
        for block in range(2):
            out = numer[block] / jnp.sum(denom[block], axis=1, keepdims=True)
            rows = slice(block * BLOCK, (block + 1) * BLOCK)
            context[rows, pl.ds(first, HEAD)] = out[:BLOCK].astype(BF16)
            context[rows, pl.ds(first + HEAD, HEAD)] = out[BLOCK:].astype(BF16)


def out_kernel(flat, context, weight, *refs):
    outs, scratch = refs[:8], refs[8]
    _, _, _, z, yh = spot(flat)
    scratch[...] = lax.dot_general(
        context[...], weight[...], (((1,), (1,)), ((), ())), preferred_element_type=F32
    ).astype(BF16)
    tile = scratch.shape[1]
    cols = pl.ds(pl.multiple_of(pl.program_id(0) * tile, tile), tile)
    for dy in range(2):
        for dz in range(4):
            first = jnp.bitwise_xor(yh, dy) * 64 + jnp.bitwise_and(z + dz, 3) * 16
            first = pl.multiple_of(first, 16)
            for block in range(2):
                outs[4 * dy + dz][block * 16 : block * 16 + 16, cols] = scratch[
                    pl.ds(pl.multiple_of(first + block * BLOCK, 16), 16), :
                ]


def finish_kernel(resident, gain, *refs):
    terms, out = refs[:8], refs[8]
    total = terms[0][...].astype(F32)
    for term in terms[1:]:
        total = total + term[...].astype(F32)
    scale = lax.rsqrt(jnp.mean(total * total, axis=1, keepdims=True) + EPS)
    out[...] = (resident[...].astype(F32) + total * scale * gain[...]).astype(BF16)


def before(blocks, shard):
    result = jnp.int32(0)
    for m in range(16):
        result = result + jnp.where(m < shard, blocks[m], 0)
    return result


def owner_kernel(flat, new_blocks, *refs):
    by_w, outs = refs[:4], refs[4:]
    x, yl, c, _, _ = spot(flat)
    w = 2 * yl + c
    jobs = []
    for d in range(4):
        start = before(new_blocks, 4 * jnp.bitwise_and(x + d, 3) + w)
        level = (start + jnp.bitwise_and(x - start, 3)) >> 2
        slot = (level >= 4).astype(jnp.int32)
        source = jnp.bitwise_and(jnp.where(level < 4, level, 7 - level), 3)
        row = pl.ds(pl.multiple_of(slot * 16, 16), 16)
        jobs.append((jnp.bitwise_xor(source, w), [part.at[row, :] for part in by_w], outs[d]))
    move(jobs)


def place_kernel(flat, new_blocks, *refs):
    gathered, outs = refs[:4], refs[4:]
    x, yl, c, z, _ = spot(flat)
    start = before(new_blocks, 4 * x + 2 * yl + c)
    move([(jnp.bitwise_and(x - start - (z + d), 3), gathered, outs[d]) for d in range(4)])


def close_kernel(flat, new_blocks, *refs):
    parts, out = refs[:4], refs[4]
    x, yl, c, z, _ = spot(flat)
    count = new_blocks[4 * x + 2 * yl + c]

    @pl.when(z >= count)
    def _():
        out[...] = jnp.zeros_like(out)

    @pl.when(z < count)
    def _():
        for d in range(4):
            row = pl.multiple_of(jnp.bitwise_and(z - d, 3) * 16, 16)
            out[pl.ds(row, 16), :] = parts[d][...]


def per_device(
    x_old, old_blocks, new_blocks, order, pre_gain, post_gain, w_query, w_key, w_value, w_out_t
):
    flat = lax.axis_index(AXES).astype(jnp.int32).reshape(1)
    width = x_old.shape[1]
    count = 2 * BLOCK

    def call(kernel, name, tables, arrays, shapes, here=True):
        tables = tables and (flat, *tables)
        if here:
            arrays = [pltpu.with_memory_space_constraint(a, pltpu.VMEM) for a in arrays]
        kind = pltpu.VMEM if here else jax.ShapeDtypeStruct
        results = pl.pallas_call(
            kernel,
            in_specs=[SMEM] * len(tables) + [VMEM] * len(arrays),
            out_specs=[VMEM] * len(shapes),
            out_shape=[kind(s, BF16) for s in shapes],
            compiler_params=grant(8),
            name=name,
        )(*tables, *arrays)
        return list(results)

    (joined,) = call(
        join_kernel, "join", (), (w_key, w_value, w_query, w_out_t), [(w_key.shape[0], 12 * HEAD)], False
    )
    weights = lax.all_gather(joined, SEQ, axis=0, tiled=True)

    old = (old_blocks, order)
    near = call(leave_kernel, "leave", old, (x_old.T,), [(width, BLOCK)] * 4)
    near = near[:1] + [shift(near[d], "x", d) for d in range(1, 4)]
    far = [shift(part, "c", 1) for part in near]
    mine, cross = call(sort_kernel, "sort", old, near + far, [(width, count)] * 2)
    cross = shift(cross, "yl", 1)
    (rows,) = call(settle_kernel, "settle", old, (mine, cross), [(width, count)])

    with jax.named_scope("across"):
        facing = shift(rows, "yh", 1)
    with jax.named_scope("along"):
        pieces = [rows] + [shift(rows, "z", d) for d in range(1, 4)]
    with jax.named_scope("beyond"):
        pieces += [facing] + [shift(facing, "z", d) for d in range(1, 4)]

    slot_rows = jnp.arange(BLOCK, dtype=jnp.int32)
    x, w = flat[0] >> 5, (flat[0] >> 3) & 3
    positions = jnp.concatenate(
        [b * BLOCK + slot_rows for b in (x + 4 * w, x + 28 - 4 * w)]
    )
    inverse = jnp.exp(jnp.arange(HEAD // 2, dtype=F32) * (-2.0 * math.log(10000.0) / HEAD))
    angles = positions.astype(F32)[:, None] * inverse[None, :]
    cosine, sine = jnp.cos(angles), jnp.sin(angles)
    cosine = jnp.concatenate([cosine, cosine], axis=1)
    sine = jnp.concatenate([-sine, sine], axis=1)

    def near_by(arrays):
        return [pltpu.with_memory_space_constraint(a, pltpu.VMEM) for a in arrays]

    normed, resident = pl.pallas_call(
        norm_kernel,
        in_specs=[SMEM] + [VMEM] * 9,
        out_specs=[VMEM] * 2,
        out_shape=[pltpu.VMEM((count, D), BF16), pltpu.VMEM((32, D), BF16)],
        scratch_shapes=[pltpu.VMEM((D, count), BF16), pltpu.VMEM((count, D), BF16)],
        compiler_params=grant(24),
        name="norm",
    )(flat, *near_by(pieces), pre_gain.reshape(1, D))
    tables = near_by((cosine, sine))

    def heads(kernel, name, first):
        return pl.pallas_call(
            kernel,
            grid=(2,),
            in_specs=[VMEM, pl.BlockSpec((D, 2 * HEAD), lambda n: (0, n + first)), VMEM, VMEM],
            out_specs=VMEM,
            out_shape=pltpu.VMEM((count, 4 * HEAD), BF16),
            compiler_params=grant(24),
            name=name,
        )(*near_by((normed,)), weights, *tables)

    kv = heads(key_value_kernel, "key_value", 0)

    with jax.named_scope("pair"):
        pair = shift(kv, "yl", 1)
    spread = []
    for part in (kv, pair):
        same = [part] + [shift(part, "x", d) for d in range(1, 4)]
        spread.append(same)
        spread.append([shift(s, "c", 1) for s in same])
    spread = [s for same in spread for s in same]

    query = heads(query_kernel, "query", 2)
    context = pl.pallas_call(
        attention_kernel,
        in_specs=[SMEM] + [VMEM] * 17,
        out_specs=VMEM,
        out_shape=pltpu.VMEM((count, 4 * HEAD), BF16),
        scratch_shapes=[pltpu.VMEM((2, 2 * BLOCK, HEAD), F32), pltpu.VMEM((2, 2 * BLOCK, HEAD), F32)],
        compiler_params=grant(24),
        name="attention",
    )(flat, *near_by((query, *spread)))

    tile = 512
    shares = pl.pallas_call(
        out_kernel,
        grid=(D // tile,),
        in_specs=[SMEM, VMEM, pl.BlockSpec((tile, 4 * HEAD), lambda n: (n, 2))],
        out_specs=[VMEM] * 8,
        out_shape=[pltpu.VMEM((32, D), BF16)] * 8,
        scratch_shapes=[pltpu.VMEM((count, tile), BF16)],
        compiler_params=grant(16),
        name="project",
    )(flat, *near_by((context,)), weights)
    received = []
    for dy in range(2):
        for dz in range(4):
            part = shares[4 * dy + dz]
            if dy and dz:
                n = [(i, j) for i in range(4) for j in range(2)]
                part = lax.ppermute(
                    part, TP, [(2 * i + j, 2 * ((i + dz) % 4) + (j ^ dy)) for i, j in n]
                )
            elif dy:
                part = shift(part, "yh", 1)
            elif dz:
                part = shift(part, "z", dz)
            received.append(part)

    refreshed = pl.pallas_call(
        finish_kernel,
        in_specs=[VMEM] * 10,
        out_specs=VMEM,
        out_shape=pltpu.VMEM((32, D), BF16),
        compiler_params=grant(8),
        name="finish",
    )(*near_by((resident, post_gain.reshape(1, D), *received)))

    by_yl = shift(refreshed, "yl", 1)
    by_w = [refreshed, shift(refreshed, "c", 1), by_yl, shift(by_yl, "c", 1)]
    new = (new_blocks,)
    slices = [(16, D)] * 4
    gathered = call(owner_kernel, "owner", new, by_w, slices)
    gathered = gathered[:1] + [shift(gathered[d], "x", d) for d in range(1, 4)]
    final = call(place_kernel, "place", new, gathered, slices)
    final = final[:1] + [shift(final[d], "z", d) for d in range(1, 4)]
    (layer_out,) = call(close_kernel, "close", new, final, [(64, D)])
    return layer_out


def solution(mesh):
    torus = Mesh(mesh.devices.reshape(4, 2, 2, 4, 2), AXES)
    in_specs = (
        P(SEQ, TP),
        P(),
        P(),
        P(),
        P(),
        P(),
        P(SEQ, TP),
        P(SEQ, TP),
        P(SEQ, TP),
        P(SEQ, TP),
    )
    out_specs = P(SEQ + TP, None)
    return jax.shard_map(
        per_device, mesh=torus, in_specs=in_specs, out_specs=out_specs, check_vma=False
    )
```

```python
import math

import jax
import jax.numpy as jnp
from jax import lax
from jax.experimental import pallas as pl
from jax.experimental.pallas import tpu as pltpu
from jax.sharding import Mesh
from jax.sharding import PartitionSpec as P

D = 4608
HEADS = 32
HEAD = 128
BLOCK = 128
EPS = 1e-06
F32 = jnp.float32
BF16 = jnp.bfloat16

AXES = ("x", "yl", "c", "z", "yh")
SEQ = ("x", "yl", "c")
TP = ("z", "yh")


SMEM = pl.BlockSpec(memory_space=pltpu.SMEM)


def shift(value, axis, by):
    n = lax.axis_size(axis)
    return lax.ppermute(value, axis, [(i, (i + by) % n) for i in range(n)])


def rope(values, cos, sin):
    half = HEAD // 2
    swapped = jnp.concatenate([values[:, half:], values[:, :half]], axis=1)
    return values * cos + swapped * sin


def spot(flat):
    me = flat[0]
    return me >> 5, (me >> 4) & 1, (me >> 3) & 1, (me >> 1) & 3, me & 1


def starts(blocks):
    result, so_far = [], jnp.int32(0)
    for m in range(16):
        result.append(so_far)
        so_far = so_far + blocks[m]
    return result


VMEM = pl.BlockSpec(memory_space=pltpu.VMEM)


def grant(mib):
    return pltpu.CompilerParams(vmem_limit_bytes=mib << 20)


def move(jobs):
    for index, sources, target in jobs:
        for k, source in enumerate(sources):

            def copy(source=source, target=target):
                target[...] = source[...]

            if len(sources) == 1:
                copy()
            else:
                pl.when(index == k)(copy)


def lanes(first):
    return pl.ds(pl.multiple_of(first, BLOCK), BLOCK)


def fetch(jobs, sems):
    copies = [pltpu.make_async_copy(s, t, sems.at[n]) for n, (s, t) in enumerate(jobs)]
    for copy in copies:
        copy.start()
    for copy in copies:
        copy.wait()


def join_kernel(key, value, query, joined, sems):
    jobs, at = [], 0
    for source, first, width in (
        (key, 0, HEAD),
        (value, 0, HEAD),
        (key, HEAD, HEAD),
        (value, HEAD, HEAD),
        (query, 0, 4 * HEAD),
    ):
        jobs.append((source.at[:, first : first + width], joined.at[:, at : at + width]))
        at += width
    fetch(jobs, sems)


def leave_kernel(flat, old_blocks, order, x_old, *refs):
    outs, sems = refs[:4], refs[4]
    x, yl, c, _, _ = spot(flat)
    shard = order[4 * x + 2 * yl + c]
    first = jnp.int32(0)
    for m in range(16):
        first = first + jnp.where(m < shard, old_blocks[m], 0)
    jobs = []
    for d in range(4):
        row = jnp.bitwise_and(x + d - first, 3) * BLOCK
        jobs.append((x_old.at[:, lanes(row)], outs[d]))
    fetch(jobs, sems)


def holders(old_blocks, order, blocks):
    begin = starts(old_blocks)
    result = []
    for block in blocks:
        shard = jnp.int32(-1)
        for m in range(16):
            shard = shard + (begin[m] <= block).astype(jnp.int32)
        holder = jnp.int32(0)
        for m in range(16):
            holder = holder + jnp.where(order[m] == shard, m, 0)
        result.append(holder)
    return result


def targets(x, yl, c):
    to = 2 * yl + c
    return [x + 4 * to, x + 28 - 4 * to]


def sort_kernel(flat, old_blocks, order, *refs):
    sources, (mine, cross) = refs[:8], refs[8:]
    x, yl, c, _, _ = spot(flat)
    blocks = targets(x, yl, c) + targets(x, 1 - yl, c)
    jobs = []
    for n, holder in enumerate(holders(old_blocks, order, blocks)):
        index = jnp.bitwise_and(x - (holder >> 2), 3) + 4 * jnp.bitwise_xor(holder & 1, c)
        out, at = (mine, n) if n < 2 else (cross, n - 2)
        jobs.append((index, sources, out.at[:, at * BLOCK : (at + 1) * BLOCK]))
    move(jobs)


def settle_kernel(flat, old_blocks, order, mine, crossed, rows):
    x, yl, c, _, _ = spot(flat)
    jobs = []
    for n, holder in enumerate(holders(old_blocks, order, targets(x, yl, c))):
        at = slice(n * BLOCK, (n + 1) * BLOCK)
        index = jnp.bitwise_xor((holder >> 1) & 1, yl)
        jobs.append((index, [mine.at[:, at], crossed.at[:, at]], rows.at[:, at]))
    move(jobs)


def norm_kernel(flat, *refs):
    pieces, (gain, normed, resident, features, raw) = refs[:8], refs[8:]
    _, _, _, z, yh = spot(flat)
    width, count = pieces[0].shape
    total = jnp.zeros((1, count), F32)
    for n, piece in enumerate(pieces):
        wide = piece[...].astype(F32)
        total = total + jnp.sum(wide * wide, axis=0, keepdims=True)
        t = 2 * jnp.bitwise_and(z - n % 4, 3) + jnp.bitwise_xor(yh, n // 4)
        features[pl.ds(pl.multiple_of(t * width, 64), width), :] = piece[...]
    scale = lax.rsqrt(total / D + EPS)
    scale = jnp.transpose(jnp.broadcast_to(scale, (BLOCK, count)))
    step = 512
    for at in range(0, D, step):
        rows = jnp.transpose(features[at : at + step, :])
        raw[:, at : at + step] = rows
        for k in range(0, step, BLOCK):
            cols = slice(at + k, at + k + BLOCK)
            wide = rows[:, k : k + BLOCK].astype(F32) * scale * gain[:, cols]
            normed[:, cols] = wide.astype(BF16)
    first = pl.multiple_of(64 * yh + 16 * z, 16)
    for block in range(2):
        source = pl.ds(pl.multiple_of(first + block * BLOCK, 16), 16)
        resident[block * 16 : block * 16 + 16, :] = raw[source, :]


def key_value_kernel(normed, weight, cos, sin, kv):
    total = jnp.dot(normed[...], weight[...], preferred_element_type=F32)
    at = pl.multiple_of(pl.program_id(0) * 2 * HEAD, 2 * HEAD)
    kv[:, pl.ds(at, HEAD)] = rope(total[:, :HEAD], cos[...], sin[...]).astype(BF16)
    kv[:, pl.ds(at + HEAD, HEAD)] = total[:, HEAD:].astype(BF16)


def query_kernel(normed, weight, cos, sin, query):
    total = jnp.dot(normed[...], weight[...], preferred_element_type=F32)
    at = pl.multiple_of(pl.program_id(0) * 2 * HEAD, 2 * HEAD)
    for h in range(2):
        part = total[:, h * HEAD : (h + 1) * HEAD]
        turned = rope(part, cos[...], sin[...]) * (D // HEADS) ** (-0.5)
        query[:, pl.ds(at + h * HEAD, HEAD)] = turned.astype(BF16)


def attention_kernel(flat, query, *refs):
    kv = [refs[4 * k : 4 * k + 4] for k in range(4)]
    context, numer, denom = refs[16:]
    x, yl, c, _, _ = spot(flat)
    w = 2 * yl + c
    row = lax.broadcasted_iota(jnp.int32, (2 * BLOCK, BLOCK), 0) % BLOCK
    col = lax.broadcasted_iota(jnp.int32, (2 * BLOCK, BLOCK), 1)

    def chunk(first, dw, block, slot, masked):
        near, far = pl.ds(first, HEAD), pl.ds(first + HEAD, HEAD)
        if isinstance(block, int):
            q_rows, k_rows = pl.ds(block * BLOCK, BLOCK), pl.ds(slot * BLOCK, BLOCK)
        else:
            q_rows = pl.ds(pl.multiple_of(block * BLOCK, BLOCK), BLOCK)
            k_rows = pl.ds(pl.multiple_of(slot * BLOCK, BLOCK), BLOCK)
        q2 = jnp.concatenate([query[q_rows, near], query[q_rows, far]], axis=0)
        keys = jnp.concatenate([kv[dw][d][k_rows, near] for d in range(4)], axis=0)
        values = jnp.concatenate([kv[dw][d][k_rows, far] for d in range(4)], axis=0)
        score = lax.dot_general(q2, keys, (((1,), (1,)), ((), ())), preferred_element_type=F32)
        weight = jnp.exp(50.0 * jnp.tanh(score * (1.0 / 50.0)))
        parts = [weight[:, d * BLOCK : (d + 1) * BLOCK] for d in range(4)]
        if masked:
            parts = [jnp.where(col <= row, parts[0], 0.0)] + [
                jnp.where(x >= d, parts[d], 0.0) for d in range(1, 4)
            ]
            weight = jnp.concatenate(parts, axis=1)
        denom[block] += (parts[0] + parts[1]) + (parts[2] + parts[3])
        numer[block] += jnp.dot(weight.astype(BF16), values, preferred_element_type=F32)

    @pl.loop(0, 2)
    def _(head):
        first = pl.multiple_of(head * 2 * HEAD, 2 * HEAD)
        numer[...] = jnp.zeros_like(numer)
        denom[...] = jnp.zeros_like(denom)
        chunk(first, 0, 0, 0, True)
        chunk(first, 0, 1, 0, False)
        chunk(first, 0, 1, 1, True)
        for dw in range(1, 4):
            later = (jnp.bitwise_xor(w, dw) > w).astype(jnp.int32)
            chunk(first, dw, 1, 0, False)
            chunk(first, dw, later, later, False)
        for block in range(2):
            out = numer[block] / jnp.sum(denom[block], axis=1, keepdims=True)
            rows = slice(block * BLOCK, (block + 1) * BLOCK)
            context[rows, pl.ds(first, HEAD)] = out[:BLOCK].astype(BF16)
            context[rows, pl.ds(first + HEAD, HEAD)] = out[BLOCK:].astype(BF16)


def out_kernel(flat, context, weight, *refs):
    outs, scratch = refs[:8], refs[8]
    _, _, _, z, yh = spot(flat)
    scratch[...] = lax.dot_general(
        context[...], weight[...], (((1,), (1,)), ((), ())), preferred_element_type=F32
    ).astype(BF16)
    tile = scratch.shape[1]
    cols = pl.ds(pl.multiple_of(pl.program_id(0) * tile, tile), tile)
    for dy in range(2):
        for dz in range(4):
            first = jnp.bitwise_xor(yh, dy) * 64 + jnp.bitwise_and(z + dz, 3) * 16
            first = pl.multiple_of(first, 16)
            for block in range(2):
                outs[4 * dy + dz][block * 16 : block * 16 + 16, cols] = scratch[
                    pl.ds(pl.multiple_of(first + block * BLOCK, 16), 16), :
                ]


def finish_kernel(resident, gain, *refs):
    terms, out = refs[:8], refs[8]
    total = terms[0][...].astype(F32)
    for term in terms[1:]:
        total = total + term[...].astype(F32)
    scale = lax.rsqrt(jnp.mean(total * total, axis=1, keepdims=True) + EPS)
    out[...] = (resident[...].astype(F32) + total * scale * gain[...]).astype(BF16)


def before(blocks, shard):
    result = jnp.int32(0)
    for m in range(16):
        result = result + jnp.where(m < shard, blocks[m], 0)
    return result


def owner_kernel(flat, new_blocks, *refs):
    by_w, outs = refs[:4], refs[4:]
    x, yl, c, _, _ = spot(flat)
    w = 2 * yl + c
    jobs = []
    for d in range(4):
        start = before(new_blocks, 4 * jnp.bitwise_and(x + d, 3) + w)
        level = (start + jnp.bitwise_and(x - start, 3)) >> 2
        slot = (level >= 4).astype(jnp.int32)
        source = jnp.bitwise_and(jnp.where(level < 4, level, 7 - level), 3)
        row = pl.ds(pl.multiple_of(slot * 16, 16), 16)
        jobs.append((jnp.bitwise_xor(source, w), [part.at[row, :] for part in by_w], outs[d]))
    move(jobs)


def place_kernel(flat, new_blocks, *refs):
    gathered, outs = refs[:4], refs[4:]
    x, yl, c, z, _ = spot(flat)
    start = before(new_blocks, 4 * x + 2 * yl + c)
    move([(jnp.bitwise_and(x - start - (z + d), 3), gathered, outs[d]) for d in range(4)])


def close_kernel(flat, new_blocks, *refs):
    parts, out = refs[:4], refs[4]
    x, yl, c, z, _ = spot(flat)
    count = new_blocks[4 * x + 2 * yl + c]

    @pl.when(z >= count)
    def _():
        out[...] = jnp.zeros_like(out)

    @pl.when(z < count)
    def _():
        for d in range(4):
            row = pl.multiple_of(jnp.bitwise_and(z - d, 3) * 16, 16)
            out[pl.ds(row, 16), :] = parts[d][...]


def per_device(
    x_old, old_blocks, new_blocks, order, pre_gain, post_gain, w_query, w_key, w_value, w_out_t
):
    flat = lax.axis_index(AXES).astype(jnp.int32).reshape(1)
    width = x_old.shape[1]
    count = 2 * BLOCK

    def near_by(arrays):
        return [pltpu.with_memory_space_constraint(a, pltpu.VMEM) for a in arrays]

    def far_off(arrays):
        return [pltpu.with_memory_space_constraint(a, pltpu.HBM) for a in arrays]

    def call(kernel, name, tables, arrays, shapes):
        results = pl.pallas_call(
            kernel,
            in_specs=[SMEM] * (1 + len(tables)) + [VMEM] * len(arrays),
            out_specs=[VMEM] * len(shapes),
            out_shape=[pltpu.VMEM(s, BF16) for s in shapes],
            compiler_params=grant(8),
            name=name,
        )(flat, *tables, *near_by(arrays))
        return list(results)

    def bring(kernel, name, tables, arrays, shapes, copies, kind):
        results = pl.pallas_call(
            kernel,
            in_specs=[SMEM] * len(tables) + [pl.BlockSpec(memory_space=pl.ANY)] * len(arrays),
            out_specs=[VMEM] * len(shapes),
            out_shape=[kind(s, BF16) for s in shapes],
            scratch_shapes=[pltpu.SemaphoreType.DMA((copies,))],
            compiler_params=grant(8),
            name=name,
        )(*tables, *far_off(arrays))
        return list(results)

    (joined,) = bring(
        join_kernel,
        "join",
        (),
        (w_key, w_value, w_query),
        [(w_key.shape[0], 8 * HEAD)],
        5,
        jax.ShapeDtypeStruct,
    )
    qkv_full = lax.all_gather(joined, SEQ, axis=0, tiled=True)
    out_full = lax.all_gather(w_out_t, SEQ, axis=0, tiled=True)

    old = far_off((old_blocks, order))
    near = bring(
        leave_kernel, "leave", (flat, *old), (x_old.T,), [(width, BLOCK)] * 4, 4, pltpu.VMEM
    )
    near = near[:1] + [shift(near[d], "x", d) for d in range(1, 4)]
    far = [shift(part, "c", 1) for part in near]
    mine, cross = call(sort_kernel, "sort", old, near + far, [(width, count)] * 2)
    cross = shift(cross, "yl", 1)
    (rows,) = call(settle_kernel, "settle", old, (mine, cross), [(width, count)])

    with jax.named_scope("across"):
        facing = shift(rows, "yh", 1)
    with jax.named_scope("along"):
        pieces = [rows] + [shift(rows, "z", d) for d in range(1, 4)]
    with jax.named_scope("beyond"):
        pieces += [facing] + [shift(facing, "z", d) for d in range(1, 4)]

    slot_rows = jnp.arange(BLOCK, dtype=jnp.int32)
    x, w = flat[0] >> 5, (flat[0] >> 3) & 3
    positions = jnp.concatenate(
        [b * BLOCK + slot_rows for b in (x + 4 * w, x + 28 - 4 * w)]
    )
    inverse = jnp.exp(jnp.arange(HEAD // 2, dtype=F32) * (-2.0 * math.log(10000.0) / HEAD))
    angles = positions.astype(F32)[:, None] * inverse[None, :]
    cosine, sine = jnp.cos(angles), jnp.sin(angles)
    cosine = jnp.concatenate([cosine, cosine], axis=1)
    sine = jnp.concatenate([-sine, sine], axis=1)

    normed, resident = pl.pallas_call(
        norm_kernel,
        in_specs=[SMEM] + [VMEM] * 9,
        out_specs=[VMEM] * 2,
        out_shape=[pltpu.VMEM((count, D), BF16), pltpu.VMEM((32, D), BF16)],
        scratch_shapes=[pltpu.VMEM((D, count), BF16), pltpu.VMEM((count, D), BF16)],
        compiler_params=grant(24),
        name="norm",
    )(flat, *near_by(pieces), pre_gain.reshape(1, D))
    tables = near_by((cosine, sine))

    def heads(kernel, name, first):
        return pl.pallas_call(
            kernel,
            grid=(2,),
            in_specs=[VMEM, pl.BlockSpec((D, 2 * HEAD), lambda n: (0, n + first)), VMEM, VMEM],
            out_specs=VMEM,
            out_shape=pltpu.VMEM((count, 4 * HEAD), BF16),
            compiler_params=grant(24),
            name=name,
        )(*near_by((normed,)), *far_off((qkv_full,)), *tables)

    kv = heads(key_value_kernel, "key_value", 0)

    same = [kv] + [shift(kv, "x", d) for d in range(1, 4)]
    pair = shift(kv, "yl", 1)
    other = [pair, shift(pair, "x", 1), shift(same[2], "yl", 1), shift(pair, "x", 3)]
    spread = []
    for part in (same, other):
        spread += part
        spread += [shift(s, "c", 1) for s in part]

    query = heads(query_kernel, "query", 2)
    context = pl.pallas_call(
        attention_kernel,
        in_specs=[SMEM] + [VMEM] * 17,
        out_specs=VMEM,
        out_shape=pltpu.VMEM((count, 4 * HEAD), BF16),
        scratch_shapes=[pltpu.VMEM((2, 2 * BLOCK, HEAD), F32), pltpu.VMEM((2, 2 * BLOCK, HEAD), F32)],
        compiler_params=grant(24),
        name="attention",
    )(flat, *near_by((query, *spread)))

    tile = 512
    shares = pl.pallas_call(
        out_kernel,
        grid=(D // tile,),
        in_specs=[SMEM, VMEM, pl.BlockSpec((tile, 4 * HEAD), lambda n: (n, 0))],
        out_specs=[VMEM] * 8,
        out_shape=[pltpu.VMEM((32, D), BF16)] * 8,
        scratch_shapes=[pltpu.VMEM((count, tile), BF16)],
        compiler_params=grant(16),
        name="project",
    )(flat, *near_by((context,)), *far_off((out_full,)))
    received = []
    for dy in range(2):
        for dz in range(4):
            part = shares[4 * dy + dz]
            if dy and dz:
                n = [(i, j) for i in range(4) for j in range(2)]
                part = lax.ppermute(
                    part, TP, [(2 * i + j, 2 * ((i + dz) % 4) + (j ^ dy)) for i, j in n]
                )
            elif dy:
                part = shift(part, "yh", 1)
            elif dz:
                part = shift(part, "z", dz)
            received.append(part)

    refreshed = pl.pallas_call(
        finish_kernel,
        in_specs=[VMEM] * 10,
        out_specs=VMEM,
        out_shape=pltpu.VMEM((32, D), BF16),
        compiler_params=grant(8),
        name="finish",
    )(*near_by((resident, post_gain.reshape(1, D), *received)))

    by_yl = shift(refreshed, "yl", 1)
    by_w = [refreshed, shift(refreshed, "c", 1), by_yl, shift(by_yl, "c", 1)]
    new = far_off((new_blocks,))
    slices = [(16, D)] * 4
    gathered = call(owner_kernel, "owner", new, by_w, slices)
    gathered = gathered[:1] + [shift(gathered[d], "x", d) for d in range(1, 4)]
    final = call(place_kernel, "place", new, gathered, slices)
    final = final[:1] + [shift(final[d], "z", d) for d in range(1, 4)]
    (layer_out,) = call(close_kernel, "close", new, final, [(64, D)])
    return layer_out


def solution(mesh):
    torus = Mesh(mesh.devices.reshape(4, 2, 2, 4, 2), AXES)
    in_specs = (
        P(SEQ, TP),
        P(),
        P(),
        P(),
        P(),
        P(),
        P(SEQ, TP),
        P(SEQ, TP),
        P(SEQ, TP),
        P(SEQ, TP),
    )
    out_specs = P(SEQ + TP, None)
    return jax.shard_map(
        per_device, mesh=torus, in_specs=in_specs, out_specs=out_specs, check_vma=False
    )
```

```python
import math

import jax
import jax.numpy as jnp
from jax import lax
from jax.experimental import pallas as pl
from jax.experimental.pallas import tpu as pltpu
from jax.sharding import Mesh
from jax.sharding import PartitionSpec as P

D = 4608
HEADS = 32
HEAD = 128
BLOCK = 128
EPS = 1e-06
F32 = jnp.float32
BF16 = jnp.bfloat16

AXES = ("x", "yl", "c", "z", "yh")
SEQ = ("x", "yl", "c")
TP = ("z", "yh")


SMEM = pl.BlockSpec(memory_space=pltpu.SMEM)


def shift(value, axis, by):
    n = lax.axis_size(axis)
    return lax.ppermute(value, axis, [(i, (i + by) % n) for i in range(n)])


def rope(values, cos, sin):
    half = HEAD // 2
    swapped = jnp.concatenate([values[:, half:], values[:, :half]], axis=1)
    return values * cos + swapped * sin


def spot(flat):
    me = flat[0]
    return me >> 5, (me >> 4) & 1, (me >> 3) & 1, (me >> 1) & 3, me & 1


def starts(blocks):
    result, so_far = [], jnp.int32(0)
    for m in range(16):
        result.append(so_far)
        so_far = so_far + blocks[m]
    return result


VMEM = pl.BlockSpec(memory_space=pltpu.VMEM)
AWAY = pl.BlockSpec(memory_space=pl.ANY)


def grant(mib):
    return pltpu.CompilerParams(vmem_limit_bytes=mib << 20)


def move(jobs):
    for index, sources, target in jobs:
        for k, source in enumerate(sources):

            def copy(source=source, target=target):
                target[...] = source[...]

            if len(sources) == 1:
                copy()
            else:
                pl.when(index == k)(copy)


def lanes(first):
    return pl.ds(pl.multiple_of(first, BLOCK), BLOCK)


def fetch(jobs, sems):
    copies = [pltpu.make_async_copy(s, t, sems.at[n]) for n, (s, t) in enumerate(jobs)]
    for copy in copies:
        copy.start()
    for copy in copies:
        copy.wait()


def join_kernel(key, value, query, joined, sems):
    jobs, at = [], 0
    for source, first, width in (
        (key, 0, HEAD),
        (value, 0, HEAD),
        (key, HEAD, HEAD),
        (value, HEAD, HEAD),
        (query, 0, 4 * HEAD),
    ):
        jobs.append((source.at[:, first : first + width], joined.at[:, at : at + width]))
        at += width
    fetch(jobs, sems)


def leave_kernel(flat, old_blocks, order, x_old, *refs):
    outs, sems = refs[:4], refs[4]
    x, yl, c, _, _ = spot(flat)
    shard = order[4 * x + 2 * yl + c]
    first = jnp.int32(0)
    for m in range(16):
        first = first + jnp.where(m < shard, old_blocks[m], 0)
    jobs = []
    for d in range(4):
        row = jnp.bitwise_and(x + d - first, 3) * BLOCK
        jobs.append((x_old.at[:, lanes(row)], outs[d]))
    fetch(jobs, sems)


def holders(old_blocks, order, blocks):
    begin = starts(old_blocks)
    result = []
    for block in blocks:
        shard = jnp.int32(-1)
        for m in range(16):
            shard = shard + (begin[m] <= block).astype(jnp.int32)
        holder = jnp.int32(0)
        for m in range(16):
            holder = holder + jnp.where(order[m] == shard, m, 0)
        result.append(holder)
    return result


def targets(x, yl, c):
    to = 2 * yl + c
    return [x + 4 * to, x + 28 - 4 * to]


def sort_kernel(flat, old_blocks, order, *refs):
    sources, (mine, cross) = refs[:8], refs[8:]
    x, yl, c, _, _ = spot(flat)
    blocks = targets(x, yl, c) + targets(x, 1 - yl, c)
    jobs = []
    for n, holder in enumerate(holders(old_blocks, order, blocks)):
        index = jnp.bitwise_and(x - (holder >> 2), 3) + 4 * jnp.bitwise_xor(holder & 1, c)
        out, at = (mine, n) if n < 2 else (cross, n - 2)
        jobs.append((index, sources, out.at[:, at * BLOCK : (at + 1) * BLOCK]))
    move(jobs)


def settle_kernel(flat, old_blocks, order, mine, crossed, rows):
    x, yl, c, _, _ = spot(flat)
    jobs = []
    for n, holder in enumerate(holders(old_blocks, order, targets(x, yl, c))):
        at = slice(n * BLOCK, (n + 1) * BLOCK)
        index = jnp.bitwise_xor((holder >> 1) & 1, yl)
        jobs.append((index, [mine.at[:, at], crossed.at[:, at]], rows.at[:, at]))
    move(jobs)


def norm_kernel(flat, *refs):
    pieces, (gain, normed, resident, features, raw) = refs[:8], refs[8:]
    _, _, _, z, yh = spot(flat)
    width, count = pieces[0].shape
    total = jnp.zeros((1, count), F32)
    for n, piece in enumerate(pieces):
        wide = piece[...].astype(F32)
        total = total + jnp.sum(wide * wide, axis=0, keepdims=True)
        t = 2 * jnp.bitwise_and(z - n % 4, 3) + jnp.bitwise_xor(yh, n // 4)
        features[pl.ds(pl.multiple_of(t * width, 64), width), :] = piece[...]
    scale = lax.rsqrt(total / D + EPS)
    scale = jnp.transpose(jnp.broadcast_to(scale, (BLOCK, count)))
    step = 512
    for at in range(0, D, step):
        rows = jnp.transpose(features[at : at + step, :])
        raw[:, at : at + step] = rows
        for k in range(0, step, BLOCK):
            cols = slice(at + k, at + k + BLOCK)
            wide = rows[:, k : k + BLOCK].astype(F32) * scale * gain[:, cols]
            normed[:, cols] = wide.astype(BF16)
    first = pl.multiple_of(64 * yh + 16 * z, 16)
    for block in range(2):
        source = pl.ds(pl.multiple_of(first + block * BLOCK, 16), 16)
        resident[block * 16 : block * 16 + 16, :] = raw[source, :]


def key_value_kernel(normed, weight, cos, sin, kv, buffer, total, sems):
    step = buffer.shape[0] // sems.shape[0]

    def copy(n):
        rows = pl.ds(n * step, step)
        return pltpu.make_async_copy(
            weight.at[rows, : 4 * HEAD], buffer.at[rows, :], sems.at[n]
        )

    for n in range(sems.shape[0]):
        copy(n).start()
    for n in range(sems.shape[0]):
        copy(n).wait()
        rows = slice(n * step, (n + 1) * step)
        part = jnp.dot(normed[:, rows], buffer[rows, :], preferred_element_type=F32)
        total[...] = part if n == 0 else total[...] + part
    for h in range(2):
        at = 2 * h * HEAD
        kv[:, at : at + HEAD] = rope(total[:, at : at + HEAD], cos[...], sin[...]).astype(BF16)
        kv[:, at + HEAD : at + 2 * HEAD] = total[:, at + HEAD : at + 2 * HEAD].astype(BF16)


def query_kernel(normed, weight, cos, sin, query):
    total = jnp.dot(normed[...], weight[...], preferred_element_type=F32)
    at = pl.multiple_of(pl.program_id(0) * 2 * HEAD, 2 * HEAD)
    for h in range(2):
        part = total[:, h * HEAD : (h + 1) * HEAD]
        turned = rope(part, cos[...], sin[...]) * (D // HEADS) ** (-0.5)
        query[:, pl.ds(at + h * HEAD, HEAD)] = turned.astype(BF16)


def attention_kernel(flat, query, *refs):
    kv = [refs[4 * k : 4 * k + 4] for k in range(4)]
    context, numer, denom = refs[16:]
    x, yl, c, _, _ = spot(flat)
    w = 2 * yl + c
    row = lax.broadcasted_iota(jnp.int32, (2 * BLOCK, BLOCK), 0) % BLOCK
    col = lax.broadcasted_iota(jnp.int32, (2 * BLOCK, BLOCK), 1)

    def chunk(first, dw, block, slot, masked):
        near, far = pl.ds(first, HEAD), pl.ds(first + HEAD, HEAD)
        if isinstance(block, int):
            q_rows, k_rows = pl.ds(block * BLOCK, BLOCK), pl.ds(slot * BLOCK, BLOCK)
        else:
            q_rows = pl.ds(pl.multiple_of(block * BLOCK, BLOCK), BLOCK)
            k_rows = pl.ds(pl.multiple_of(slot * BLOCK, BLOCK), BLOCK)
        q2 = jnp.concatenate([query[q_rows, near], query[q_rows, far]], axis=0)
        keys = jnp.concatenate([kv[dw][d][k_rows, near] for d in range(4)], axis=0)
        values = jnp.concatenate([kv[dw][d][k_rows, far] for d in range(4)], axis=0)
        score = lax.dot_general(q2, keys, (((1,), (1,)), ((), ())), preferred_element_type=F32)
        weight = jnp.exp(50.0 * jnp.tanh(score * (1.0 / 50.0)))
        parts = [weight[:, d * BLOCK : (d + 1) * BLOCK] for d in range(4)]
        if masked:
            parts = [jnp.where(col <= row, parts[0], 0.0)] + [
                jnp.where(x >= d, parts[d], 0.0) for d in range(1, 4)
            ]
            weight = jnp.concatenate(parts, axis=1)
        denom[block] += (parts[0] + parts[1]) + (parts[2] + parts[3])
        numer[block] += jnp.dot(weight.astype(BF16), values, preferred_element_type=F32)

    @pl.loop(0, 2)
    def _(head):
        first = pl.multiple_of(head * 2 * HEAD, 2 * HEAD)
        numer[...] = jnp.zeros_like(numer)
        denom[...] = jnp.zeros_like(denom)
        chunk(first, 0, 0, 0, True)
        chunk(first, 0, 1, 0, False)
        chunk(first, 0, 1, 1, True)
        for dw in range(1, 4):
            later = (jnp.bitwise_xor(w, dw) > w).astype(jnp.int32)
            chunk(first, dw, 1, 0, False)
            chunk(first, dw, later, later, False)
        for block in range(2):
            out = numer[block] / jnp.sum(denom[block], axis=1, keepdims=True)
            rows = slice(block * BLOCK, (block + 1) * BLOCK)
            context[rows, pl.ds(first, HEAD)] = out[:BLOCK].astype(BF16)
            context[rows, pl.ds(first + HEAD, HEAD)] = out[BLOCK:].astype(BF16)


def out_kernel(flat, context, weight, *refs):
    outs, (buffer, scratch, sems) = refs[:8], refs[8:]
    _, _, _, z, yh = spot(flat)
    tile, steps = scratch.shape[1], sems.shape[0]

    def copy(n):
        rows = pl.ds(pl.multiple_of(n * tile, tile), tile)
        return pltpu.make_async_copy(weight.at[rows, :], buffer.at[rows, :], sems.at[n])

    @pl.loop(0, steps)
    def _(n):
        copy(n).start()

    @pl.loop(0, steps)
    def _(n):
        copy(n).wait()
        cols = pl.ds(pl.multiple_of(n * tile, tile), tile)
        scratch[...] = lax.dot_general(
            context[...], buffer[cols, :], (((1,), (1,)), ((), ())), preferred_element_type=F32
        ).astype(BF16)
        for dy in range(2):
            for dz in range(4):
                first = jnp.bitwise_xor(yh, dy) * 64 + jnp.bitwise_and(z + dz, 3) * 16
                for block in range(2):
                    rows = pl.ds(pl.multiple_of(first + block * BLOCK, 16), 16)
                    outs[4 * dy + dz][block * 16 : block * 16 + 16, cols] = scratch[rows, :]


def finish_kernel(resident, gain, *refs):
    terms, out = refs[:8], refs[8]
    total = terms[0][...].astype(F32)
    for term in terms[1:]:
        total = total + term[...].astype(F32)
    scale = lax.rsqrt(jnp.mean(total * total, axis=1, keepdims=True) + EPS)
    out[...] = (resident[...].astype(F32) + total * scale * gain[...]).astype(BF16)


def before(blocks, shard):
    result = jnp.int32(0)
    for m in range(16):
        result = result + jnp.where(m < shard, blocks[m], 0)
    return result


def owner_kernel(flat, new_blocks, *refs):
    by_w, outs = refs[:4], refs[4:]
    x, yl, c, _, _ = spot(flat)
    w = 2 * yl + c
    jobs = []
    for d in range(4):
        start = before(new_blocks, 4 * jnp.bitwise_and(x + d, 3) + w)
        level = (start + jnp.bitwise_and(x - start, 3)) >> 2
        slot = (level >= 4).astype(jnp.int32)
        source = jnp.bitwise_and(jnp.where(level < 4, level, 7 - level), 3)
        row = pl.ds(pl.multiple_of(slot * 16, 16), 16)
        jobs.append((jnp.bitwise_xor(source, w), [part.at[row, :] for part in by_w], outs[d]))
    move(jobs)


def place_kernel(flat, new_blocks, *refs):
    gathered, outs = refs[:4], refs[4:]
    x, yl, c, z, _ = spot(flat)
    start = before(new_blocks, 4 * x + 2 * yl + c)
    move([(jnp.bitwise_and(x - start - (z + d), 3), gathered, outs[d]) for d in range(4)])


def close_kernel(flat, new_blocks, *refs):
    parts, out = refs[:4], refs[4]
    x, yl, c, z, _ = spot(flat)
    count = new_blocks[4 * x + 2 * yl + c]

    @pl.when(z >= count)
    def _():
        out[...] = jnp.zeros_like(out)

    @pl.when(z < count)
    def _():
        for d in range(4):
            row = pl.multiple_of(jnp.bitwise_and(z - d, 3) * 16, 16)
            out[pl.ds(row, 16), :] = parts[d][...]


def per_device(
    x_old, old_blocks, new_blocks, order, pre_gain, post_gain, w_query, w_key, w_value, w_out_t
):
    flat = lax.axis_index(AXES).astype(jnp.int32).reshape(1)
    width = x_old.shape[1]
    count = 2 * BLOCK

    def near_by(arrays):
        return [pltpu.with_memory_space_constraint(a, pltpu.VMEM) for a in arrays]

    def far_off(arrays):
        return [pltpu.with_memory_space_constraint(a, pltpu.HBM) for a in arrays]

    def call(kernel, tables, arrays, shapes):
        results = pl.pallas_call(
            kernel,
            in_specs=[SMEM] * (1 + len(tables)) + [VMEM] * len(arrays),
            out_specs=[VMEM] * len(shapes),
            out_shape=[pltpu.VMEM(s, BF16) for s in shapes],
            compiler_params=grant(8),
        )(flat, *tables, *near_by(arrays))
        return list(results)

    def bring(kernel, tables, arrays, shapes, copies, kind):
        results = pl.pallas_call(
            kernel,
            in_specs=[SMEM] * len(tables) + [AWAY] * len(arrays),
            out_specs=[VMEM] * len(shapes),
            out_shape=[kind(s, BF16) for s in shapes],
            scratch_shapes=[pltpu.SemaphoreType.DMA((copies,))],
            compiler_params=grant(8),
        )(*tables, *far_off(arrays))
        return list(results)

    (joined,) = bring(
        join_kernel,
        (),
        (w_key, w_value, w_query),
        [(w_key.shape[0], 8 * HEAD)],
        5,
        jax.ShapeDtypeStruct,
    )
    qkv_full = lax.all_gather(joined, SEQ, axis=0, tiled=True)
    out_full = lax.all_gather(w_out_t, SEQ, axis=0, tiled=True)

    old = far_off((old_blocks, order))
    near = bring(leave_kernel, (flat, *old), (x_old.T,), [(width, BLOCK)] * 4, 4, pltpu.VMEM)
    near = near[:1] + [shift(near[d], "x", d) for d in range(1, 4)]
    far = [shift(part, "c", 1) for part in near]
    mine, cross = call(sort_kernel, old, near + far, [(width, count)] * 2)
    cross = shift(cross, "yl", 1)
    (rows,) = call(settle_kernel, old, (mine, cross), [(width, count)])

    facing = shift(rows, "yh", 1)
    pieces = [rows] + [shift(rows, "z", d) for d in range(1, 4)]
    pieces += [facing] + [shift(facing, "z", d) for d in range(1, 4)]

    slot_rows = jnp.arange(BLOCK, dtype=jnp.int32)
    x, w = flat[0] >> 5, (flat[0] >> 3) & 3
    positions = jnp.concatenate(
        [b * BLOCK + slot_rows for b in (x + 4 * w, x + 28 - 4 * w)]
    )
    inverse = jnp.exp(jnp.arange(HEAD // 2, dtype=F32) * (-2.0 * math.log(10000.0) / HEAD))
    angles = positions.astype(F32)[:, None] * inverse[None, :]
    cosine, sine = jnp.cos(angles), jnp.sin(angles)
    cosine = jnp.concatenate([cosine, cosine], axis=1)
    sine = jnp.concatenate([-sine, sine], axis=1)

    normed, resident = pl.pallas_call(
        norm_kernel,
        in_specs=[SMEM] + [VMEM] * 9,
        out_specs=[VMEM] * 2,
        out_shape=[pltpu.VMEM((count, D), BF16), pltpu.VMEM((32, D), BF16)],
        scratch_shapes=[pltpu.VMEM((D, count), BF16), pltpu.VMEM((count, D), BF16)],
        compiler_params=grant(24),
        name="norm",
    )(flat, *near_by(pieces), pre_gain.reshape(1, D))
    tables = near_by((cosine, sine))

    def heads(kernel, first):
        return pl.pallas_call(
            kernel,
            grid=(2,),
            in_specs=[VMEM, pl.BlockSpec((D, 2 * HEAD), lambda n: (0, n + first)), VMEM, VMEM],
            out_specs=VMEM,
            out_shape=pltpu.VMEM((count, 4 * HEAD), BF16),
            compiler_params=grant(24),
        )(*near_by((normed,)), *far_off((qkv_full,)), *tables)

    kv = pl.pallas_call(
        key_value_kernel,
        in_specs=[VMEM, AWAY, VMEM, VMEM],
        out_specs=VMEM,
        out_shape=pltpu.VMEM((count, 4 * HEAD), BF16),
        scratch_shapes=[
            pltpu.VMEM((D, 4 * HEAD), BF16),
            pltpu.VMEM((count, 4 * HEAD), F32),
            pltpu.SemaphoreType.DMA((4,)),
        ],
        compiler_params=grant(24),
        name="key_value",
    )(*near_by((normed,)), *far_off((qkv_full,)), *tables)

    opposite = shift(kv, "x", 2)
    same = [kv, shift(kv, "x", 1), opposite, shift(kv, "x", 3)]
    pair = shift(kv, "yl", 1)
    other = [pair, shift(pair, "x", 1), shift(same[2], "yl", 1), shift(pair, "x", 3)]
    spread = []
    for part in (same, other):
        spread += part
        spread += [shift(s, "c", 1) for s in part]

    query = heads(query_kernel, 2)
    context = pl.pallas_call(
        attention_kernel,
        in_specs=[SMEM] + [VMEM] * 17,
        out_specs=VMEM,
        out_shape=pltpu.VMEM((count, 4 * HEAD), BF16),
        scratch_shapes=[pltpu.VMEM((2, 2 * BLOCK, HEAD), F32), pltpu.VMEM((2, 2 * BLOCK, HEAD), F32)],
        compiler_params=grant(24),
        name="attention",
    )(flat, *near_by((query, *spread)))

    tile = 512
    shares = pl.pallas_call(
        out_kernel,
        in_specs=[SMEM, VMEM, AWAY],
        out_specs=[VMEM] * 8,
        out_shape=[pltpu.VMEM((32, D), BF16)] * 8,
        scratch_shapes=[
            pltpu.VMEM((D, 4 * HEAD), BF16),
            pltpu.VMEM((count, tile), BF16),
            pltpu.SemaphoreType.DMA((D // tile,)),
        ],
        compiler_params=grant(16),
        name="project",
    )(flat, *near_by((context,)), *far_off((out_full,)))
    received = []
    for dy in range(2):
        for dz in range(4):
            part = shares[4 * dy + dz]
            if dy and dz:
                n = [(i, j) for i in range(4) for j in range(2)]
                part = lax.ppermute(
                    part, TP, [(2 * i + j, 2 * ((i + dz) % 4) + (j ^ dy)) for i, j in n]
                )
            elif dy:
                part = shift(part, "yh", 1)
            elif dz:
                part = shift(part, "z", dz)
            received.append(part)

    refreshed = pl.pallas_call(
        finish_kernel,
        in_specs=[VMEM] * 10,
        out_specs=VMEM,
        out_shape=pltpu.VMEM((32, D), BF16),
        compiler_params=grant(8),
        name="finish",
    )(*near_by((resident, post_gain.reshape(1, D), *received)))

    by_yl = shift(refreshed, "yl", 1)
    by_w = [refreshed, shift(refreshed, "c", 1), by_yl, shift(by_yl, "c", 1)]
    new = far_off((new_blocks,))
    slices = [(16, D)] * 4
    gathered = call(owner_kernel, new, by_w, slices)
    gathered = gathered[:1] + [shift(gathered[d], "x", d) for d in range(1, 4)]
    final = call(place_kernel, new, gathered, slices)
    final = final[:1] + [shift(final[d], "z", d) for d in range(1, 4)]
    (layer_out,) = call(close_kernel, new, final, [(64, D)])
    return layer_out


def solution(mesh):
    torus = Mesh(mesh.devices.reshape(4, 2, 2, 4, 2), AXES)
    in_specs = (
        P(SEQ, TP),
        P(),
        P(),
        P(),
        P(),
        P(),
        P(SEQ, TP),
        P(SEQ, TP),
        P(SEQ, TP),
        P(SEQ, TP),
    )
    out_specs = P(SEQ + TP, None)

    return jax.shard_map(
        per_device, mesh=torus, in_specs=in_specs, out_specs=out_specs, check_vma=False
    )
```

```python
import math

import jax
import jax.numpy as jnp
from jax import lax
from jax.experimental import pallas as pl
from jax.experimental.pallas import tpu as pltpu
from jax.sharding import Mesh
from jax.sharding import PartitionSpec as P

D = 4608
HEADS = 32
HEAD = 128
BLOCK = 128
EPS = 1e-06
F32 = jnp.float32
BF16 = jnp.bfloat16

AXES = ("x", "yl", "c", "z", "yh")
SEQ = ("x", "yl", "c")
TP = ("z", "yh")


SMEM = pl.BlockSpec(memory_space=pltpu.SMEM)


def shift(value, axis, by):
    n = lax.axis_size(axis)
    return lax.ppermute(value, axis, [(i, (i + by) % n) for i in range(n)])


def rope(values, cos, sin):
    half = HEAD // 2
    swapped = jnp.concatenate([values[:, half:], values[:, :half]], axis=1)
    return values * cos + swapped * sin


def spot(flat):
    me = flat[0]
    return me >> 5, (me >> 4) & 1, (me >> 3) & 1, (me >> 1) & 3, me & 1


def starts(blocks):
    result, so_far = [], jnp.int32(0)
    for m in range(16):
        result.append(so_far)
        so_far = so_far + blocks[m]
    return result


VMEM = pl.BlockSpec(memory_space=pltpu.VMEM)
AWAY = pl.BlockSpec(memory_space=pl.ANY)


def grant(mib):
    return pltpu.CompilerParams(vmem_limit_bytes=mib << 20)


def move(jobs):
    for index, sources, target in jobs:
        for k, source in enumerate(sources):

            def copy(source=source, target=target):
                target[...] = source[...]

            if len(sources) == 1:
                copy()
            else:
                pl.when(index == k)(copy)


def lanes(first):
    return pl.ds(pl.multiple_of(first, BLOCK), BLOCK)


def fetch(jobs, sems):
    copies = [pltpu.make_async_copy(s, t, sems.at[n]) for n, (s, t) in enumerate(jobs)]
    for copy in copies:
        copy.start()
    for copy in copies:
        copy.wait()


def join_kernel(key, value, query, joined, sems):
    jobs, at = [], 0
    for source, first, width in (
        (key, 0, HEAD),
        (value, 0, HEAD),
        (key, HEAD, HEAD),
        (value, HEAD, HEAD),
        (query, 0, 4 * HEAD),
    ):
        jobs.append((source.at[:, first : first + width], joined.at[:, at : at + width]))
        at += width
    fetch(jobs, sems)


def hold_kernel(source, after, target, sems):
    del after
    fetch([(source, target)], sems)


def pack_kernel(flat, *refs):
    parts, whole = refs[:16], refs[16]
    x, yl, c, _, _ = spot(flat)
    size = parts[0].shape[0]
    for n, part in enumerate(parts):
        w = jnp.bitwise_xor(2 * yl + c, n // 4)
        first = (4 * jnp.bitwise_and(x - n % 4, 3) + w) * size
        whole[pl.ds(pl.multiple_of(first, 32), size), :] = part[...]


def leave_kernel(flat, old_blocks, order, x_old, *refs):
    outs, sems = refs[:4], refs[4]
    x, yl, c, _, _ = spot(flat)
    shard = order[4 * x + 2 * yl + c]
    first = jnp.int32(0)
    for m in range(16):
        first = first + jnp.where(m < shard, old_blocks[m], 0)
    jobs = []
    for d in range(4):
        row = jnp.bitwise_and(x + d - first, 3) * BLOCK
        jobs.append((x_old.at[:, lanes(row)], outs[d]))
    fetch(jobs, sems)


def holders(old_blocks, order, blocks):
    begin = starts(old_blocks)
    result = []
    for block in blocks:
        shard = jnp.int32(-1)
        for m in range(16):
            shard = shard + (begin[m] <= block).astype(jnp.int32)
        holder = jnp.int32(0)
        for m in range(16):
            holder = holder + jnp.where(order[m] == shard, m, 0)
        result.append(holder)
    return result


def targets(x, yl, c):
    to = 2 * yl + c
    return [x + 4 * to, x + 28 - 4 * to]


def sort_kernel(flat, old_blocks, order, *refs):
    sources, (mine, cross) = refs[:8], refs[8:]
    x, yl, c, _, _ = spot(flat)
    blocks = targets(x, yl, c) + targets(x, 1 - yl, c)
    jobs = []
    for n, holder in enumerate(holders(old_blocks, order, blocks)):
        index = jnp.bitwise_and(x - (holder >> 2), 3) + 4 * jnp.bitwise_xor(holder & 1, c)
        out, at = (mine, n) if n < 2 else (cross, n - 2)
        jobs.append((index, sources, out.at[:, at * BLOCK : (at + 1) * BLOCK]))
    move(jobs)


def settle_kernel(flat, old_blocks, order, mine, crossed, rows):
    x, yl, c, _, _ = spot(flat)
    jobs = []
    for n, holder in enumerate(holders(old_blocks, order, targets(x, yl, c))):
        at = slice(n * BLOCK, (n + 1) * BLOCK)
        index = jnp.bitwise_xor((holder >> 1) & 1, yl)
        jobs.append((index, [mine.at[:, at], crossed.at[:, at]], rows.at[:, at]))
    move(jobs)


def norm_kernel(flat, *refs):
    pieces, (gain, normed, resident, features, raw) = refs[:8], refs[8:]
    _, _, _, z, yh = spot(flat)
    width, count = pieces[0].shape
    total = jnp.zeros((1, count), F32)
    for n, piece in enumerate(pieces):
        wide = piece[...].astype(F32)
        total = total + jnp.sum(wide * wide, axis=0, keepdims=True)
        t = 2 * jnp.bitwise_and(z - n % 4, 3) + jnp.bitwise_xor(yh, n // 4)
        features[pl.ds(pl.multiple_of(t * width, 64), width), :] = piece[...]
    scale = lax.rsqrt(total / D + EPS)
    scale = jnp.transpose(jnp.broadcast_to(scale, (BLOCK, count)))
    step = 512
    for at in range(0, D, step):
        rows = jnp.transpose(features[at : at + step, :])
        raw[:, at : at + step] = rows
        for k in range(0, step, BLOCK):
            cols = slice(at + k, at + k + BLOCK)
            wide = rows[:, k : k + BLOCK].astype(F32) * scale * gain[:, cols]
            normed[:, cols] = wide.astype(BF16)
    first = pl.multiple_of(64 * yh + 16 * z, 16)
    for block in range(2):
        source = pl.ds(pl.multiple_of(first + block * BLOCK, 16), 16)
        resident[block * 16 : block * 16 + 16, :] = raw[source, :]


def key_value_kernel(normed, weight, cos, sin, kv, buffer, total, sems):
    step = buffer.shape[0] // sems.shape[0]

    def copy(n):
        rows = pl.ds(n * step, step)
        return pltpu.make_async_copy(
            weight.at[rows, : 4 * HEAD], buffer.at[rows, :], sems.at[n]
        )

    for n in range(sems.shape[0]):
        copy(n).start()
    for n in range(sems.shape[0]):
        copy(n).wait()
        rows = slice(n * step, (n + 1) * step)
        part = jnp.dot(normed[:, rows], buffer[rows, :], preferred_element_type=F32)
        total[...] = part if n == 0 else total[...] + part
    for h in range(2):
        at = 2 * h * HEAD
        kv[:, at : at + HEAD] = rope(total[:, at : at + HEAD], cos[...], sin[...]).astype(BF16)
        kv[:, at + HEAD : at + 2 * HEAD] = total[:, at + HEAD : at + 2 * HEAD].astype(BF16)


def query_kernel(normed, weight, cos, sin, query):
    total = jnp.dot(normed[...], weight[...], preferred_element_type=F32)
    at = pl.multiple_of(pl.program_id(0) * 2 * HEAD, 2 * HEAD)
    for h in range(2):
        part = total[:, h * HEAD : (h + 1) * HEAD]
        turned = rope(part, cos[...], sin[...]) * (D // HEADS) ** (-0.5)
        query[:, pl.ds(at + h * HEAD, HEAD)] = turned.astype(BF16)


def attention_kernel(flat, query, *refs):
    kv = [refs[4 * k : 4 * k + 4] for k in range(4)]
    context, numer, denom = refs[16:]
    x, yl, c, _, _ = spot(flat)
    w = 2 * yl + c
    row = lax.broadcasted_iota(jnp.int32, (2 * BLOCK, BLOCK), 0) % BLOCK
    col = lax.broadcasted_iota(jnp.int32, (2 * BLOCK, BLOCK), 1)

    def chunk(first, dw, block, slot, masked):
        near, far = pl.ds(first, HEAD), pl.ds(first + HEAD, HEAD)
        if isinstance(block, int):
            q_rows, k_rows = pl.ds(block * BLOCK, BLOCK), pl.ds(slot * BLOCK, BLOCK)
        else:
            q_rows = pl.ds(pl.multiple_of(block * BLOCK, BLOCK), BLOCK)
            k_rows = pl.ds(pl.multiple_of(slot * BLOCK, BLOCK), BLOCK)
        q2 = jnp.concatenate([query[q_rows, near], query[q_rows, far]], axis=0)
        keys = jnp.concatenate([kv[dw][d][k_rows, near] for d in range(4)], axis=0)
        values = jnp.concatenate([kv[dw][d][k_rows, far] for d in range(4)], axis=0)
        score = lax.dot_general(q2, keys, (((1,), (1,)), ((), ())), preferred_element_type=F32)
        weight = jnp.exp(50.0 * jnp.tanh(score * (1.0 / 50.0)))
        parts = [weight[:, d * BLOCK : (d + 1) * BLOCK] for d in range(4)]
        if masked:
            parts = [jnp.where(col <= row, parts[0], 0.0)] + [
                jnp.where(x >= d, parts[d], 0.0) for d in range(1, 4)
            ]
            weight = jnp.concatenate(parts, axis=1)
        denom[block] += (parts[0] + parts[1]) + (parts[2] + parts[3])
        numer[block] += jnp.dot(weight.astype(BF16), values, preferred_element_type=F32)

    @pl.loop(0, 2)
    def _(head):
        first = pl.multiple_of(head * 2 * HEAD, 2 * HEAD)
        numer[...] = jnp.zeros_like(numer)
        denom[...] = jnp.zeros_like(denom)
        chunk(first, 0, 0, 0, True)
        chunk(first, 0, 1, 0, False)
        chunk(first, 0, 1, 1, True)
        for dw in range(1, 4):
            later = (jnp.bitwise_xor(w, dw) > w).astype(jnp.int32)
            chunk(first, dw, 1, 0, False)
            chunk(first, dw, later, later, False)
        for block in range(2):
            out = numer[block] / jnp.sum(denom[block], axis=1, keepdims=True)
            rows = slice(block * BLOCK, (block + 1) * BLOCK)
            context[rows, pl.ds(first, HEAD)] = out[:BLOCK].astype(BF16)
            context[rows, pl.ds(first + HEAD, HEAD)] = out[BLOCK:].astype(BF16)


def out_kernel(flat, context, weight, *refs):
    outs, scratch = refs[:8], refs[8]
    _, _, _, z, yh = spot(flat)
    tile = scratch.shape[1]

    @pl.loop(0, weight.shape[0] // tile)
    def _(n):
        cols = pl.ds(pl.multiple_of(n * tile, tile), tile)
        scratch[...] = lax.dot_general(
            context[...], weight[cols, :], (((1,), (1,)), ((), ())), preferred_element_type=F32
        ).astype(BF16)
        for dy in range(2):
            for dz in range(4):
                first = jnp.bitwise_xor(yh, dy) * 64 + jnp.bitwise_and(z + dz, 3) * 16
                for block in range(2):
                    rows = pl.ds(pl.multiple_of(first + block * BLOCK, 16), 16)
                    outs[4 * dy + dz][block * 16 : block * 16 + 16, cols] = scratch[rows, :]


def finish_kernel(resident, gain, *refs):
    terms, out = refs[:8], refs[8]
    total = terms[0][...].astype(F32)
    for term in terms[1:]:
        total = total + term[...].astype(F32)
    scale = lax.rsqrt(jnp.mean(total * total, axis=1, keepdims=True) + EPS)
    out[...] = (resident[...].astype(F32) + total * scale * gain[...]).astype(BF16)


def before(blocks, shard):
    result = jnp.int32(0)
    for m in range(16):
        result = result + jnp.where(m < shard, blocks[m], 0)
    return result


def owner_kernel(flat, new_blocks, *refs):
    by_w, outs = refs[:4], refs[4:]
    x, yl, c, _, _ = spot(flat)
    w = 2 * yl + c
    jobs = []
    for d in range(4):
        start = before(new_blocks, 4 * jnp.bitwise_and(x + d, 3) + w)
        level = (start + jnp.bitwise_and(x - start, 3)) >> 2
        slot = (level >= 4).astype(jnp.int32)
        source = jnp.bitwise_and(jnp.where(level < 4, level, 7 - level), 3)
        row = pl.ds(pl.multiple_of(slot * 16, 16), 16)
        jobs.append((jnp.bitwise_xor(source, w), [part.at[row, :] for part in by_w], outs[d]))
    move(jobs)


def place_kernel(flat, new_blocks, *refs):
    gathered, outs = refs[:4], refs[4:]
    x, yl, c, z, _ = spot(flat)
    start = before(new_blocks, 4 * x + 2 * yl + c)
    move([(jnp.bitwise_and(x - start - (z + d), 3), gathered, outs[d]) for d in range(4)])


def close_kernel(flat, new_blocks, *refs):
    parts, out = refs[:4], refs[4]
    x, yl, c, z, _ = spot(flat)
    count = new_blocks[4 * x + 2 * yl + c]

    @pl.when(z >= count)
    def _():
        out[...] = jnp.zeros_like(out)

    @pl.when(z < count)
    def _():
        for d in range(4):
            row = pl.multiple_of(jnp.bitwise_and(z - d, 3) * 16, 16)
            out[pl.ds(row, 16), :] = parts[d][...]


def per_device(
    x_old, old_blocks, new_blocks, order, pre_gain, post_gain, w_query, w_key, w_value, w_out_t
):
    flat = lax.axis_index(AXES).astype(jnp.int32).reshape(1)
    width = x_old.shape[1]
    count = 2 * BLOCK

    def near_by(arrays):
        return [pltpu.with_memory_space_constraint(a, pltpu.VMEM) for a in arrays]

    def far_off(arrays):
        return [pltpu.with_memory_space_constraint(a, pltpu.HBM) for a in arrays]

    def call(kernel, tables, arrays, shapes):
        results = pl.pallas_call(
            kernel,
            in_specs=[SMEM] * (1 + len(tables)) + [VMEM] * len(arrays),
            out_specs=[VMEM] * len(shapes),
            out_shape=[pltpu.VMEM(s, BF16) for s in shapes],
            compiler_params=grant(8),
        )(flat, *tables, *near_by(arrays))
        return list(results)

    def bring(kernel, tables, arrays, shapes, copies, kind):
        results = pl.pallas_call(
            kernel,
            in_specs=[SMEM] * len(tables) + [AWAY] * len(arrays),
            out_specs=[VMEM] * len(shapes),
            out_shape=[kind(s, BF16) for s in shapes],
            scratch_shapes=[pltpu.SemaphoreType.DMA((copies,))],
            compiler_params=grant(8),
        )(*tables, *far_off(arrays))
        return list(results)

    def everywhere(part):
        opposite = shift(part, "x", 2)
        pair = shift(part, "yl", 1)
        same = [part, shift(part, "x", 1), opposite, shift(part, "x", 3)]
        other = [pair, shift(pair, "x", 1), shift(opposite, "yl", 1), shift(pair, "x", 3)]
        result = []
        for parts in (same, other):
            result += parts
            result += [shift(s, "c", 1) for s in parts]
        return result

    (joined,) = bring(
        join_kernel,
        (),
        (w_key, w_value, w_query),
        [(w_key.shape[0], 8 * HEAD)],
        5,
        jax.ShapeDtypeStruct,
    )
    qkv_full = lax.all_gather(joined, SEQ, axis=0, tiled=True)

    old = far_off((old_blocks, order))
    near = bring(leave_kernel, (flat, *old), (x_old.T,), [(width, BLOCK)] * 4, 4, pltpu.VMEM)
    near = near[:1] + [shift(near[d], "x", d) for d in range(1, 4)]
    far = [shift(part, "c", 1) for part in near]
    mine, cross = call(sort_kernel, old, near + far, [(width, count)] * 2)
    cross = shift(cross, "yl", 1)
    (rows,) = call(settle_kernel, old, (mine, cross), [(width, count)])

    (held,) = pl.pallas_call(
        hold_kernel,
        in_specs=[AWAY, VMEM],
        out_specs=[VMEM],
        out_shape=[pltpu.VMEM(w_out_t.shape, BF16)],
        scratch_shapes=[pltpu.SemaphoreType.DMA((1,))],
        compiler_params=grant(8),
        name="hold",
    )(*far_off((w_out_t,)), *near_by((rows,)))
    spread_out = everywhere(held)

    facing = shift(rows, "yh", 1)
    pieces = [rows] + [shift(rows, "z", d) for d in range(1, 4)]
    pieces += [facing] + [shift(facing, "z", d) for d in range(1, 4)]

    slot_rows = jnp.arange(BLOCK, dtype=jnp.int32)
    x, w = flat[0] >> 5, (flat[0] >> 3) & 3
    positions = jnp.concatenate(
        [b * BLOCK + slot_rows for b in (x + 4 * w, x + 28 - 4 * w)]
    )
    inverse = jnp.exp(jnp.arange(HEAD // 2, dtype=F32) * (-2.0 * math.log(10000.0) / HEAD))
    angles = positions.astype(F32)[:, None] * inverse[None, :]
    cosine, sine = jnp.cos(angles), jnp.sin(angles)
    cosine = jnp.concatenate([cosine, cosine], axis=1)
    sine = jnp.concatenate([-sine, sine], axis=1)

    normed, resident = pl.pallas_call(
        norm_kernel,
        in_specs=[SMEM] + [VMEM] * 9,
        out_specs=[VMEM] * 2,
        out_shape=[pltpu.VMEM((count, D), BF16), pltpu.VMEM((32, D), BF16)],
        scratch_shapes=[pltpu.VMEM((D, count), BF16), pltpu.VMEM((count, D), BF16)],
        compiler_params=grant(24),
        name="norm",
    )(flat, *near_by(pieces), pre_gain.reshape(1, D))
    tables = near_by((cosine, sine))

    def heads(kernel, first):
        return pl.pallas_call(
            kernel,
            grid=(2,),
            in_specs=[VMEM, pl.BlockSpec((D, 2 * HEAD), lambda n: (0, n + first)), VMEM, VMEM],
            out_specs=VMEM,
            out_shape=pltpu.VMEM((count, 4 * HEAD), BF16),
            compiler_params=grant(24),
        )(*near_by((normed,)), *far_off((qkv_full,)), *tables)

    kv = pl.pallas_call(
        key_value_kernel,
        in_specs=[VMEM, AWAY, VMEM, VMEM],
        out_specs=VMEM,
        out_shape=pltpu.VMEM((count, 4 * HEAD), BF16),
        scratch_shapes=[
            pltpu.VMEM((D, 4 * HEAD), BF16),
            pltpu.VMEM((count, 4 * HEAD), F32),
            pltpu.SemaphoreType.DMA((4,)),
        ],
        compiler_params=grant(24),
        name="key_value",
    )(*near_by((normed,)), *far_off((qkv_full,)), *tables)

    spread = everywhere(kv)

    query = heads(query_kernel, 2)
    (out_full,) = call(pack_kernel, (), spread_out, [(D, 4 * HEAD)])
    context = pl.pallas_call(
        attention_kernel,
        in_specs=[SMEM] + [VMEM] * 17,
        out_specs=VMEM,
        out_shape=pltpu.VMEM((count, 4 * HEAD), BF16),
        scratch_shapes=[pltpu.VMEM((2, 2 * BLOCK, HEAD), F32), pltpu.VMEM((2, 2 * BLOCK, HEAD), F32)],
        compiler_params=grant(24),
        name="attention",
    )(flat, *near_by((query, *spread)))

    tile = 512
    shares = pl.pallas_call(
        out_kernel,
        in_specs=[SMEM, VMEM, VMEM],
        out_specs=[VMEM] * 8,
        out_shape=[pltpu.VMEM((32, D), BF16)] * 8,
        scratch_shapes=[pltpu.VMEM((count, tile), BF16)],
        compiler_params=grant(16),
        name="project",
    )(flat, *near_by((context, out_full)))
    received = []
    for dy in range(2):
        for dz in range(4):
            part = shares[4 * dy + dz]
            if dy and dz:
                n = [(i, j) for i in range(4) for j in range(2)]
                part = lax.ppermute(
                    part, TP, [(2 * i + j, 2 * ((i + dz) % 4) + (j ^ dy)) for i, j in n]
                )
            elif dy:
                part = shift(part, "yh", 1)
            elif dz:
                part = shift(part, "z", dz)
            received.append(part)

    refreshed = pl.pallas_call(
        finish_kernel,
        in_specs=[VMEM] * 10,
        out_specs=VMEM,
        out_shape=pltpu.VMEM((32, D), BF16),
        compiler_params=grant(8),
        name="finish",
    )(*near_by((resident, post_gain.reshape(1, D), *received)))

    by_yl = shift(refreshed, "yl", 1)
    by_w = [refreshed, shift(refreshed, "c", 1), by_yl, shift(by_yl, "c", 1)]
    new = far_off((new_blocks,))
    slices = [(16, D)] * 4
    gathered = call(owner_kernel, new, by_w, slices)
    gathered = gathered[:1] + [shift(gathered[d], "x", d) for d in range(1, 4)]
    final = call(place_kernel, new, gathered, slices)
    final = final[:1] + [shift(final[d], "z", d) for d in range(1, 4)]
    (layer_out,) = call(close_kernel, new, final, [(64, D)])
    return layer_out


def solution(mesh):
    torus = Mesh(mesh.devices.reshape(4, 2, 2, 4, 2), AXES)
    in_specs = (
        P(SEQ, TP),
        P(),
        P(),
        P(),
        P(),
        P(),
        P(SEQ, TP),
        P(SEQ, TP),
        P(SEQ, TP),
        P(SEQ, TP),
    )
    out_specs = P(SEQ + TP, None)

    return jax.shard_map(
        per_device, mesh=torus, in_specs=in_specs, out_specs=out_specs, check_vma=False
    )
```

```python
import math

import jax
import jax.numpy as jnp
from jax import lax
from jax.experimental import pallas as pl
from jax.experimental.pallas import tpu as pltpu
from jax.sharding import Mesh
from jax.sharding import PartitionSpec as P

D = 4608
HEADS = 32
HEAD = 128
BLOCK = 128
EPS = 1e-06
F32 = jnp.float32
BF16 = jnp.bfloat16

AXES = ("x", "yl", "c", "z", "yh")
SEQ = ("x", "yl", "c")
TP = ("z", "yh")


SMEM = pl.BlockSpec(memory_space=pltpu.SMEM)


def shift(value, axis, by):
    n = lax.axis_size(axis)
    return lax.ppermute(value, axis, [(i, (i + by) % n) for i in range(n)])


def rope(values, cos, sin):
    half = HEAD // 2
    swapped = jnp.concatenate([values[:, half:], values[:, :half]], axis=1)
    return values * cos + swapped * sin


def spot(flat):
    me = flat[0]
    return me >> 5, (me >> 4) & 1, (me >> 3) & 1, (me >> 1) & 3, me & 1


def starts(blocks):
    result, so_far = [], jnp.int32(0)
    for m in range(16):
        result.append(so_far)
        so_far = so_far + blocks[m]
    return result


VMEM = pl.BlockSpec(memory_space=pltpu.VMEM)
AWAY = pl.BlockSpec(memory_space=pl.ANY)


def grant(mib):
    return pltpu.CompilerParams(vmem_limit_bytes=mib << 20)


def move(jobs):
    for index, sources, target in jobs:
        for k, source in enumerate(sources):

            def copy(source=source, target=target):
                target[...] = source[...]

            if len(sources) == 1:
                copy()
            else:
                pl.when(index == k)(copy)


def lanes(first):
    return pl.ds(pl.multiple_of(first, BLOCK), BLOCK)


def fetch(jobs, sems):
    copies = [pltpu.make_async_copy(s, t, sems.at[n]) for n, (s, t) in enumerate(jobs)]
    for copy in copies:
        copy.start()
    for copy in copies:
        copy.wait()


def join_kernel(query, out_t, joined, sems):
    half = 4 * HEAD
    fetch([(query, joined.at[:, :half]), (out_t, joined.at[:, half:])], sems)


def hold_kernel(key, value, after, held, sems):
    del after
    jobs = []
    for n, source in enumerate((key, value, key, value)):
        first = n // 2 * HEAD
        jobs.append((source.at[:, first : first + HEAD], held.at[:, n * HEAD : (n + 1) * HEAD]))
    fetch(jobs, sems)


def pack_kernel(flat, *refs):
    parts, whole = refs[:16], refs[16]
    x, yl, c, _, _ = spot(flat)
    size = parts[0].shape[0]
    for n, part in enumerate(parts):
        w = jnp.bitwise_xor(2 * yl + c, n // 4)
        first = (4 * jnp.bitwise_and(x - n % 4, 3) + w) * size
        whole[pl.ds(pl.multiple_of(first, 32), size), :] = part[...]


def leave_kernel(flat, old_blocks, order, x_old, *refs):
    outs, sems = refs[:4], refs[4]
    x, yl, c, _, _ = spot(flat)
    shard = order[4 * x + 2 * yl + c]
    first = jnp.int32(0)
    for m in range(16):
        first = first + jnp.where(m < shard, old_blocks[m], 0)
    jobs = []
    for d in range(4):
        row = jnp.bitwise_and(x + d - first, 3) * BLOCK
        jobs.append((x_old.at[:, lanes(row)], outs[d]))
    fetch(jobs, sems)


def holders(old_blocks, order, blocks):
    begin = starts(old_blocks)
    result = []
    for block in blocks:
        shard = jnp.int32(-1)
        for m in range(16):
            shard = shard + (begin[m] <= block).astype(jnp.int32)
        holder = jnp.int32(0)
        for m in range(16):
            holder = holder + jnp.where(order[m] == shard, m, 0)
        result.append(holder)
    return result


def targets(x, yl, c):
    to = 2 * yl + c
    return [x + 4 * to, x + 28 - 4 * to]


def sort_kernel(flat, old_blocks, order, *refs):
    sources, (mine, cross) = refs[:8], refs[8:]
    x, yl, c, _, _ = spot(flat)
    blocks = targets(x, yl, c) + targets(x, 1 - yl, c)
    jobs = []
    for n, holder in enumerate(holders(old_blocks, order, blocks)):
        index = jnp.bitwise_and(x - (holder >> 2), 3) + 4 * jnp.bitwise_xor(holder & 1, c)
        out, at = (mine, n) if n < 2 else (cross, n - 2)
        jobs.append((index, sources, out.at[:, at * BLOCK : (at + 1) * BLOCK]))
    move(jobs)


def settle_kernel(flat, old_blocks, order, mine, crossed, rows):
    x, yl, c, _, _ = spot(flat)
    jobs = []
    for n, holder in enumerate(holders(old_blocks, order, targets(x, yl, c))):
        at = slice(n * BLOCK, (n + 1) * BLOCK)
        index = jnp.bitwise_xor((holder >> 1) & 1, yl)
        jobs.append((index, [mine.at[:, at], crossed.at[:, at]], rows.at[:, at]))
    move(jobs)


def norm_kernel(flat, *refs):
    pieces, (gain, normed, resident, features, raw) = refs[:8], refs[8:]
    _, _, _, z, yh = spot(flat)
    width, count = pieces[0].shape
    total = jnp.zeros((1, count), F32)
    for n, piece in enumerate(pieces):
        wide = piece[...].astype(F32)
        total = total + jnp.sum(wide * wide, axis=0, keepdims=True)
        t = 2 * jnp.bitwise_and(z - n % 4, 3) + jnp.bitwise_xor(yh, n // 4)
        features[pl.ds(pl.multiple_of(t * width, 64), width), :] = piece[...]
    scale = lax.rsqrt(total / D + EPS)
    scale = jnp.transpose(jnp.broadcast_to(scale, (BLOCK, count)))
    step = 512
    for at in range(0, D, step):
        rows = jnp.transpose(features[at : at + step, :])
        raw[:, at : at + step] = rows
        for k in range(0, step, BLOCK):
            cols = slice(at + k, at + k + BLOCK)
            wide = rows[:, k : k + BLOCK].astype(F32) * scale * gain[:, cols]
            normed[:, cols] = wide.astype(BF16)
    first = pl.multiple_of(64 * yh + 16 * z, 16)
    for block in range(2):
        source = pl.ds(pl.multiple_of(first + block * BLOCK, 16), 16)
        resident[block * 16 : block * 16 + 16, :] = raw[source, :]


def key_value_kernel(normed, weight, cos, sin, kv):
    total = jnp.dot(normed[...], weight[...], preferred_element_type=F32)
    for h in range(2):
        at = 2 * h * HEAD
        kv[:, at : at + HEAD] = rope(total[:, at : at + HEAD], cos[...], sin[...]).astype(BF16)
        kv[:, at + HEAD : at + 2 * HEAD] = total[:, at + HEAD : at + 2 * HEAD].astype(BF16)


def query_kernel(normed, weight, cos, sin, query):
    total = jnp.dot(normed[...], weight[...], preferred_element_type=F32)
    at = pl.multiple_of(pl.program_id(0) * 2 * HEAD, 2 * HEAD)
    for h in range(2):
        part = total[:, h * HEAD : (h + 1) * HEAD]
        turned = rope(part, cos[...], sin[...]) * (D // HEADS) ** (-0.5)
        query[:, pl.ds(at + h * HEAD, HEAD)] = turned.astype(BF16)


def attention_kernel(flat, query, *refs):
    kv = [refs[4 * k : 4 * k + 4] for k in range(4)]
    context, numer, denom = refs[16:]
    x, yl, c, _, _ = spot(flat)
    w = 2 * yl + c
    row = lax.broadcasted_iota(jnp.int32, (2 * BLOCK, BLOCK), 0) % BLOCK
    col = lax.broadcasted_iota(jnp.int32, (2 * BLOCK, BLOCK), 1)

    def chunk(first, dw, block, slot, masked):
        near, far = pl.ds(first, HEAD), pl.ds(first + HEAD, HEAD)
        if isinstance(block, int):
            q_rows, k_rows = pl.ds(block * BLOCK, BLOCK), pl.ds(slot * BLOCK, BLOCK)
        else:
            q_rows = pl.ds(pl.multiple_of(block * BLOCK, BLOCK), BLOCK)
            k_rows = pl.ds(pl.multiple_of(slot * BLOCK, BLOCK), BLOCK)
        q2 = jnp.concatenate([query[q_rows, near], query[q_rows, far]], axis=0)
        keys = jnp.concatenate([kv[dw][d][k_rows, near] for d in range(4)], axis=0)
        values = jnp.concatenate([kv[dw][d][k_rows, far] for d in range(4)], axis=0)
        score = lax.dot_general(q2, keys, (((1,), (1,)), ((), ())), preferred_element_type=F32)
        weight = jnp.exp(50.0 * jnp.tanh(score * (1.0 / 50.0)))
        parts = [weight[:, d * BLOCK : (d + 1) * BLOCK] for d in range(4)]
        if masked:
            parts = [jnp.where(col <= row, parts[0], 0.0)] + [
                jnp.where(x >= d, parts[d], 0.0) for d in range(1, 4)
            ]
            weight = jnp.concatenate(parts, axis=1)
        denom[block] += (parts[0] + parts[1]) + (parts[2] + parts[3])
        numer[block] += jnp.dot(weight.astype(BF16), values, preferred_element_type=F32)

    @pl.loop(0, 2)
    def _(head):
        first = pl.multiple_of(head * 2 * HEAD, 2 * HEAD)
        numer[...] = jnp.zeros_like(numer)
        denom[...] = jnp.zeros_like(denom)
        chunk(first, 0, 0, 0, True)
        chunk(first, 0, 1, 0, False)
        chunk(first, 0, 1, 1, True)
        for dw in range(1, 4):
            later = (jnp.bitwise_xor(w, dw) > w).astype(jnp.int32)
            chunk(first, dw, 1, 0, False)
            chunk(first, dw, later, later, False)
        for block in range(2):
            out = numer[block] / jnp.sum(denom[block], axis=1, keepdims=True)
            rows = slice(block * BLOCK, (block + 1) * BLOCK)
            context[rows, pl.ds(first, HEAD)] = out[:BLOCK].astype(BF16)
            context[rows, pl.ds(first + HEAD, HEAD)] = out[BLOCK:].astype(BF16)


def out_kernel(flat, context, weight, *refs):
    outs, (buffer, scratch, sems) = refs[:8], refs[8:]
    _, _, _, z, yh = spot(flat)
    tile, steps = scratch.shape[1], sems.shape[0]

    def copy(n):
        rows = pl.ds(pl.multiple_of(n * tile, tile), tile)
        source = weight.at[rows, 4 * HEAD :]
        return pltpu.make_async_copy(source, buffer.at[rows, :], sems.at[n])

    @pl.loop(0, steps)
    def _(n):
        copy(n).start()

    @pl.loop(0, steps)
    def _(n):
        copy(n).wait()
        cols = pl.ds(pl.multiple_of(n * tile, tile), tile)
        scratch[...] = lax.dot_general(
            context[...], buffer[cols, :], (((1,), (1,)), ((), ())), preferred_element_type=F32
        ).astype(BF16)
        for dy in range(2):
            for dz in range(4):
                first = jnp.bitwise_xor(yh, dy) * 64 + jnp.bitwise_and(z + dz, 3) * 16
                for block in range(2):
                    rows = pl.ds(pl.multiple_of(first + block * BLOCK, 16), 16)
                    outs[4 * dy + dz][block * 16 : block * 16 + 16, cols] = scratch[rows, :]


def finish_kernel(resident, gain, *refs):
    terms, out = refs[:8], refs[8]
    total = terms[0][...].astype(F32)
    for term in terms[1:]:
        total = total + term[...].astype(F32)
    scale = lax.rsqrt(jnp.mean(total * total, axis=1, keepdims=True) + EPS)
    out[...] = (resident[...].astype(F32) + total * scale * gain[...]).astype(BF16)


def before(blocks, shard):
    result = jnp.int32(0)
    for m in range(16):
        result = result + jnp.where(m < shard, blocks[m], 0)
    return result


def owner_kernel(flat, new_blocks, *refs):
    by_w, outs = refs[:4], refs[4:]
    x, yl, c, _, _ = spot(flat)
    w = 2 * yl + c
    jobs = []
    for d in range(4):
        start = before(new_blocks, 4 * jnp.bitwise_and(x + d, 3) + w)
        level = (start + jnp.bitwise_and(x - start, 3)) >> 2
        slot = (level >= 4).astype(jnp.int32)
        source = jnp.bitwise_and(jnp.where(level < 4, level, 7 - level), 3)
        row = pl.ds(pl.multiple_of(slot * 16, 16), 16)
        jobs.append((jnp.bitwise_xor(source, w), [part.at[row, :] for part in by_w], outs[d]))
    move(jobs)


def place_kernel(flat, new_blocks, *refs):
    gathered, outs = refs[:4], refs[4:]
    x, yl, c, z, _ = spot(flat)
    start = before(new_blocks, 4 * x + 2 * yl + c)
    move([(jnp.bitwise_and(x - start - (z + d), 3), gathered, outs[d]) for d in range(4)])


def close_kernel(flat, new_blocks, *refs):
    parts, out = refs[:4], refs[4]
    x, yl, c, z, _ = spot(flat)
    count = new_blocks[4 * x + 2 * yl + c]

    @pl.when(z >= count)
    def _():
        out[...] = jnp.zeros_like(out)

    @pl.when(z < count)
    def _():
        for d in range(4):
            row = pl.multiple_of(jnp.bitwise_and(z - d, 3) * 16, 16)
            out[pl.ds(row, 16), :] = parts[d][...]


def per_device(
    x_old, old_blocks, new_blocks, order, pre_gain, post_gain, w_query, w_key, w_value, w_out_t
):
    flat = lax.axis_index(AXES).astype(jnp.int32).reshape(1)
    width = x_old.shape[1]
    count = 2 * BLOCK

    def near_by(arrays):
        return [pltpu.with_memory_space_constraint(a, pltpu.VMEM) for a in arrays]

    def far_off(arrays):
        return [pltpu.with_memory_space_constraint(a, pltpu.HBM) for a in arrays]

    def call(kernel, tables, arrays, shapes):
        results = pl.pallas_call(
            kernel,
            in_specs=[SMEM] * (1 + len(tables)) + [VMEM] * len(arrays),
            out_specs=[VMEM] * len(shapes),
            out_shape=[pltpu.VMEM(s, BF16) for s in shapes],
            compiler_params=grant(8),
        )(flat, *tables, *near_by(arrays))
        return list(results)

    def bring(kernel, tables, arrays, shapes, copies, kind):
        results = pl.pallas_call(
            kernel,
            in_specs=[SMEM] * len(tables) + [AWAY] * len(arrays),
            out_specs=[VMEM] * len(shapes),
            out_shape=[kind(s, BF16) for s in shapes],
            scratch_shapes=[pltpu.SemaphoreType.DMA((copies,))],
            compiler_params=grant(8),
        )(*tables, *far_off(arrays))
        return list(results)

    def everywhere(part):
        opposite = shift(part, "x", 2)
        pair = shift(part, "yl", 1)
        same = [part, shift(part, "x", 1), opposite, shift(part, "x", 3)]
        other = [pair, shift(pair, "x", 1), shift(opposite, "yl", 1), shift(pair, "x", 3)]
        result = []
        for parts in (same, other):
            result += parts
            result += [shift(s, "c", 1) for s in parts]
        return result

    (joined,) = bring(
        join_kernel, (), (w_query, w_out_t), [(w_query.shape[0], 8 * HEAD)], 2, jax.ShapeDtypeStruct
    )
    joined_full = lax.all_gather(joined, SEQ, axis=0, tiled=True)

    old = far_off((old_blocks, order))
    near = bring(leave_kernel, (flat, *old), (x_old.T,), [(width, BLOCK)] * 4, 4, pltpu.VMEM)
    near = near[:1] + [shift(near[d], "x", d) for d in range(1, 4)]
    far = [shift(part, "c", 1) for part in near]
    mine, cross = call(sort_kernel, old, near + far, [(width, count)] * 2)
    (held,) = pl.pallas_call(
        hold_kernel,
        in_specs=[AWAY, AWAY, VMEM],
        out_specs=[VMEM],
        out_shape=[pltpu.VMEM((w_key.shape[0], 4 * HEAD), BF16)],
        scratch_shapes=[pltpu.SemaphoreType.DMA((4,))],
        compiler_params=grant(8),
        name="hold",
    )(*far_off((w_key, w_value)), *near_by((mine,)))
    spread_weights = everywhere(held)

    cross = shift(cross, "yl", 1)
    (rows,) = call(settle_kernel, old, (mine, cross), [(width, count)])

    facing = shift(rows, "yh", 1)
    pieces = [rows] + [shift(rows, "z", d) for d in range(1, 4)]
    pieces += [facing] + [shift(facing, "z", d) for d in range(1, 4)]

    slot_rows = jnp.arange(BLOCK, dtype=jnp.int32)
    x, w = flat[0] >> 5, (flat[0] >> 3) & 3
    positions = jnp.concatenate(
        [b * BLOCK + slot_rows for b in (x + 4 * w, x + 28 - 4 * w)]
    )
    inverse = jnp.exp(jnp.arange(HEAD // 2, dtype=F32) * (-2.0 * math.log(10000.0) / HEAD))
    angles = positions.astype(F32)[:, None] * inverse[None, :]
    cosine, sine = jnp.cos(angles), jnp.sin(angles)
    cosine = jnp.concatenate([cosine, cosine], axis=1)
    sine = jnp.concatenate([-sine, sine], axis=1)

    normed, resident = pl.pallas_call(
        norm_kernel,
        in_specs=[SMEM] + [VMEM] * 9,
        out_specs=[VMEM] * 2,
        out_shape=[pltpu.VMEM((count, D), BF16), pltpu.VMEM((32, D), BF16)],
        scratch_shapes=[pltpu.VMEM((D, count), BF16), pltpu.VMEM((count, D), BF16)],
        compiler_params=grant(24),
        name="norm",
    )(flat, *near_by(pieces), pre_gain.reshape(1, D))
    tables = near_by((cosine, sine))

    def heads(kernel, first):
        return pl.pallas_call(
            kernel,
            grid=(2,),
            in_specs=[VMEM, pl.BlockSpec((D, 2 * HEAD), lambda n: (0, n + first)), VMEM, VMEM],
            out_specs=VMEM,
            out_shape=pltpu.VMEM((count, 4 * HEAD), BF16),
            compiler_params=grant(24),
        )(*near_by((normed,)), *far_off((joined_full,)), *tables)

    (kv_weights,) = call(pack_kernel, (), spread_weights, [(D, 4 * HEAD)])
    kv = pl.pallas_call(
        key_value_kernel,
        in_specs=[VMEM] * 4,
        out_specs=VMEM,
        out_shape=pltpu.VMEM((count, 4 * HEAD), BF16),
        compiler_params=grant(16),
        name="key_value",
    )(*near_by((normed, kv_weights)), *tables)

    spread = everywhere(kv)

    query = heads(query_kernel, 0)
    context = pl.pallas_call(
        attention_kernel,
        in_specs=[SMEM] + [VMEM] * 17,
        out_specs=VMEM,
        out_shape=pltpu.VMEM((count, 4 * HEAD), BF16),
        scratch_shapes=[pltpu.VMEM((2, 2 * BLOCK, HEAD), F32), pltpu.VMEM((2, 2 * BLOCK, HEAD), F32)],
        compiler_params=grant(24),
        name="attention",
    )(flat, *near_by((query, *spread)))

    tile = 512
    shares = pl.pallas_call(
        out_kernel,
        in_specs=[SMEM, VMEM, AWAY],
        out_specs=[VMEM] * 8,
        out_shape=[pltpu.VMEM((32, D), BF16)] * 8,
        scratch_shapes=[
            pltpu.VMEM((D, 4 * HEAD), BF16),
            pltpu.VMEM((count, tile), BF16),
            pltpu.SemaphoreType.DMA((D // tile,)),
        ],
        compiler_params=grant(16),
        name="project",
    )(flat, *near_by((context,)), *far_off((joined_full,)))
    received = []
    for dy in range(2):
        for dz in range(4):
            part = shares[4 * dy + dz]
            if dy and dz:
                n = [(i, j) for i in range(4) for j in range(2)]
                part = lax.ppermute(
                    part, TP, [(2 * i + j, 2 * ((i + dz) % 4) + (j ^ dy)) for i, j in n]
                )
            elif dy:
                part = shift(part, "yh", 1)
            elif dz:
                part = shift(part, "z", dz)
            received.append(part)

    refreshed = pl.pallas_call(
        finish_kernel,
        in_specs=[VMEM] * 10,
        out_specs=VMEM,
        out_shape=pltpu.VMEM((32, D), BF16),
        compiler_params=grant(8),
        name="finish",
    )(*near_by((resident, post_gain.reshape(1, D), *received)))

    by_yl = shift(refreshed, "yl", 1)
    by_w = [refreshed, shift(refreshed, "c", 1), by_yl, shift(by_yl, "c", 1)]
    new = far_off((new_blocks,))
    slices = [(16, D)] * 4
    gathered = call(owner_kernel, new, by_w, slices)
    gathered = gathered[:1] + [shift(gathered[d], "x", d) for d in range(1, 4)]
    final = call(place_kernel, new, gathered, slices)
    final = final[:1] + [shift(final[d], "z", d) for d in range(1, 4)]
    (layer_out,) = call(close_kernel, new, final, [(64, D)])
    return layer_out


def solution(mesh):
    torus = Mesh(mesh.devices.reshape(4, 2, 2, 4, 2), AXES)
    in_specs = (
        P(SEQ, TP),
        P(),
        P(),
        P(),
        P(),
        P(),
        P(SEQ, TP),
        P(SEQ, TP),
        P(SEQ, TP),
        P(SEQ, TP),
    )
    out_specs = P(SEQ + TP, None)

    return jax.shard_map(
        per_device, mesh=torus, in_specs=in_specs, out_specs=out_specs, check_vma=False
    )
```

```python
import math

import jax
import jax.numpy as jnp
from jax import lax
from jax.experimental import pallas as pl
from jax.experimental.pallas import tpu as pltpu
from jax.sharding import Mesh
from jax.sharding import PartitionSpec as P

D = 4608
HEADS = 32
HEAD = 128
BLOCK = 128
EPS = 1e-06
F32 = jnp.float32
BF16 = jnp.bfloat16

AXES = ("x", "yl", "c", "z", "yh")
SEQ = ("x", "yl", "c")
TP = ("z", "yh")


SMEM = pl.BlockSpec(memory_space=pltpu.SMEM)


def shift(value, axis, by):
    n = lax.axis_size(axis)
    return lax.ppermute(value, axis, [(i, (i + by) % n) for i in range(n)])


def rope(values, cos, sin):
    half = HEAD // 2
    swapped = jnp.concatenate([values[:, half:], values[:, :half]], axis=1)
    return values * cos + swapped * sin


def spot(flat):
    me = flat[0]
    return me >> 5, (me >> 4) & 1, (me >> 3) & 1, (me >> 1) & 3, me & 1


def starts(blocks):
    result, so_far = [], jnp.int32(0)
    for m in range(16):
        result.append(so_far)
        so_far = so_far + blocks[m]
    return result


VMEM = pl.BlockSpec(memory_space=pltpu.VMEM)
AWAY = pl.BlockSpec(memory_space=pl.ANY)


def grant(mib):
    return pltpu.CompilerParams(vmem_limit_bytes=mib << 20)


def move(jobs):
    for index, sources, target in jobs:
        for k, source in enumerate(sources):

            def copy(source=source, target=target):
                target[...] = source[...]

            if len(sources) == 1:
                copy()
            else:
                pl.when(index == k)(copy)


def lanes(first):
    return pl.ds(pl.multiple_of(first, BLOCK), BLOCK)


def fetch(jobs, sems):
    copies = [pltpu.make_async_copy(s, t, sems.at[n]) for n, (s, t) in enumerate(jobs)]
    for copy in copies:
        copy.start()
    for copy in copies:
        copy.wait()


def join_kernel(query, out_t, joined, sems):
    half = 4 * HEAD
    fetch([(query, joined.at[:, :half]), (out_t, joined.at[:, half:])], sems)


def hold_kernel(key, value, held, sems):
    jobs = []
    for n, source in enumerate((key, value, key, value)):
        first = n // 2 * HEAD
        jobs.append((source.at[:, first : first + HEAD], held.at[:, n * HEAD : (n + 1) * HEAD]))
    fetch(jobs, sems)


def pack_kernel(flat, *refs):
    parts, whole = refs[:16], refs[16]
    x, yl, c, _, _ = spot(flat)
    size = parts[0].shape[0]
    for n, part in enumerate(parts):
        w = jnp.bitwise_xor(2 * yl + c, n // 4)
        first = (4 * jnp.bitwise_and(x - n % 4, 3) + w) * size
        whole[pl.ds(pl.multiple_of(first, 32), size), :] = part[...]


def leave_kernel(flat, old_blocks, order, x_old, *refs):
    outs, sems = refs[:4], refs[4]
    x, yl, c, _, _ = spot(flat)
    shard = order[4 * x + 2 * yl + c]
    first = jnp.int32(0)
    for m in range(16):
        first = first + jnp.where(m < shard, old_blocks[m], 0)
    jobs = []
    for d in range(4):
        row = jnp.bitwise_and(x + d - first, 3) * BLOCK
        jobs.append((x_old.at[:, lanes(row)], outs[d]))
    fetch(jobs, sems)


def holders(old_blocks, order, blocks):
    begin = starts(old_blocks)
    result = []
    for block in blocks:
        shard = jnp.int32(-1)
        for m in range(16):
            shard = shard + (begin[m] <= block).astype(jnp.int32)
        holder = jnp.int32(0)
        for m in range(16):
            holder = holder + jnp.where(order[m] == shard, m, 0)
        result.append(holder)
    return result


def targets(x, yl, c):
    to = 2 * yl + c
    return [x + 4 * to, x + 28 - 4 * to]


def sort_kernel(flat, old_blocks, order, *refs):
    sources, (mine, cross) = refs[:8], refs[8:]
    x, yl, c, _, _ = spot(flat)
    blocks = targets(x, yl, c) + targets(x, 1 - yl, c)
    jobs = []
    for n, holder in enumerate(holders(old_blocks, order, blocks)):
        index = jnp.bitwise_and(x - (holder >> 2), 3) + 4 * jnp.bitwise_xor(holder & 1, c)
        out, at = (mine, n) if n < 2 else (cross, n - 2)
        jobs.append((index, sources, out.at[:, at * BLOCK : (at + 1) * BLOCK]))
    move(jobs)


def settle_kernel(flat, old_blocks, order, mine, crossed, rows):
    x, yl, c, _, _ = spot(flat)
    jobs = []
    for n, holder in enumerate(holders(old_blocks, order, targets(x, yl, c))):
        at = slice(n * BLOCK, (n + 1) * BLOCK)
        index = jnp.bitwise_xor((holder >> 1) & 1, yl)
        jobs.append((index, [mine.at[:, at], crossed.at[:, at]], rows.at[:, at]))
    move(jobs)


def norm_kernel(flat, *refs):
    pieces, (gain, normed, resident, features, raw) = refs[:8], refs[8:]
    _, _, _, z, yh = spot(flat)
    width, count = pieces[0].shape
    total = jnp.zeros((1, count), F32)
    for n, piece in enumerate(pieces):
        wide = piece[...].astype(F32)
        total = total + jnp.sum(wide * wide, axis=0, keepdims=True)
        t = 2 * jnp.bitwise_and(z - n % 4, 3) + jnp.bitwise_xor(yh, n // 4)
        features[pl.ds(pl.multiple_of(t * width, 64), width), :] = piece[...]
    scale = lax.rsqrt(total / D + EPS)
    scale = jnp.transpose(jnp.broadcast_to(scale, (BLOCK, count)))
    step = 512
    for at in range(0, D, step):
        rows = jnp.transpose(features[at : at + step, :])
        raw[:, at : at + step] = rows
        for k in range(0, step, BLOCK):
            cols = slice(at + k, at + k + BLOCK)
            wide = rows[:, k : k + BLOCK].astype(F32) * scale * gain[:, cols]
            normed[:, cols] = wide.astype(BF16)
    first = pl.multiple_of(64 * yh + 16 * z, 16)
    for block in range(2):
        source = pl.ds(pl.multiple_of(first + block * BLOCK, 16), 16)
        resident[block * 16 : block * 16 + 16, :] = raw[source, :]


def key_value_kernel(normed, weight, cos, sin, kv):
    total = jnp.dot(normed[...], weight[...], preferred_element_type=F32)
    for h in range(2):
        at = 2 * h * HEAD
        kv[:, at : at + HEAD] = rope(total[:, at : at + HEAD], cos[...], sin[...]).astype(BF16)
        kv[:, at + HEAD : at + 2 * HEAD] = total[:, at + HEAD : at + 2 * HEAD].astype(BF16)


def query_kernel(normed, weight, cos, sin, query):
    total = jnp.dot(normed[...], weight[...], preferred_element_type=F32)
    at = pl.multiple_of(pl.program_id(0) * 2 * HEAD, 2 * HEAD)
    for h in range(2):
        part = total[:, h * HEAD : (h + 1) * HEAD]
        turned = rope(part, cos[...], sin[...]) * (D // HEADS) ** (-0.5)
        query[:, pl.ds(at + h * HEAD, HEAD)] = turned.astype(BF16)


def attention_kernel(flat, query, *refs):
    kv = [refs[4 * k : 4 * k + 4] for k in range(4)]
    context, numer, denom = refs[16:]
    x, yl, c, _, _ = spot(flat)
    w = 2 * yl + c
    row = lax.broadcasted_iota(jnp.int32, (2 * BLOCK, BLOCK), 0) % BLOCK
    col = lax.broadcasted_iota(jnp.int32, (2 * BLOCK, BLOCK), 1)

    def chunk(first, dw, block, slot, masked):
        near, far = pl.ds(first, HEAD), pl.ds(first + HEAD, HEAD)
        if isinstance(block, int):
            q_rows, k_rows = pl.ds(block * BLOCK, BLOCK), pl.ds(slot * BLOCK, BLOCK)
        else:
            q_rows = pl.ds(pl.multiple_of(block * BLOCK, BLOCK), BLOCK)
            k_rows = pl.ds(pl.multiple_of(slot * BLOCK, BLOCK), BLOCK)
        q2 = jnp.concatenate([query[q_rows, near], query[q_rows, far]], axis=0)
        keys = jnp.concatenate([kv[dw][d][k_rows, near] for d in range(4)], axis=0)
        values = jnp.concatenate([kv[dw][d][k_rows, far] for d in range(4)], axis=0)
        score = lax.dot_general(q2, keys, (((1,), (1,)), ((), ())), preferred_element_type=F32)
        weight = jnp.exp(50.0 * jnp.tanh(score * (1.0 / 50.0)))
        parts = [weight[:, d * BLOCK : (d + 1) * BLOCK] for d in range(4)]
        if masked:
            parts = [jnp.where(col <= row, parts[0], 0.0)] + [
                jnp.where(x >= d, parts[d], 0.0) for d in range(1, 4)
            ]
            weight = jnp.concatenate(parts, axis=1)
        denom[block] += (parts[0] + parts[1]) + (parts[2] + parts[3])
        numer[block] += jnp.dot(weight.astype(BF16), values, preferred_element_type=F32)

    @pl.loop(0, 2)
    def _(head):
        first = pl.multiple_of(head * 2 * HEAD, 2 * HEAD)
        numer[...] = jnp.zeros_like(numer)
        denom[...] = jnp.zeros_like(denom)
        chunk(first, 0, 0, 0, True)
        chunk(first, 0, 1, 0, False)
        chunk(first, 0, 1, 1, True)
        for dw in range(1, 4):
            later = (jnp.bitwise_xor(w, dw) > w).astype(jnp.int32)
            chunk(first, dw, 1, 0, False)
            chunk(first, dw, later, later, False)
        for block in range(2):
            out = numer[block] / jnp.sum(denom[block], axis=1, keepdims=True)
            rows = slice(block * BLOCK, (block + 1) * BLOCK)
            context[rows, pl.ds(first, HEAD)] = out[:BLOCK].astype(BF16)
            context[rows, pl.ds(first + HEAD, HEAD)] = out[BLOCK:].astype(BF16)


def out_kernel(flat, context, weight, *refs):
    outs, (buffer, scratch, sems) = refs[:8], refs[8:]
    _, _, _, z, yh = spot(flat)
    tile, steps = scratch.shape[1], sems.shape[0]

    def copy(n):
        rows = pl.ds(pl.multiple_of(n * tile, tile), tile)
        source = weight.at[rows, 4 * HEAD :]
        return pltpu.make_async_copy(source, buffer.at[rows, :], sems.at[n])

    @pl.loop(0, steps)
    def _(n):
        copy(n).start()

    @pl.loop(0, steps)
    def _(n):
        copy(n).wait()
        cols = pl.ds(pl.multiple_of(n * tile, tile), tile)
        scratch[...] = lax.dot_general(
            context[...], buffer[cols, :], (((1,), (1,)), ((), ())), preferred_element_type=F32
        ).astype(BF16)
        for dy in range(2):
            for dz in range(4):
                first = jnp.bitwise_xor(yh, dy) * 64 + jnp.bitwise_and(z + dz, 3) * 16
                for block in range(2):
                    rows = pl.ds(pl.multiple_of(first + block * BLOCK, 16), 16)
                    outs[4 * dy + dz][block * 16 : block * 16 + 16, cols] = scratch[rows, :]


def finish_kernel(resident, gain, *refs):
    terms, out = refs[:8], refs[8]
    total = terms[0][...].astype(F32)
    for term in terms[1:]:
        total = total + term[...].astype(F32)
    scale = lax.rsqrt(jnp.mean(total * total, axis=1, keepdims=True) + EPS)
    out[...] = (resident[...].astype(F32) + total * scale * gain[...]).astype(BF16)


def before(blocks, shard):
    result = jnp.int32(0)
    for m in range(16):
        result = result + jnp.where(m < shard, blocks[m], 0)
    return result


def owner_kernel(flat, new_blocks, *refs):
    by_w, outs = refs[:4], refs[4:]
    x, yl, c, _, _ = spot(flat)
    w = 2 * yl + c
    jobs = []
    for d in range(4):
        start = before(new_blocks, 4 * jnp.bitwise_and(x + d, 3) + w)
        level = (start + jnp.bitwise_and(x - start, 3)) >> 2
        slot = (level >= 4).astype(jnp.int32)
        source = jnp.bitwise_and(jnp.where(level < 4, level, 7 - level), 3)
        row = pl.ds(pl.multiple_of(slot * 16, 16), 16)
        jobs.append((jnp.bitwise_xor(source, w), [part.at[row, :] for part in by_w], outs[d]))
    move(jobs)


def place_kernel(flat, new_blocks, *refs):
    gathered, outs = refs[:4], refs[4:]
    x, yl, c, z, _ = spot(flat)
    start = before(new_blocks, 4 * x + 2 * yl + c)
    move([(jnp.bitwise_and(x - start - (z + d), 3), gathered, outs[d]) for d in range(4)])


def close_kernel(flat, new_blocks, *refs):
    parts, out = refs[:4], refs[4]
    x, yl, c, z, _ = spot(flat)
    count = new_blocks[4 * x + 2 * yl + c]

    @pl.when(z >= count)
    def _():
        out[...] = jnp.zeros_like(out)

    @pl.when(z < count)
    def _():
        for d in range(4):
            row = pl.multiple_of(jnp.bitwise_and(z - d, 3) * 16, 16)
            out[pl.ds(row, 16), :] = parts[d][...]


def per_device(
    x_old, old_blocks, new_blocks, order, pre_gain, post_gain, w_query, w_key, w_value, w_out_t
):
    flat = lax.axis_index(AXES).astype(jnp.int32).reshape(1)
    width = x_old.shape[1]
    count = 2 * BLOCK

    def near_by(arrays):
        return [pltpu.with_memory_space_constraint(a, pltpu.VMEM) for a in arrays]

    def far_off(arrays):
        return [pltpu.with_memory_space_constraint(a, pltpu.HBM) for a in arrays]

    def call(kernel, tables, arrays, shapes):
        results = pl.pallas_call(
            kernel,
            in_specs=[SMEM] * (1 + len(tables)) + [VMEM] * len(arrays),
            out_specs=[VMEM] * len(shapes),
            out_shape=[pltpu.VMEM(s, BF16) for s in shapes],
            compiler_params=grant(8),
        )(flat, *tables, *near_by(arrays))
        return list(results)

    def bring(kernel, tables, arrays, shapes, copies, kind):
        results = pl.pallas_call(
            kernel,
            in_specs=[SMEM] * len(tables) + [AWAY] * len(arrays),
            out_specs=[VMEM] * len(shapes),
            out_shape=[kind(s, BF16) for s in shapes],
            scratch_shapes=[pltpu.SemaphoreType.DMA((copies,))],
            compiler_params=grant(8),
        )(*tables, *far_off(arrays))
        return list(results)

    def everywhere(part):
        opposite = shift(part, "x", 2)
        pair = shift(part, "yl", 1)
        same = [part, shift(part, "x", 1), opposite, shift(part, "x", 3)]
        other = [pair, shift(pair, "x", 1), shift(opposite, "yl", 1), shift(pair, "x", 3)]
        result = []
        for parts in (same, other):
            result += parts
            result += [shift(s, "c", 1) for s in parts]
        return result

    (joined,) = bring(
        join_kernel, (), (w_query, w_out_t), [(w_query.shape[0], 8 * HEAD)], 2, jax.ShapeDtypeStruct
    )
    joined_full = lax.all_gather(joined, SEQ, axis=0, tiled=True)

    (held,) = bring(hold_kernel, (), (w_key, w_value), [(w_key.shape[0], 4 * HEAD)], 4, pltpu.VMEM)
    pair = shift(held, "yl", 1)

    old = far_off((old_blocks, order))
    near = bring(leave_kernel, (flat, *old), (x_old.T,), [(width, BLOCK)] * 4, 4, pltpu.VMEM)
    near = near[:1] + [shift(near[d], "x", d) for d in range(1, 4)]
    far = [shift(part, "c", 1) for part in near]
    mine, cross = call(sort_kernel, old, near + far, [(width, count)] * 2)
    same = [held] + [shift(held, "x", d) for d in range(1, 4)]
    other = [pair] + [shift(pair, "x", d) for d in range(1, 4)]
    spread_weights = [
        w
        for parts in (same, other)
        for w in parts + [shift(s, "c", 1) for s in parts]
    ]

    cross = shift(cross, "yl", 1)
    (rows,) = call(settle_kernel, old, (mine, cross), [(width, count)])

    facing = shift(rows, "yh", 1)
    pieces = [rows] + [shift(rows, "z", d) for d in range(1, 4)]
    pieces += [facing] + [shift(facing, "z", d) for d in range(1, 4)]

    slot_rows = jnp.arange(BLOCK, dtype=jnp.int32)
    x, w = flat[0] >> 5, (flat[0] >> 3) & 3
    positions = jnp.concatenate(
        [b * BLOCK + slot_rows for b in (x + 4 * w, x + 28 - 4 * w)]
    )
    inverse = jnp.exp(jnp.arange(HEAD // 2, dtype=F32) * (-2.0 * math.log(10000.0) / HEAD))
    angles = positions.astype(F32)[:, None] * inverse[None, :]
    cosine, sine = jnp.cos(angles), jnp.sin(angles)
    cosine = jnp.concatenate([cosine, cosine], axis=1)
    sine = jnp.concatenate([-sine, sine], axis=1)

    normed, resident = pl.pallas_call(
        norm_kernel,
        in_specs=[SMEM] + [VMEM] * 9,
        out_specs=[VMEM] * 2,
        out_shape=[pltpu.VMEM((count, D), BF16), pltpu.VMEM((32, D), BF16)],
        scratch_shapes=[pltpu.VMEM((D, count), BF16), pltpu.VMEM((count, D), BF16)],
        compiler_params=grant(24),
        name="norm",
    )(flat, *near_by(pieces), pre_gain.reshape(1, D))
    tables = near_by((cosine, sine))

    def heads(kernel, first):
        return pl.pallas_call(
            kernel,
            grid=(2,),
            in_specs=[VMEM, pl.BlockSpec((D, 2 * HEAD), lambda n: (0, n + first)), VMEM, VMEM],
            out_specs=VMEM,
            out_shape=pltpu.VMEM((count, 4 * HEAD), BF16),
            compiler_params=grant(24),
        )(*near_by((normed,)), *far_off((joined_full,)), *tables)

    (kv_weights,) = call(pack_kernel, (), spread_weights, [(D, 4 * HEAD)])
    kv = pl.pallas_call(
        key_value_kernel,
        in_specs=[VMEM] * 4,
        out_specs=VMEM,
        out_shape=pltpu.VMEM((count, 4 * HEAD), BF16),
        compiler_params=grant(16),
        name="key_value",
    )(*near_by((normed, kv_weights)), *tables)

    spread = everywhere(kv)

    query = heads(query_kernel, 0)
    context = pl.pallas_call(
        attention_kernel,
        in_specs=[SMEM] + [VMEM] * 17,
        out_specs=VMEM,
        out_shape=pltpu.VMEM((count, 4 * HEAD), BF16),
        scratch_shapes=[pltpu.VMEM((2, 2 * BLOCK, HEAD), F32), pltpu.VMEM((2, 2 * BLOCK, HEAD), F32)],
        compiler_params=grant(24),
        name="attention",
    )(flat, *near_by((query, *spread)))

    tile = 512
    shares = pl.pallas_call(
        out_kernel,
        in_specs=[SMEM, VMEM, AWAY],
        out_specs=[VMEM] * 8,
        out_shape=[pltpu.VMEM((32, D), BF16)] * 8,
        scratch_shapes=[
            pltpu.VMEM((D, 4 * HEAD), BF16),
            pltpu.VMEM((count, tile), BF16),
            pltpu.SemaphoreType.DMA((D // tile,)),
        ],
        compiler_params=grant(16),
        name="project",
    )(flat, *near_by((context,)), *far_off((joined_full,)))
    received = []
    for dy in range(2):
        for dz in range(4):
            part = shares[4 * dy + dz]
            if dy and dz:
                n = [(i, j) for i in range(4) for j in range(2)]
                part = lax.ppermute(
                    part, TP, [(2 * i + j, 2 * ((i + dz) % 4) + (j ^ dy)) for i, j in n]
                )
            elif dy:
                part = shift(part, "yh", 1)
            elif dz:
                part = shift(part, "z", dz)
            received.append(part)

    refreshed = pl.pallas_call(
        finish_kernel,
        in_specs=[VMEM] * 10,
        out_specs=VMEM,
        out_shape=pltpu.VMEM((32, D), BF16),
        compiler_params=grant(8),
        name="finish",
    )(*near_by((resident, post_gain.reshape(1, D), *received)))

    by_yl = shift(refreshed, "yl", 1)
    by_w = [refreshed, shift(refreshed, "c", 1), by_yl, shift(by_yl, "c", 1)]
    new = far_off((new_blocks,))
    slices = [(16, D)] * 4
    gathered = call(owner_kernel, new, by_w, slices)
    gathered = gathered[:1] + [shift(gathered[d], "x", d) for d in range(1, 4)]
    final = call(place_kernel, new, gathered, slices)
    final = final[:1] + [shift(final[d], "z", d) for d in range(1, 4)]
    (layer_out,) = call(close_kernel, new, final, [(64, D)])
    return layer_out


def solution(mesh):
    torus = Mesh(mesh.devices.reshape(4, 2, 2, 4, 2), AXES)
    in_specs = (
        P(SEQ, TP),
        P(),
        P(),
        P(),
        P(),
        P(),
        P(SEQ, TP),
        P(SEQ, TP),
        P(SEQ, TP),
        P(SEQ, TP),
    )
    out_specs = P(SEQ + TP, None)

    return jax.shard_map(
        per_device, mesh=torus, in_specs=in_specs, out_specs=out_specs, check_vma=False
    )
```

```python
import math

import jax
import jax.numpy as jnp
from jax import lax
from jax.experimental import pallas as pl
from jax.experimental.pallas import tpu as pltpu
from jax.sharding import Mesh
from jax.sharding import PartitionSpec as P

D = 4608
HEADS = 32
HEAD = 128
BLOCK = 128
EPS = 1e-06
F32 = jnp.float32
BF16 = jnp.bfloat16

AXES = ("x", "yl", "c", "z", "yh")
SEQ = ("x", "yl", "c")
TP = ("z", "yh")


SMEM = pl.BlockSpec(memory_space=pltpu.SMEM)


def shift(value, axis, by):
    n = lax.axis_size(axis)
    return lax.ppermute(value, axis, [(i, (i + by) % n) for i in range(n)])


def rope(values, cos, sin):
    half = HEAD // 2
    swapped = jnp.concatenate([values[:, half:], values[:, :half]], axis=1)
    return values * cos + swapped * sin


def spot(flat):
    me = flat[0]
    return me >> 5, (me >> 4) & 1, (me >> 3) & 1, (me >> 1) & 3, me & 1


def starts(blocks):
    result, so_far = [], jnp.int32(0)
    for m in range(16):
        result.append(so_far)
        so_far = so_far + blocks[m]
    return result


VMEM = pl.BlockSpec(memory_space=pltpu.VMEM)
AWAY = pl.BlockSpec(memory_space=pl.ANY)


def grant(mib):
    return pltpu.CompilerParams(vmem_limit_bytes=mib << 20)


def move(jobs):
    for index, sources, target in jobs:
        for k, source in enumerate(sources):

            def copy(source=source, target=target):
                target[...] = source[...]

            if len(sources) == 1:
                copy()
            else:
                pl.when(index == k)(copy)


def lanes(first):
    return pl.ds(pl.multiple_of(first, BLOCK), BLOCK)


def fetch(jobs, sems):
    copies = [pltpu.make_async_copy(s, t, sems.at[n]) for n, (s, t) in enumerate(jobs)]
    for copy in copies:
        copy.start()
    for copy in copies:
        copy.wait()


def pack_kernel(flat, *refs):
    parts, whole = refs[:16], refs[16]
    x, yl, c, _, _ = spot(flat)
    size = parts[0].shape[0]
    for n, part in enumerate(parts):
        w = jnp.bitwise_xor(2 * yl + c, n // 4)
        first = (4 * jnp.bitwise_and(x - n % 4, 3) + w) * size
        whole[pl.ds(pl.multiple_of(first, 32), size), :] = part[...]


def before(blocks, shard):
    result = jnp.int32(0)
    for m in range(16):
        result = result + jnp.where(m < shard, blocks[m], 0)
    return result


def leave_kernel(flat, old_blocks, order, key, value, query, out_t, x_old, *refs):
    joined, held, outs, sems = refs[0], refs[1], refs[2:6], refs[6]
    x, yl, c, _, _ = spot(flat)
    half = 4 * HEAD
    jobs = [(query, joined.at[:, :half]), (out_t, joined.at[:, half:])]
    for n, source in enumerate((key, value, key, value)):
        first = n // 2 * HEAD
        jobs.append((source.at[:, first : first + HEAD], held.at[:, n * HEAD : (n + 1) * HEAD]))
    first = before(old_blocks, order[4 * x + 2 * yl + c])
    for d in range(4):
        row = jnp.bitwise_and(x + d - first, 3) * BLOCK
        jobs.append((x_old.at[:, lanes(row)], outs[d]))
    fetch(jobs, sems)


def holders(old_blocks, order, blocks):
    begin = starts(old_blocks)
    result = []
    for block in blocks:
        shard = jnp.int32(-1)
        for m in range(16):
            shard = shard + (begin[m] <= block).astype(jnp.int32)
        holder = jnp.int32(0)
        for m in range(16):
            holder = holder + jnp.where(order[m] == shard, m, 0)
        result.append(holder)
    return result


def targets(x, yl, c):
    to = 2 * yl + c
    return [x + 4 * to, x + 28 - 4 * to]


def sort_kernel(flat, old_blocks, order, *refs):
    sources, (mine, cross) = refs[:8], refs[8:]
    x, yl, c, _, _ = spot(flat)
    blocks = targets(x, yl, c) + targets(x, 1 - yl, c)
    jobs = []
    for n, holder in enumerate(holders(old_blocks, order, blocks)):
        index = jnp.bitwise_and(x - (holder >> 2), 3) + 4 * jnp.bitwise_xor(holder & 1, c)
        out, at = (mine, n) if n < 2 else (cross, n - 2)
        jobs.append((index, sources, out.at[:, at * BLOCK : (at + 1) * BLOCK]))
    move(jobs)


def settle_kernel(flat, old_blocks, order, mine, crossed, rows):
    x, yl, c, _, _ = spot(flat)
    jobs = []
    for n, holder in enumerate(holders(old_blocks, order, targets(x, yl, c))):
        at = slice(n * BLOCK, (n + 1) * BLOCK)
        index = jnp.bitwise_xor((holder >> 1) & 1, yl)
        jobs.append((index, [mine.at[:, at], crossed.at[:, at]], rows.at[:, at]))
    move(jobs)


def norm_kernel(flat, *refs):
    pieces, (gain, normed, resident, features, raw) = refs[:8], refs[8:]
    _, _, _, z, yh = spot(flat)
    width, count = pieces[0].shape
    total = jnp.zeros((1, count), F32)
    for n, piece in enumerate(pieces):
        wide = piece[...].astype(F32)
        total = total + jnp.sum(wide * wide, axis=0, keepdims=True)
        t = 2 * jnp.bitwise_and(z - n % 4, 3) + jnp.bitwise_xor(yh, n // 4)
        features[pl.ds(pl.multiple_of(t * width, 64), width), :] = piece[...]
    scale = lax.rsqrt(total / D + EPS)
    scale = jnp.transpose(jnp.broadcast_to(scale, (BLOCK, count)))
    step = 512
    for at in range(0, D, step):
        rows = jnp.transpose(features[at : at + step, :])
        raw[:, at : at + step] = rows
        for k in range(0, step, BLOCK):
            cols = slice(at + k, at + k + BLOCK)
            wide = rows[:, k : k + BLOCK].astype(F32) * scale * gain[:, cols]
            normed[:, cols] = wide.astype(BF16)
    first = pl.multiple_of(64 * yh + 16 * z, 16)
    for block in range(2):
        source = pl.ds(pl.multiple_of(first + block * BLOCK, 16), 16)
        resident[block * 16 : block * 16 + 16, :] = raw[source, :]


def key_value_kernel(normed, weight, cos, sin, kv):
    total = jnp.dot(normed[...], weight[...], preferred_element_type=F32)
    for h in range(2):
        at = 2 * h * HEAD
        kv[:, at : at + HEAD] = rope(total[:, at : at + HEAD], cos[...], sin[...]).astype(BF16)
        kv[:, at + HEAD : at + 2 * HEAD] = total[:, at + HEAD : at + 2 * HEAD].astype(BF16)


def query_kernel(normed, weight, cos, sin, query):
    total = jnp.dot(normed[...], weight[...], preferred_element_type=F32)
    at = pl.multiple_of(pl.program_id(0) * 2 * HEAD, 2 * HEAD)
    for h in range(2):
        part = total[:, h * HEAD : (h + 1) * HEAD]
        turned = rope(part, cos[...], sin[...]) * (D // HEADS) ** (-0.5)
        query[:, pl.ds(at + h * HEAD, HEAD)] = turned.astype(BF16)


def attention_kernel(flat, query, *refs):
    kv = [refs[4 * k : 4 * k + 4] for k in range(4)]
    context, numer, denom = refs[16:]
    x, yl, c, _, _ = spot(flat)
    w = 2 * yl + c
    row = lax.broadcasted_iota(jnp.int32, (2 * BLOCK, BLOCK), 0) % BLOCK
    col = lax.broadcasted_iota(jnp.int32, (2 * BLOCK, BLOCK), 1)

    def chunk(first, dw, block, slot, masked):
        near, far = pl.ds(first, HEAD), pl.ds(first + HEAD, HEAD)
        if isinstance(block, int):
            q_rows, k_rows = pl.ds(block * BLOCK, BLOCK), pl.ds(slot * BLOCK, BLOCK)
        else:
            q_rows = pl.ds(pl.multiple_of(block * BLOCK, BLOCK), BLOCK)
            k_rows = pl.ds(pl.multiple_of(slot * BLOCK, BLOCK), BLOCK)
        q2 = jnp.concatenate([query[q_rows, near], query[q_rows, far]], axis=0)
        keys = jnp.concatenate([kv[dw][d][k_rows, near] for d in range(4)], axis=0)
        values = jnp.concatenate([kv[dw][d][k_rows, far] for d in range(4)], axis=0)
        score = lax.dot_general(q2, keys, (((1,), (1,)), ((), ())), preferred_element_type=F32)
        weight = jnp.exp(50.0 * jnp.tanh(score * (1.0 / 50.0)))
        parts = [weight[:, d * BLOCK : (d + 1) * BLOCK] for d in range(4)]
        if masked:
            parts = [jnp.where(col <= row, parts[0], 0.0)] + [
                jnp.where(x >= d, parts[d], 0.0) for d in range(1, 4)
            ]
            weight = jnp.concatenate(parts, axis=1)
        denom[block] += (parts[0] + parts[1]) + (parts[2] + parts[3])
        numer[block] += jnp.dot(weight.astype(BF16), values, preferred_element_type=F32)

    @pl.loop(0, 2)
    def _(head):
        first = pl.multiple_of(head * 2 * HEAD, 2 * HEAD)
        numer[...] = jnp.zeros_like(numer)
        denom[...] = jnp.zeros_like(denom)
        chunk(first, 0, 0, 0, True)
        chunk(first, 0, 1, 0, False)
        chunk(first, 0, 1, 1, True)
        for dw in range(1, 4):
            later = (jnp.bitwise_xor(w, dw) > w).astype(jnp.int32)
            chunk(first, dw, 1, 0, False)
            chunk(first, dw, later, later, False)
        for block in range(2):
            out = numer[block] / jnp.sum(denom[block], axis=1, keepdims=True)
            rows = slice(block * BLOCK, (block + 1) * BLOCK)
            context[rows, pl.ds(first, HEAD)] = out[:BLOCK].astype(BF16)
            context[rows, pl.ds(first + HEAD, HEAD)] = out[BLOCK:].astype(BF16)


def out_kernel(flat, context, weight, *refs):
    outs, (buffer, scratch, sems) = refs[:8], refs[8:]
    _, _, _, z, yh = spot(flat)
    tile, steps = scratch.shape[1], sems.shape[0]

    def copy(n):
        rows = pl.ds(pl.multiple_of(n * tile, tile), tile)
        source = weight.at[rows, 4 * HEAD :]
        return pltpu.make_async_copy(source, buffer.at[rows, :], sems.at[n])

    @pl.loop(0, steps)
    def _(n):
        copy(n).start()

    @pl.loop(0, steps)
    def _(n):
        copy(n).wait()
        cols = pl.ds(pl.multiple_of(n * tile, tile), tile)
        scratch[...] = lax.dot_general(
            context[...], buffer[cols, :], (((1,), (1,)), ((), ())), preferred_element_type=F32
        ).astype(BF16)
        for dy in range(2):
            for dz in range(4):
                first = jnp.bitwise_xor(yh, dy) * 64 + jnp.bitwise_and(z + dz, 3) * 16
                for block in range(2):
                    rows = pl.ds(pl.multiple_of(first + block * BLOCK, 16), 16)
                    outs[4 * dy + dz][block * 16 : block * 16 + 16, cols] = scratch[rows, :]


def finish_kernel(resident, gain, *refs):
    terms, out = refs[:8], refs[8]
    total = terms[0][...].astype(F32)
    for term in terms[1:]:
        total = total + term[...].astype(F32)
    scale = lax.rsqrt(jnp.mean(total * total, axis=1, keepdims=True) + EPS)
    out[...] = (resident[...].astype(F32) + total * scale * gain[...]).astype(BF16)


def owner_kernel(flat, new_blocks, *refs):
    by_w, outs = refs[:4], refs[4:]
    x, yl, c, _, _ = spot(flat)
    w = 2 * yl + c
    jobs = []
    for d in range(4):
        start = before(new_blocks, 4 * jnp.bitwise_and(x + d, 3) + w)
        level = (start + jnp.bitwise_and(x - start, 3)) >> 2
        slot = (level >= 4).astype(jnp.int32)
        source = jnp.bitwise_and(jnp.where(level < 4, level, 7 - level), 3)
        row = pl.ds(pl.multiple_of(slot * 16, 16), 16)
        jobs.append((jnp.bitwise_xor(source, w), [part.at[row, :] for part in by_w], outs[d]))
    move(jobs)


def place_kernel(flat, new_blocks, *refs):
    gathered, outs = refs[:4], refs[4:]
    x, yl, c, z, _ = spot(flat)
    start = before(new_blocks, 4 * x + 2 * yl + c)
    move([(jnp.bitwise_and(x - start - (z + d), 3), gathered, outs[d]) for d in range(4)])


def close_kernel(flat, new_blocks, *refs):
    parts, out = refs[:4], refs[4]
    x, yl, c, z, _ = spot(flat)
    count = new_blocks[4 * x + 2 * yl + c]

    @pl.when(z >= count)
    def _():
        out[...] = jnp.zeros_like(out)

    @pl.when(z < count)
    def _():
        for d in range(4):
            row = pl.multiple_of(jnp.bitwise_and(z - d, 3) * 16, 16)
            out[pl.ds(row, 16), :] = parts[d][...]


def per_device(
    x_old, old_blocks, new_blocks, order, pre_gain, post_gain, w_query, w_key, w_value, w_out_t
):
    flat = lax.axis_index(AXES).astype(jnp.int32).reshape(1)
    width = x_old.shape[1]
    count = 2 * BLOCK

    def near_by(arrays):
        return [pltpu.with_memory_space_constraint(a, pltpu.VMEM) for a in arrays]

    def far_off(arrays):
        return [pltpu.with_memory_space_constraint(a, pltpu.HBM) for a in arrays]

    def call(kernel, tables, arrays, shapes):
        results = pl.pallas_call(
            kernel,
            in_specs=[SMEM] * (1 + len(tables)) + [VMEM] * len(arrays),
            out_specs=[VMEM] * len(shapes),
            out_shape=[pltpu.VMEM(s, BF16) for s in shapes],
            compiler_params=grant(8),
        )(flat, *tables, *near_by(arrays))
        return list(results)

    def everywhere(part):
        opposite = shift(part, "x", 2)
        pair = shift(part, "yl", 1)
        same = [part, shift(part, "x", 1), opposite, shift(part, "x", 3)]
        other = [pair, shift(pair, "x", 1), shift(opposite, "yl", 1), shift(pair, "x", 3)]
        result = []
        for parts in (same, other):
            result += parts
            result += [shift(s, "c", 1) for s in parts]
        return result

    old = far_off((old_blocks, order))
    depth = w_key.shape[0]
    joined, held, *near = pl.pallas_call(
        leave_kernel,
        in_specs=[SMEM] * 3 + [AWAY] * 5,
        out_specs=[VMEM] * 6,
        out_shape=[
            jax.ShapeDtypeStruct((depth, 8 * HEAD), BF16),
            pltpu.VMEM((depth, 4 * HEAD), BF16),
        ]
        + [pltpu.VMEM((width, BLOCK), BF16)] * 4,
        scratch_shapes=[pltpu.SemaphoreType.DMA((10,))],
        compiler_params=grant(8),
        name="leave",
    )(flat, *old, *far_off((w_key, w_value, w_query, w_out_t, x_old.T)))
    joined_full = lax.all_gather(joined, SEQ, axis=0, tiled=True)
    pair = shift(held, "yl", 1)
    near = near[:1] + [shift(near[d], "x", d) for d in range(1, 4)]
    same = [held] + [shift(held, "x", d) for d in range(1, 4)]
    far = [shift(near[0], "c", 1)]
    far += [shift(part, "c", 1) for part in near[1:]]
    mine, cross = call(sort_kernel, old, near + far, [(width, count)] * 2)

    crossed = shift(cross, "yl", 1)
    both = [(a, b) for a in range(2) for b in range(2)]
    diagonal = lax.ppermute(
        cross, ("yl", "yh"), [(2 * a + b, 2 * (1 - a) + 1 - b) for a, b in both]
    )
    opposite = shift(mine, "yh", 1)
    other = [pair, shift(pair, "x", 1), shift(pair, "x", 3)]
    (rows,) = call(settle_kernel, old, (mine, crossed), [(width, count)])
    pieces = [rows] + [shift(rows, "z", d) for d in range(1, 4)]
    (facing,) = call(settle_kernel, old, (opposite, diagonal), [(width, count)])
    pieces += [facing] + [shift(facing, "z", d) for d in range(1, 4)]
    other.insert(2, shift(same[2], "yl", 1))
    spread_weights = [
        w for parts in (same, other) for w in parts + [shift(s, "c", 1) for s in parts]
    ]

    slot_rows = jnp.arange(BLOCK, dtype=jnp.int32)
    x, w = flat[0] >> 5, (flat[0] >> 3) & 3
    positions = jnp.concatenate(
        [b * BLOCK + slot_rows for b in (x + 4 * w, x + 28 - 4 * w)]
    )
    inverse = jnp.exp(jnp.arange(HEAD // 2, dtype=F32) * (-2.0 * math.log(10000.0) / HEAD))
    angles = positions.astype(F32)[:, None] * inverse[None, :]
    cosine, sine = jnp.cos(angles), jnp.sin(angles)
    cosine = jnp.concatenate([cosine, cosine], axis=1)
    sine = jnp.concatenate([-sine, sine], axis=1)

    normed, resident = pl.pallas_call(
        norm_kernel,
        in_specs=[SMEM] + [VMEM] * 9,
        out_specs=[VMEM] * 2,
        out_shape=[pltpu.VMEM((count, D), BF16), pltpu.VMEM((32, D), BF16)],
        scratch_shapes=[pltpu.VMEM((D, count), BF16), pltpu.VMEM((count, D), BF16)],
        compiler_params=grant(24),
        name="norm",
    )(flat, *near_by(pieces), pre_gain.reshape(1, D))
    tables = near_by((cosine, sine))

    def heads(kernel, first):
        return pl.pallas_call(
            kernel,
            grid=(2,),
            in_specs=[VMEM, pl.BlockSpec((D, 2 * HEAD), lambda n: (0, n + first)), VMEM, VMEM],
            out_specs=VMEM,
            out_shape=pltpu.VMEM((count, 4 * HEAD), BF16),
            compiler_params=grant(24),
        )(*near_by((normed,)), *far_off((joined_full,)), *tables)

    (kv_weights,) = call(pack_kernel, (), spread_weights, [(D, 4 * HEAD)])
    kv = pl.pallas_call(
        key_value_kernel,
        in_specs=[VMEM] * 4,
        out_specs=VMEM,
        out_shape=pltpu.VMEM((count, 4 * HEAD), BF16),
        compiler_params=grant(16),
        name="key_value",
    )(*near_by((normed, kv_weights)), *tables)

    spread = everywhere(kv)

    query = heads(query_kernel, 0)
    context = pl.pallas_call(
        attention_kernel,
        in_specs=[SMEM] + [VMEM] * 17,
        out_specs=VMEM,
        out_shape=pltpu.VMEM((count, 4 * HEAD), BF16),
        scratch_shapes=[pltpu.VMEM((2, 2 * BLOCK, HEAD), F32), pltpu.VMEM((2, 2 * BLOCK, HEAD), F32)],
        compiler_params=grant(24),
        name="attention",
    )(flat, *near_by((query, *spread)))

    tile = 512
    shares = pl.pallas_call(
        out_kernel,
        in_specs=[SMEM, VMEM, AWAY],
        out_specs=[VMEM] * 8,
        out_shape=[pltpu.VMEM((32, D), BF16)] * 8,
        scratch_shapes=[
            pltpu.VMEM((D, 4 * HEAD), BF16),
            pltpu.VMEM((count, tile), BF16),
            pltpu.SemaphoreType.DMA((D // tile,)),
        ],
        compiler_params=grant(16),
        name="project",
    )(flat, *near_by((context,)), *far_off((joined_full,)))
    received = []
    for dy in range(2):
        for dz in range(4):
            part = shares[4 * dy + dz]
            if dy and dz:
                n = [(i, j) for i in range(4) for j in range(2)]
                part = lax.ppermute(
                    part, TP, [(2 * i + j, 2 * ((i + dz) % 4) + (j ^ dy)) for i, j in n]
                )
            elif dy:
                part = shift(part, "yh", 1)
            elif dz:
                part = shift(part, "z", dz)
            received.append(part)

    refreshed = pl.pallas_call(
        finish_kernel,
        in_specs=[VMEM] * 10,
        out_specs=VMEM,
        out_shape=pltpu.VMEM((32, D), BF16),
        compiler_params=grant(8),
        name="finish",
    )(*near_by((resident, post_gain.reshape(1, D), *received)))

    by_yl = shift(refreshed, "yl", 1)
    by_w = [refreshed, shift(refreshed, "c", 1), by_yl, shift(by_yl, "c", 1)]
    new = far_off((new_blocks,))
    slices = [(16, D)] * 4
    gathered = call(owner_kernel, new, by_w, slices)
    gathered = gathered[:1] + [shift(gathered[d], "x", d) for d in range(1, 4)]
    final = call(place_kernel, new, gathered, slices)
    final = final[:1] + [shift(final[d], "z", d) for d in range(1, 4)]
    (layer_out,) = call(close_kernel, new, final, [(64, D)])
    return layer_out


def solution(mesh):
    torus = Mesh(mesh.devices.reshape(4, 2, 2, 4, 2), AXES)
    in_specs = (
        P(SEQ, TP),
        P(),
        P(),
        P(),
        P(),
        P(),
        P(SEQ, TP),
        P(SEQ, TP),
        P(SEQ, TP),
        P(SEQ, TP),
    )
    out_specs = P(SEQ + TP, None)

    return jax.shard_map(
        per_device, mesh=torus, in_specs=in_specs, out_specs=out_specs, check_vma=False
    )
```

```python
import math

import jax
import jax.numpy as jnp
from jax import lax
from jax.experimental import pallas as pl
from jax.experimental.pallas import tpu as pltpu
from jax.sharding import Mesh
from jax.sharding import PartitionSpec as P

D = 4608
HEADS = 32
HEAD = 128
BLOCK = 128
EPS = 1e-06
F32 = jnp.float32
BF16 = jnp.bfloat16

AXES = ("x", "yl", "c", "z", "yh")
SEQ = ("x", "yl", "c")
TP = ("z", "yh")


SMEM = pl.BlockSpec(memory_space=pltpu.SMEM)


def shift(value, axis, by):
    n = lax.axis_size(axis)
    return lax.ppermute(value, axis, [(i, (i + by) % n) for i in range(n)])


def rope(values, cos, sin):
    half = HEAD // 2
    swapped = jnp.concatenate([values[:, half:], values[:, :half]], axis=1)
    return values * cos + swapped * sin


def spot(flat):
    me = flat[0]
    return me >> 5, (me >> 4) & 1, (me >> 3) & 1, (me >> 1) & 3, me & 1


def starts(blocks):
    result, so_far = [], jnp.int32(0)
    for m in range(16):
        result.append(so_far)
        so_far = so_far + blocks[m]
    return result


VMEM = pl.BlockSpec(memory_space=pltpu.VMEM)
AWAY = pl.BlockSpec(memory_space=pl.ANY)


def grant(mib):
    return pltpu.CompilerParams(vmem_limit_bytes=mib << 20)


def move(jobs):
    for index, sources, target in jobs:
        for k, source in enumerate(sources):

            def copy(source=source, target=target):
                target[...] = source[...]

            if len(sources) == 1:
                copy()
            else:
                pl.when(index == k)(copy)


def lanes(first):
    return pl.ds(pl.multiple_of(first, BLOCK), BLOCK)


def fetch(jobs, sems):
    copies = [pltpu.make_async_copy(s, t, sems.at[n]) for n, (s, t) in enumerate(jobs)]
    for copy in copies:
        copy.start()
    for copy in copies:
        copy.wait()


def pack_kernel(flat, *refs):
    parts, whole = refs[:16], refs[16]
    x, yl, c, _, _ = spot(flat)
    size = parts[0].shape[0]
    for n, part in enumerate(parts):
        w = jnp.bitwise_xor(2 * yl + c, n // 4)
        first = (4 * jnp.bitwise_and(x - n % 4, 3) + w) * size
        whole[pl.ds(pl.multiple_of(first, 32), size), :] = part[...]


def before(blocks, shard):
    result = jnp.int32(0)
    for m in range(16):
        result = result + jnp.where(m < shard, blocks[m], 0)
    return result


def leave_kernel(flat, old_blocks, order, key, value, query, out_t, x_old, *refs):
    joined, held, outs, sems = refs[0], refs[1], refs[2:6], refs[6]
    x, yl, c, _, _ = spot(flat)
    half = 4 * HEAD
    jobs = [(query, joined.at[:, :half]), (out_t, joined.at[:, half:])]
    for n, source in enumerate((key, value, key, value)):
        first = n // 2 * HEAD
        jobs.append((source.at[:, first : first + HEAD], held.at[:, n * HEAD : (n + 1) * HEAD]))
    first = before(old_blocks, order[4 * x + 2 * yl + c])
    for d in range(4):
        row = jnp.bitwise_and(x + d - first, 3) * BLOCK
        jobs.append((x_old.at[:, lanes(row)], outs[d]))
    fetch(jobs, sems)


def holders(old_blocks, order, blocks):
    begin = starts(old_blocks)
    result = []
    for block in blocks:
        shard = jnp.int32(-1)
        for m in range(16):
            shard = shard + (begin[m] <= block).astype(jnp.int32)
        holder = jnp.int32(0)
        for m in range(16):
            holder = holder + jnp.where(order[m] == shard, m, 0)
        result.append(holder)
    return result


def targets(x, yl, c):
    to = 2 * yl + c
    return [x + 4 * to, x + 28 - 4 * to]


def sort_kernel(flat, old_blocks, order, *refs):
    sources, (mine, cross) = refs[:8], refs[8:]
    x, yl, c, _, _ = spot(flat)
    blocks = targets(x, yl, c) + targets(x, 1 - yl, c)
    jobs = []
    for n, holder in enumerate(holders(old_blocks, order, blocks)):
        index = jnp.bitwise_and(x - (holder >> 2), 3) + 4 * jnp.bitwise_xor(holder & 1, c)
        out, at = (mine, n) if n < 2 else (cross, n - 2)
        jobs.append((index, sources, out.at[:, at * BLOCK : (at + 1) * BLOCK]))
    move(jobs)


def settle_kernel(flat, old_blocks, order, mine, crossed, rows):
    x, yl, c, _, _ = spot(flat)
    jobs = []
    for n, holder in enumerate(holders(old_blocks, order, targets(x, yl, c))):
        at = slice(n * BLOCK, (n + 1) * BLOCK)
        index = jnp.bitwise_xor((holder >> 1) & 1, yl)
        jobs.append((index, [mine.at[:, at], crossed.at[:, at]], rows.at[:, at]))
    move(jobs)


def norm_kernel(flat, *refs):
    pieces, (gain, normed, resident, features, raw) = refs[:8], refs[8:]
    _, _, _, z, yh = spot(flat)
    width, count = pieces[0].shape
    total = jnp.zeros((1, count), F32)
    for n, piece in enumerate(pieces):
        wide = piece[...].astype(F32)
        total = total + jnp.sum(wide * wide, axis=0, keepdims=True)
        t = 2 * jnp.bitwise_and(z - n % 4, 3) + jnp.bitwise_xor(yh, n // 4)
        features[pl.ds(pl.multiple_of(t * width, 64), width), :] = piece[...]
    scale = lax.rsqrt(total / D + EPS)
    scale = jnp.transpose(jnp.broadcast_to(scale, (BLOCK, count)))
    step = 512
    for at in range(0, D, step):
        rows = jnp.transpose(features[at : at + step, :])
        raw[:, at : at + step] = rows
        for k in range(0, step, BLOCK):
            cols = slice(at + k, at + k + BLOCK)
            wide = rows[:, k : k + BLOCK].astype(F32) * scale * gain[:, cols]
            normed[:, cols] = wide.astype(BF16)
    first = pl.multiple_of(64 * yh + 16 * z, 16)
    for block in range(2):
        source = pl.ds(pl.multiple_of(first + block * BLOCK, 16), 16)
        resident[block * 16 : block * 16 + 16, :] = raw[source, :]


def key_value_kernel(normed, weight, cos, sin, kv):
    total = jnp.dot(normed[...], weight[...], preferred_element_type=F32)
    for h in range(2):
        at = 2 * h * HEAD
        kv[:, at : at + HEAD] = rope(total[:, at : at + HEAD], cos[...], sin[...]).astype(BF16)
        kv[:, at + HEAD : at + 2 * HEAD] = total[:, at + HEAD : at + 2 * HEAD].astype(BF16)


def query_kernel(normed, weight, cos, sin, query):
    total = jnp.dot(normed[...], weight[...], preferred_element_type=F32)
    at = pl.multiple_of(pl.program_id(0) * 2 * HEAD, 2 * HEAD)
    for h in range(2):
        part = total[:, h * HEAD : (h + 1) * HEAD]
        turned = rope(part, cos[...], sin[...]) * (D // HEADS) ** (-0.5)
        query[:, pl.ds(at + h * HEAD, HEAD)] = turned.astype(BF16)


def attention_kernel(flat, query, *refs):
    kv = [refs[4 * k : 4 * k + 4] for k in range(4)]
    weight, context, ready, numer, denom, sems = refs[16:]
    copy = pltpu.make_async_copy(weight.at[:, 4 * HEAD :], ready, sems.at[0])
    copy.start()
    x, yl, c, _, _ = spot(flat)
    w = 2 * yl + c
    row = lax.broadcasted_iota(jnp.int32, (2 * BLOCK, BLOCK), 0) % BLOCK
    col = lax.broadcasted_iota(jnp.int32, (2 * BLOCK, BLOCK), 1)

    def chunk(first, dw, block, slot, masked):
        near, far = pl.ds(first, HEAD), pl.ds(first + HEAD, HEAD)
        if isinstance(block, int):
            q_rows, k_rows = pl.ds(block * BLOCK, BLOCK), pl.ds(slot * BLOCK, BLOCK)
        else:
            q_rows = pl.ds(pl.multiple_of(block * BLOCK, BLOCK), BLOCK)
            k_rows = pl.ds(pl.multiple_of(slot * BLOCK, BLOCK), BLOCK)
        q2 = jnp.concatenate([query[q_rows, near], query[q_rows, far]], axis=0)
        keys = jnp.concatenate([kv[dw][d][k_rows, near] for d in range(4)], axis=0)
        values = jnp.concatenate([kv[dw][d][k_rows, far] for d in range(4)], axis=0)
        score = lax.dot_general(q2, keys, (((1,), (1,)), ((), ())), preferred_element_type=F32)
        weight = jnp.exp(50.0 * jnp.tanh(score * (1.0 / 50.0)))
        parts = [weight[:, d * BLOCK : (d + 1) * BLOCK] for d in range(4)]
        if masked:
            parts = [jnp.where(col <= row, parts[0], 0.0)] + [
                jnp.where(x >= d, parts[d], 0.0) for d in range(1, 4)
            ]
            weight = jnp.concatenate(parts, axis=1)
        denom[block] += (parts[0] + parts[1]) + (parts[2] + parts[3])
        numer[block] += jnp.dot(weight.astype(BF16), values, preferred_element_type=F32)

    @pl.loop(0, 2)
    def _(head):
        first = pl.multiple_of(head * 2 * HEAD, 2 * HEAD)
        numer[...] = jnp.zeros_like(numer)
        denom[...] = jnp.zeros_like(denom)
        chunk(first, 0, 0, 0, True)
        chunk(first, 0, 1, 0, False)
        chunk(first, 0, 1, 1, True)
        for dw in range(1, 4):
            later = (jnp.bitwise_xor(w, dw) > w).astype(jnp.int32)
            chunk(first, dw, 1, 0, False)
            chunk(first, dw, later, later, False)
        for block in range(2):
            out = numer[block] / jnp.sum(denom[block], axis=1, keepdims=True)
            rows = slice(block * BLOCK, (block + 1) * BLOCK)
            context[rows, pl.ds(first, HEAD)] = out[:BLOCK].astype(BF16)
            context[rows, pl.ds(first + HEAD, HEAD)] = out[BLOCK:].astype(BF16)

    copy.wait()


def out_kernel(flat, context, weight, *refs):
    outs, scratch = refs[:8], refs[8]
    _, _, _, z, yh = spot(flat)
    tile = scratch.shape[1]

    @pl.loop(0, weight.shape[0] // tile)
    def _(n):
        cols = pl.ds(pl.multiple_of(n * tile, tile), tile)
        scratch[...] = lax.dot_general(
            context[...], weight[cols, :], (((1,), (1,)), ((), ())), preferred_element_type=F32
        ).astype(BF16)
        for dy in range(2):
            for dz in range(4):
                first = jnp.bitwise_xor(yh, dy) * 64 + jnp.bitwise_and(z + dz, 3) * 16
                for block in range(2):
                    rows = pl.ds(pl.multiple_of(first + block * BLOCK, 16), 16)
                    outs[4 * dy + dz][block * 16 : block * 16 + 16, cols] = scratch[rows, :]


def finish_kernel(resident, gain, *refs):
    terms, out = refs[:8], refs[8]
    total = terms[0][...].astype(F32)
    for term in terms[1:]:
        total = total + term[...].astype(F32)
    scale = lax.rsqrt(jnp.mean(total * total, axis=1, keepdims=True) + EPS)
    out[...] = (resident[...].astype(F32) + total * scale * gain[...]).astype(BF16)


def owner_kernel(flat, new_blocks, *refs):
    by_w, outs = refs[:4], refs[4:]
    x, yl, c, _, _ = spot(flat)
    w = 2 * yl + c
    jobs = []
    for d in range(4):
        start = before(new_blocks, 4 * jnp.bitwise_and(x + d, 3) + w)
        level = (start + jnp.bitwise_and(x - start, 3)) >> 2
        slot = (level >= 4).astype(jnp.int32)
        source = jnp.bitwise_and(jnp.where(level < 4, level, 7 - level), 3)
        row = pl.ds(pl.multiple_of(slot * 16, 16), 16)
        jobs.append((jnp.bitwise_xor(source, w), [part.at[row, :] for part in by_w], outs[d]))
    move(jobs)


def place_kernel(flat, new_blocks, *refs):
    gathered, outs = refs[:4], refs[4:]
    x, yl, c, z, _ = spot(flat)
    start = before(new_blocks, 4 * x + 2 * yl + c)
    move([(jnp.bitwise_and(x - start - (z + d), 3), gathered, outs[d]) for d in range(4)])


def close_kernel(flat, new_blocks, *refs):
    parts, out = refs[:4], refs[4]
    x, yl, c, z, _ = spot(flat)
    count = new_blocks[4 * x + 2 * yl + c]

    @pl.when(z >= count)
    def _():
        out[...] = jnp.zeros_like(out)

    @pl.when(z < count)
    def _():
        for d in range(4):
            row = pl.multiple_of(jnp.bitwise_and(z - d, 3) * 16, 16)
            out[pl.ds(row, 16), :] = parts[d][...]


def per_device(
    x_old, old_blocks, new_blocks, order, pre_gain, post_gain, w_query, w_key, w_value, w_out_t
):
    flat = lax.axis_index(AXES).astype(jnp.int32).reshape(1)
    width = x_old.shape[1]
    count = 2 * BLOCK

    def near_by(arrays):
        return [pltpu.with_memory_space_constraint(a, pltpu.VMEM) for a in arrays]

    def far_off(arrays):
        return [pltpu.with_memory_space_constraint(a, pltpu.HBM) for a in arrays]

    def call(kernel, tables, arrays, shapes):
        results = pl.pallas_call(
            kernel,
            in_specs=[SMEM] * (1 + len(tables)) + [VMEM] * len(arrays),
            out_specs=[VMEM] * len(shapes),
            out_shape=[pltpu.VMEM(s, BF16) for s in shapes],
            compiler_params=grant(8),
        )(flat, *tables, *near_by(arrays))
        return list(results)

    def everywhere(part):
        opposite = shift(part, "x", 2)
        pair = shift(part, "yl", 1)
        same = [part, shift(part, "x", 1), opposite, shift(part, "x", 3)]
        other = [pair, shift(pair, "x", 1), shift(opposite, "yl", 1), shift(pair, "x", 3)]
        result = []
        for parts in (same, other):
            result += parts
            result += [shift(s, "c", 1) for s in parts]
        return result

    old = far_off((old_blocks, order))
    depth = w_key.shape[0]
    joined, held, *near = pl.pallas_call(
        leave_kernel,
        in_specs=[SMEM] * 3 + [AWAY] * 5,
        out_specs=[VMEM] * 6,
        out_shape=[
            jax.ShapeDtypeStruct((depth, 8 * HEAD), BF16),
            pltpu.VMEM((depth, 4 * HEAD), BF16),
        ]
        + [pltpu.VMEM((width, BLOCK), BF16)] * 4,
        scratch_shapes=[pltpu.SemaphoreType.DMA((10,))],
        compiler_params=grant(8),
        name="leave",
    )(flat, *old, *far_off((w_key, w_value, w_query, w_out_t, x_old.T)))
    joined_full = lax.all_gather(joined, SEQ, axis=0, tiled=True)
    pair = shift(held, "yl", 1)
    near = near[:1] + [shift(near[d], "x", d) for d in range(1, 4)]
    same = [held] + [shift(held, "x", d) for d in range(1, 4)]
    far = [shift(near[0], "c", 1)]
    far += [shift(part, "c", 1) for part in near[1:]]
    mine, cross = call(sort_kernel, old, near + far, [(width, count)] * 2)

    crossed = shift(cross, "yl", 1)
    both = [(a, b) for a in range(2) for b in range(2)]
    diagonal = lax.ppermute(
        cross, ("yl", "yh"), [(2 * a + b, 2 * (1 - a) + 1 - b) for a, b in both]
    )
    opposite = shift(mine, "yh", 1)
    other = [pair, shift(pair, "x", 1), shift(pair, "x", 3)]
    (rows,) = call(settle_kernel, old, (mine, crossed), [(width, count)])
    pieces = [rows] + [shift(rows, "z", d) for d in range(1, 4)]
    (facing,) = call(settle_kernel, old, (opposite, diagonal), [(width, count)])
    pieces += [facing] + [shift(facing, "z", d) for d in range(1, 4)]
    other.insert(2, shift(same[2], "yl", 1))
    spread_weights = [
        w for parts in (same, other) for w in parts + [shift(s, "c", 1) for s in parts]
    ]

    slot_rows = jnp.arange(BLOCK, dtype=jnp.int32)
    x, w = flat[0] >> 5, (flat[0] >> 3) & 3
    positions = jnp.concatenate(
        [b * BLOCK + slot_rows for b in (x + 4 * w, x + 28 - 4 * w)]
    )
    inverse = jnp.exp(jnp.arange(HEAD // 2, dtype=F32) * (-2.0 * math.log(10000.0) / HEAD))
    angles = positions.astype(F32)[:, None] * inverse[None, :]
    cosine, sine = jnp.cos(angles), jnp.sin(angles)
    cosine = jnp.concatenate([cosine, cosine], axis=1)
    sine = jnp.concatenate([-sine, sine], axis=1)

    normed, resident = pl.pallas_call(
        norm_kernel,
        in_specs=[SMEM] + [VMEM] * 9,
        out_specs=[VMEM] * 2,
        out_shape=[pltpu.VMEM((count, D), BF16), pltpu.VMEM((32, D), BF16)],
        scratch_shapes=[pltpu.VMEM((D, count), BF16), pltpu.VMEM((count, D), BF16)],
        compiler_params=grant(24),
        name="norm",
    )(flat, *near_by(pieces), pre_gain.reshape(1, D))
    tables = near_by((cosine, sine))

    def heads(kernel, first):
        return pl.pallas_call(
            kernel,
            grid=(2,),
            in_specs=[VMEM, pl.BlockSpec((D, 2 * HEAD), lambda n: (0, n + first)), VMEM, VMEM],
            out_specs=VMEM,
            out_shape=pltpu.VMEM((count, 4 * HEAD), BF16),
            compiler_params=grant(24),
        )(*near_by((normed,)), *far_off((joined_full,)), *tables)

    (kv_weights,) = call(pack_kernel, (), spread_weights, [(D, 4 * HEAD)])
    kv = pl.pallas_call(
        key_value_kernel,
        in_specs=[VMEM] * 4,
        out_specs=VMEM,
        out_shape=pltpu.VMEM((count, 4 * HEAD), BF16),
        compiler_params=grant(16),
        name="key_value",
    )(*near_by((normed, kv_weights)), *tables)

    spread = everywhere(kv)

    query = heads(query_kernel, 0)
    context, out_weights = pl.pallas_call(
        attention_kernel,
        in_specs=[SMEM] + [VMEM] * 17 + [AWAY],
        out_specs=[VMEM] * 2,
        out_shape=[pltpu.VMEM((count, 4 * HEAD), BF16), pltpu.VMEM((D, 4 * HEAD), BF16)],
        scratch_shapes=[
            pltpu.VMEM((2, 2 * BLOCK, HEAD), F32),
            pltpu.VMEM((2, 2 * BLOCK, HEAD), F32),
            pltpu.SemaphoreType.DMA((1,)),
        ],
        compiler_params=grant(24),
        name="attention",
    )(flat, *near_by((query, *spread)), *far_off((joined_full,)))

    tile = 512
    shares = pl.pallas_call(
        out_kernel,
        in_specs=[SMEM, VMEM, VMEM],
        out_specs=[VMEM] * 8,
        out_shape=[pltpu.VMEM((32, D), BF16)] * 8,
        scratch_shapes=[pltpu.VMEM((count, tile), BF16)],
        compiler_params=grant(16),
        name="project",
    )(flat, *near_by((context, out_weights)))
    received = []
    for dy in (1, 0):
        for dz in (2, 1, 3, 0):
            part = shares[4 * dy + dz]
            if dy and dz:
                n = [(i, j) for i in range(4) for j in range(2)]
                part = lax.ppermute(
                    part, TP, [(2 * i + j, 2 * ((i + dz) % 4) + (j ^ dy)) for i, j in n]
                )
            elif dy:
                part = shift(part, "yh", 1)
            elif dz:
                part = shift(part, "z", dz)
            received.append(part)

    refreshed = pl.pallas_call(
        finish_kernel,
        in_specs=[VMEM] * 10,
        out_specs=VMEM,
        out_shape=pltpu.VMEM((32, D), BF16),
        compiler_params=grant(8),
        name="finish",
    )(*near_by((resident, post_gain.reshape(1, D), *received)))

    by_yl = shift(refreshed, "yl", 1)
    by_w = [refreshed, shift(refreshed, "c", 1), by_yl, shift(by_yl, "c", 1)]
    new = far_off((new_blocks,))
    slices = [(16, D)] * 4
    gathered = call(owner_kernel, new, by_w, slices)
    gathered = gathered[:1] + [shift(gathered[d], "x", d) for d in range(1, 4)]
    final = call(place_kernel, new, gathered, slices)
    final = final[:1] + [shift(final[d], "z", d) for d in range(1, 4)]
    (layer_out,) = call(close_kernel, new, final, [(64, D)])
    return layer_out


def solution(mesh):
    torus = Mesh(mesh.devices.reshape(4, 2, 2, 4, 2), AXES)
    in_specs = (
        P(SEQ, TP),
        P(),
        P(),
        P(),
        P(),
        P(),
        P(SEQ, TP),
        P(SEQ, TP),
        P(SEQ, TP),
        P(SEQ, TP),
    )
    out_specs = P(SEQ + TP, None)

    return jax.shard_map(
        per_device, mesh=torus, in_specs=in_specs, out_specs=out_specs, check_vma=False
    )
```
